128 devices in a mesh: row: 4 (over z), col: 32 (over y, x, core).
Axes of the slice: x: 4, y: 4, z: 4, core: 2. Of those that a mesh axis runs over, the one named last changes fastest.
Arguments:
- inv_depth: float32 [256, 3072], P(('row', 'col')), may hold values from 0.2 to 1
- rotation: float32 [3, 256], P(None, ('row', 'col')), may hold values from -0.05 to 0.05
- translation: float32 [3, 256], P(None, ('row', 'col')), may hold values from -0.25 to 0.25
- edge_target: int32 [256, 24], P(('row', 'col')), may hold values from 0 to 255, as said below
- flow_obs: float32 [2, 256, 24, 3072], P(None, ('row', 'col')), may hold values from -2.8 to 2.8
- weight: float32 [2, 256, 24, 3072], P(None, ('row', 'col')), may hold values from 0.1 to 1
Outputs:
- depth_next: float32 [256, 3072], P(('row', 'col'))
- pose_step: float32 [6, 256], P(None, ('row', 'col'))
The draws below stay inside these ranges and needn't reach their ends.
Inputs may be any that keep to these rules, and one draw needn't show every extreme that they name: `edge_target`: each keyframe's targets are distinct, differ from the keyframe itself, are sorted ascending, and lie in the keyframe's own block of 64 consecutive keyframes or in one of the two neighbouring blocks, the blocks counted cyclically.
All inputs are finite; a program needn't handle non-finite values.
Results may differ from the reference program's by a relative error of at most 0.0003.
Values sent between devices are 32-bit elements; how exact they have to be, the bound alone decides.
A program may use at most 128 MiB of HBM per device.

```python
import math
import jax
import jax.numpy as jnp
from jax import lax

IMG_H = 48
IMG_W = 64
PIXELS = 3072
F_DEV = 2
E_FRAME = 24
GROUP = 64
FRAMES = 256


def draw_edge_target(key, part):
    base_key = jax.random.fold_in(key, 11)
    key_pop, key_mix = jax.random.split(base_key)
    frames = jnp.arange(FRAMES, dtype=jnp.int32)
    group_id = frames // GROUP
    candidates = 3 * GROUP
    popular = jax.random.randint(key_pop, (FRAMES,), 0, 4) * 16384
    jitter = jax.random.randint(key_mix, (FRAMES, candidates), 0, 65536)
    cand_index = jnp.arange(candidates, dtype=jnp.int32)
    cand_group = (group_id[:, None] - 1 + cand_index[None, :] // GROUP + FRAMES // GROUP) % (FRAMES // GROUP)
    cand_frame = cand_group * GROUP + cand_index[None, :] % GROUP
    scores = jitter + jnp.take(popular, cand_frame)
    scores = jnp.where(cand_frame == frames[:, None], -1, scores)
    scores = scores * 4096 + cand_index[None, :]
    _, picked = lax.top_k(scores, E_FRAME)
    chosen = jnp.take_along_axis(cand_frame, picked, 1)
    return jnp.sort(chosen, 1).astype(jnp.int32)


def draw_flow_obs(key, part):
    base_key = jax.random.fold_in(key, 23)
    key_bias, key_noise = jax.random.split(base_key)
    offset_part = 0.4 * jnp.clip(jax.random.normal(key_bias, (2, FRAMES, E_FRAME, 1), jnp.float32), -4.0, 4.0)
    jitter = 0.3 * jnp.clip(jax.random.normal(key_noise, (2, FRAMES, E_FRAME, PIXELS), jnp.float32), -4.0, 4.0)
    return (offset_part + jitter).astype(jnp.float32)


def block_levels(own_key, extent, cuts, smallest, high):
    loudness, own = 1.0, jax.random.fold_in(own_key, 6)
    for axis_at, parts in cuts:
        steps = jnp.exp(jax.random.uniform(jax.random.fold_in(own, axis_at), (parts,), jnp.float32, smallest / len(cuts), high / len(cuts)))
        loudness = loudness * jnp.repeat(steps, extent[axis_at] // parts).reshape([-1 if axis == axis_at else 1 for axis in range(len(extent))])
    return loudness


def setup_inputs(seed: int = 0) -> dict:
    key_of = jax.random.split(jax.random.key(seed), 7)
    inv_depth = jnp.clip(jnp.exp(math.log(1.0) - 1.609438 * jax.random.uniform(key_of[0], (FRAMES, PIXELS), jnp.float32) ** block_levels(key_of[0], (FRAMES, PIXELS), ((0, 128),), -0.2, 0.2)), 0.2, 1.0)
    rotation = jnp.clip(jax.random.uniform(key_of[1], (3, FRAMES), jnp.float32, -0.05, 0.05) * block_levels(key_of[1], (3, FRAMES), ((1, 128),), -0.4, 0.0), -0.05, 0.05)
    translation = jnp.clip(jax.random.uniform(key_of[2], (3, FRAMES), jnp.float32, -0.25, 0.25) * block_levels(key_of[2], (3, FRAMES), ((1, 128),), -0.4, 0.0), -0.25, 0.25)
    edge_target = draw_edge_target(jax.random.fold_in(key_of[6], 71), 0)
    flow_obs = draw_flow_obs(jax.random.fold_in(key_of[6], 71), 0)
    weight = jnp.clip(jnp.exp(math.log(1.0) - 2.3025851 * jax.random.uniform(key_of[5], (2, FRAMES, E_FRAME, PIXELS), jnp.float32) ** block_levels(key_of[5], (2, FRAMES, E_FRAME, PIXELS), ((1, 128),), -0.2, 0.2)), 0.1, 1.0)
    return {"inv_depth": inv_depth, "rotation": rotation, "translation": translation, "edge_target": edge_target, "flow_obs": flow_obs, "weight": weight}


PRECISE = lax.Precision.HIGHEST
DAMP_DEPTH = 0.1
LEVENBERG = 0.1
RIDGE = 0.001

def pixel_grid(pixel_count):
    pixel_index = jnp.arange(pixel_count, dtype=jnp.int32)
    across = (pixel_index % IMG_W).astype(jnp.float32)
    downward = (pixel_index // IMG_W).astype(jnp.float32)
    return ((across + 0.5) / IMG_W - 0.5, (downward + 0.5 - 0.5 * IMG_H) / IMG_W)

def edge_terms(relative, target_depth, flows, weights, across, downward):
    spin_x, spin_y, spin_z, move_x, move_y, move_z = [relative[i][:, None] for i in range(6)]
    point_x = across + spin_y - spin_z * downward + move_x * target_depth
    point_y = downward + spin_z * across - spin_x + move_y * target_depth
    point_z = 1.0 + spin_x * downward - spin_y * across + move_z * target_depth
    recip_z = 1.0 / point_z
    image_u = point_x * recip_z
    image_v = point_y * recip_z
    resid_u = flows[0] - (image_u - across)
    resid_v = flows[1] - (image_v - downward)
    slope_u = recip_z * (move_x - image_u * move_z)
    slope_v = recip_z * (move_y - image_v * move_z)
    depth_recip = target_depth * recip_z
    blank_map = jnp.zeros_like(recip_z)
    jac_u = jnp.stack([-image_u * downward * recip_z, (1.0 + image_u * across) * recip_z, -downward * recip_z, depth_recip, blank_map, -image_u * depth_recip])
    jac_v = jnp.stack([(-1.0 - image_v * downward) * recip_z, image_v * across * recip_z, across * recip_z, blank_map, depth_recip, -image_v * depth_recip])
    weight_u = weights[0]
    weight_v = weights[1]
    depth_grad = weight_u * slope_u * resid_u + weight_v * slope_v * resid_v
    depth_curv = weight_u * slope_u * slope_u + weight_v * slope_v * slope_v
    scaled_u = weight_u * jac_u
    scaled_v = weight_v * jac_v
    coupling = scaled_u * slope_u + scaled_v * slope_v
    block = jnp.einsum('aep,bep->eab', scaled_u, jac_u, precision=PRECISE) + jnp.einsum('aep,bep->eab', scaled_v, jac_v, precision=PRECISE)
    pose_grad = jnp.einsum('aep,ep->ea', scaled_u, resid_u, precision=PRECISE) + jnp.einsum('aep,ep->ea', scaled_v, resid_v, precision=PRECISE)
    return (depth_grad, depth_curv, coupling, block, pose_grad)

def solve_frames(block_table):
    frame_count = block_table.shape[0]
    matrix = block_table[:, :36].reshape(frame_count, 6, 6).transpose(1, 2, 0)
    right_side = block_table[:, 36:].T
    factor = {}
    for i in range(6):
        for j in range(i + 1):
            element = matrix[i, j]
            if i == j:
                element = element * (1.0 + LEVENBERG) + RIDGE
            for k in range(j):
                element = element - factor[i, k] * factor[j, k]
            factor[i, j] = jnp.sqrt(element) if i == j else element / factor[j, j]
    forward = []
    for i in range(6):
        element = right_side[i]
        for k in range(i):
            element = element - factor[i, k] * forward[k]
        forward.append(element / factor[i, i])
    result = [None] * 6
    for i in reversed(range(6)):
        element = forward[i]
        for k in range(i + 1, 6):
            element = element - factor[k, i] * result[k]
        result[i] = element / factor[i, i]
    return jnp.stack(result, 1)

def reference(inv_depth, rotation, translation, edge_target, flow_obs, weight):
    across, downward = pixel_grid(PIXELS)
    blocks = FRAMES // F_DEV
    block_edges = F_DEV * E_FRAME
    targets = edge_target.reshape(blocks, block_edges)
    sources = (jnp.arange(FRAMES * E_FRAME, dtype=jnp.int32) // E_FRAME).reshape(blocks, block_edges)
    flows = flow_obs.reshape(2, blocks, block_edges, PIXELS).transpose(1, 0, 2, 3)
    weights = weight.reshape(2, blocks, block_edges, PIXELS).transpose(1, 0, 2, 3)
    pose_all = jnp.concatenate([rotation, translation], 0)
    pieces_all = (sources, targets, flows, weights)

    def block_terms(pieces):
        source, target, flow_block, weight_block = pieces
        relative = pose_all[:, source] - pose_all[:, target]
        return edge_terms(relative, inv_depth[target], flow_block, weight_block, across, downward)

    def first_pass(state_sum, pieces):
        grad_part, curv_part, _, _, _ = block_terms(pieces)
        target = pieces[1]
        return ((state_sum[0] + jax.ops.segment_sum(grad_part, target, num_segments=FRAMES), state_sum[1] + jax.ops.segment_sum(curv_part, target, num_segments=FRAMES)), None)
    zeros_map = jnp.zeros((FRAMES, PIXELS), jnp.float32)
    (grad_sum, curv_sum), _ = lax.scan(first_pass, (zeros_map, zeros_map), pieces_all)
    inverse = 1.0 / (DAMP_DEPTH + curv_sum)
    scaled = grad_sum * inverse

    def second_pass(state_sum, pieces):
        _, _, coupling, block, pose_grad = block_terms(pieces)
        source, target = (pieces[0], pieces[1])
        reduced = block - jnp.einsum('aep,bep->eab', coupling * inverse[target][None], coupling, precision=PRECISE)
        reduced_grad = pose_grad - jnp.einsum('aep,ep->ea', coupling, scaled[target], precision=PRECISE)
        flat_block = reduced.reshape(-1, 36)
        out_rows = jnp.concatenate([flat_block, reduced_grad], 1)
        in_rows = jnp.concatenate([flat_block, -reduced_grad], 1)
        return (state_sum + jax.ops.segment_sum(out_rows, source, num_segments=FRAMES) + jax.ops.segment_sum(in_rows, target, num_segments=FRAMES), None)
    block_table, _ = lax.scan(second_pass, jnp.zeros((FRAMES, 42), jnp.float32), pieces_all)
    frame_steps = solve_frames(block_table)

    def third_pass(state_sum, pieces):
        _, _, coupling, _, _ = block_terms(pieces)
        source, target = (pieces[0], pieces[1])
        motion = frame_steps[source] - frame_steps[target]
        correction = jnp.einsum('aep,ea->ep', coupling, motion, precision=PRECISE)
        return (state_sum + jax.ops.segment_sum(correction, target, num_segments=FRAMES), None)
    fix_sum, _ = lax.scan(third_pass, zeros_map, pieces_all)
    depth_next = inv_depth + (grad_sum - fix_sum) * inverse
    return (depth_next, frame_steps.T)
```

```python
import functools

import jax
import jax.numpy as jnp
from jax import lax
from jax.experimental import pallas as pl
from jax.experimental.pallas import tpu as pltpu
from jax.sharding import PartitionSpec as P

F32 = jnp.float32
BF16 = jnp.bfloat16
NDEV = 128
PX = 24
GROUPS = 16
LANES = 384
MESH = pl.DeviceIdType.MESH
PAIRS = [(a, b) for a in (0, 1, 2, 5) for b in (0, 1, 2, 5) if a <= b]
K_ROWS = [*PAIRS, *[(3, b) for b in range(6)], *[(4, b) for b in (0, 1, 2, 4, 5)]]
K_INDEX = {}
for _n, (_a, _b) in enumerate(K_ROWS):
    K_INDEX[_a, _b] = _n
    K_INDEX[_b, _a] = _n
H_ROW = 21


def lane_iota(shape=(8, 128)):
    return lax.broadcasted_iota(jnp.int32, shape, 1)


def pack_kernel(flow_ref, weight_ref, depth_ref, extra_ref, out_ref, low, high):
    turn = lax.axis_index("col") % 8

    def put(ref, block, value):
        at = pl.multiple_of(((3 * turn + block) % 8) * 16, 16)
        ref[pl.ds(at, 16), :] = value

    for n in range(3):
        put(low, n, flow_ref[0, 16 * n : 16 * n + 16, :])
        put(low, 3 + n, flow_ref[1, 16 * n : 16 * n + 16, :])
        put(high, 1 + n, weight_ref[1, 16 * n : 16 * n + 16, :])
        put(high, 4 + n, jnp.zeros((16, LANES), F32))
    put(low, 6, weight_ref[0, 0:16, :])
    put(low, 7, weight_ref[0, 16:32, :])
    put(high, 0, weight_ref[0, 32:48, :])
    dep = depth_ref[...]
    put(high, 7, jnp.concatenate([dep, dep], 0))
    low_t = low[...].T
    high_t = high[...].T
    where_at = (lane_iota() - 48 * turn + 384) % 128
    extra = pltpu.roll(extra_ref[...], 48 * turn, 1)
    for d in range(16):
        base = 24 * d
        for j in range(3):
            out_ref[d, 8 * j : 8 * j + 8, :] = low_t[base + 8 * j : base + 8 * j + 8]
        u0 = high_t[base : base + 8]
        u1 = high_t[base + 8 : base + 16]
        u2 = high_t[base + 16 : base + 24]
        out_ref[d, 24:32, :] = jnp.where(where_at < 64, u0, pltpu.roll(u1, 64, 1))
        tail = jnp.where(where_at < 114, u0, jnp.where(where_at < 116, u1, u2))
        tail = jnp.where(where_at < 112, extra, tail)
        out_ref[d, 32:40, :] = jnp.where(where_at < 64, u2, tail)


def pack(flow, weight, depth8, extra):
    return pl.pallas_call(
        pack_kernel,
        grid=(8,),
        in_specs=[
            pl.BlockSpec((2, 48, LANES), lambda i: (0, 0, i)),
            pl.BlockSpec((2, 48, LANES), lambda i: (0, 0, i)),
            pl.BlockSpec((8, LANES), lambda i: (0, i)),
            pl.BlockSpec((8, 128), lambda i: (0, 0)),
        ],
        out_specs=pl.BlockSpec((16, 40, 128), lambda i: (i, 0, 0)),
        out_shape=jax.ShapeDtypeStruct((NDEV, 40, 128), F32),
        scratch_shapes=[pltpu.VMEM((128, LANES), F32), pltpu.VMEM((128, LANES), F32)],
        name="pack",
    )(flow, weight, depth8, extra)


def strip(tiles, lane, offset, width):
    out = []
    for t in range(3):
        acc = None
        for i in range(8):
            start = 48 * i + offset
            for wrap in (0, 384, 768):
                a = max(start - wrap, 128 * t) - 128 * t
                b = min(start + width - wrap, 128 * t + 128) - 128 * t
                if a < b:
                    if acc is None:
                        acc = tiles[i]
                    else:
                        acc = jnp.where((lane >= a) & (lane < b), tiles[i], acc)
        out.append(acc)
    return out


def shifted(tiles, lane, shift):
    whole, part = divmod(shift % 384, 128)
    if part == 0:
        return [tiles[(t - whole) % 3] for t in range(3)]
    rolled = [pltpu.roll(t, part, 1) for t in tiles]
    return [
        jnp.where(lane < part, rolled[(t - whole - 1) % 3], rolled[(t - whole) % 3])
        for t in range(3)
    ]


def split3(x):
    top = x.astype(BF16).astype(F32)
    rest = x - top
    mid = rest.astype(BF16).astype(F32)
    return jnp.concatenate([top, mid, rest - mid], 0).astype(BF16)


def join3(y):
    n = y.shape[0] // 3
    return y[:n] + y[n : 2 * n] + y[2 * n :]


def gathered(table, hot):
    return join3(jnp.dot(split3(table), hot, preferred_element_type=F32))


def summed(values, hot):
    return join3(
        lax.dot_general(
            split3(values), hot, (((1,), (1,)), ((), ())), preferred_element_type=F32
        )
    )


def unpack_group(g, recv, comps, extras, table):
    lane = lane_iota()
    block_lane = [(lane + 128 * t) % 48 for t in range(3)]
    srcs = [8 * g + i for i in range(8)]
    tile3 = [recv[s, 24:32, :] for s in srcs]
    tile4 = [recv[s, 32:40, :] for s in srcs]
    for j in range(3):
        low = [recv[s, 8 * j : 8 * j + 8, :] for s in srcs]
        high = (tile3, tile3, tile4)[j]
        at = (0, 64, 0)[j]
        first = shifted(strip(low, lane, 96, 32), lane, -96)
        second = shifted(strip(high, lane, at, 16), lane, 32 - at)
        parts = [
            strip(low, lane, 0, 48),
            shifted(strip(low, lane, 48, 48), lane, -48),
            [jnp.where(b < 32, f, s) for b, f, s in zip(block_lane, first, second)],
            shifted(strip(high, lane, at + 16, 48), lane, -16 - at),
        ]
        for c, tiles in enumerate(parts):
            for t in range(3):
                comps[g, 24 * c + 8 * j : 24 * c + 8 * j + 8, 128 * t : 128 * t + 128] = tiles[t]
    for t, tile in enumerate(shifted(strip(tile4, lane, 64, 48), lane, -64)):
        extras[g, :, 128 * t : 128 * t + 128] = tile
    for f in range(2):
        for j in range(4):
            offset = 112 + 2 * j + f if j < 3 else 64 + 24 * f
            acc = jnp.zeros((8, 128), F32)
            for i in range(8):
                moved = pltpu.roll(tile4[i], (i - 48 * i - offset) % 128, 1)
                acc = jnp.where(lane == i, moved, acc)
            acc = pltpu.roll(acc, 8 * g, 1)
            rows, cols = slice(8 * j, 8 * j + 8), slice(128 * f, 128 * f + 128)
            table[rows, cols] = jnp.where(lane // 8 == g, acc, table[rows, cols])


def pixel_xy(me, j):
    p = me * PX + 8 * j + lax.broadcasted_iota(jnp.int32, (8, 128), 0)
    x = ((p % 64).astype(F32) + 0.5) / 64 - 0.5
    y = ((p // 64).astype(F32) + 0.5 - 24.0) / 64
    return x, y


def first_pass(g, me, comps, extras, table, hot, geom, rel, both, sums):
    target = extras[g, 0:1, :]
    rows = lax.broadcasted_iota(jnp.int32, (256, LANES), 0).astype(F32)
    hot[g] = jnp.where(rows == target, 1.0, 0.0).astype(BF16)
    near = gathered(table[...], hot[g])
    rel[g] = extras[g] - near[24:32]
    for j in range(3):
        x, y = pixel_xy(me, j)
        for t in range(3):
            cols = slice(128 * t, 128 * t + 128)
            w0, w1, w2, m0, m1, m2 = [rel[g, 1 + k : 2 + k, cols] for k in range(6)]
            at = [slice(24 * c + 8 * j, 24 * c + 8 * j + 8) for c in range(4)]
            d = near[8 * j : 8 * j + 8, cols]
            x0 = x + w1 - w2 * y + m0 * d
            x1 = y + w2 * x - w0 + m1 * d
            x2 = 1.0 + w0 * y - w1 * x + m2 * d
            q = 1.0 / x2
            u = x0 * q
            v = x1 * q
            ru = comps[g, at[0], cols] - (u - x)
            rv = comps[g, at[1], cols] - (v - y)
            du = q * (m0 - u * m2)
            dv = q * (m1 - v * m2)
            eu = comps[g, at[2], cols] * du
            ev = comps[g, at[3], cols] * dv
            comps[g, at[0], cols] = ru
            comps[g, at[1], cols] = rv
            geom[g, at[0], cols] = d
            geom[g, at[1], cols] = q
            geom[g, at[2], cols] = u
            geom[g, at[3], cols] = v
            both[8 * j : 8 * j + 8, cols] = eu * ru + ev * rv
            both[24 + 8 * j : 32 + 8 * j, cols] = eu * du + ev * dv
    sums[...] += summed(both[...], hot[g])


def source_hot(g):
    rows = lax.broadcasted_iota(jnp.int32, (256, LANES), 0)
    lanes = lax.broadcasted_iota(jnp.int32, (256, LANES), 1)
    frame = lanes // 24
    col = (frame % 2) * 128 + 8 * g + frame // 2
    return jnp.where(rows == col, 1.0, 0.0).astype(BF16)


def second_pass(g, me, comps, geom, rel, hot, inverse, trio, rows_kh, total):
    near = gathered(inverse[...], hot[g])
    for t in range(3):
        cols = slice(128 * t, 128 * t + 128)
        acc = [None] * 27
        m0, m1, m2 = [rel[g, 4 + k : 5 + k, cols] for k in range(3)]

        def add(row, value):
            acc[row] = value if acc[row] is None else acc[row] + value

        for j in range(3):
            x, y = pixel_xy(me, j)
            at = [slice(24 * c + 8 * j, 24 * c + 8 * j + 8) for c in range(4)]
            d, q, u, v = [geom[g, at[c], cols] for c in range(4)]
            ru, rv, cu, cv = [comps[g, at[c], cols] for c in range(4)]
            ci = near[8 * j : 8 * j + 8, cols]
            gi = near[24 + 8 * j : 32 + 8 * j, cols]
            du = q * (m0 - u * m2)
            dv = q * (m1 - v * m2)
            eu = cu * du
            ev = cv * dv
            a1 = eu * q
            a2 = ev * q
            trio[g, at[0], cols] = a1
            trio[g, at[1], cols] = a2
            trio[g, at[2], cols] = a1 * u + a2 * v
            qq = q * q
            iu = ci * eu
            alpha = (cu - iu * eu) * qq
            gamma = (iu * ev) * qq
            beta = (cv - ci * ev * ev) * qq
            hu = (cu * ru - eu * gi) * q
            hv = (cv * rv - ev * gi) * q
            nd = -d
            ju = {0: -(u * y), 1: 1.0 + u * x, 2: -y, 5: u * nd}
            jv = {0: -1.0 - v * y, 1: v * x, 2: x, 5: v * nd}
            gd = gamma * d
            pp = {b: alpha * ju[b] - gamma * jv[b] for b in ju}
            qb = {b: beta * jv[b] - gamma * ju[b] for b in ju}
            pp[3], pp[4] = alpha * d, -gd
            qb[4] = beta * d
            for a, b in PAIRS:
                add(K_INDEX[a, b], ju[a] * pp[b] + jv[a] * qb[b])
            for b in range(6):
                add(K_INDEX[3, b], d * pp[b])
            for b in (0, 1, 2, 4, 5):
                add(K_INDEX[4, b], d * qb[b])
            for b in ju:
                add(H_ROW + b, ju[b] * hu + jv[b] * hv)
            add(H_ROW + 3, d * hu)
            add(H_ROW + 4, d * hv)
        for row in range(27):
            rows_kh[row : row + 1, cols] = jnp.sum(acc[row], axis=0, keepdims=True)
    src = source_hot(g)
    values = rows_kh[...]
    plus = summed(values, src + hot[g])
    minus = summed(values, src - hot[g])
    kind = lax.broadcasted_iota(jnp.int32, (32, 256), 0)
    total[...] += jnp.where(kind < H_ROW, plus, minus)


def third_pass(g, me, geom, trio, hot, steps, corr, fix):
    motion = gathered(steps[...], source_hot(g) - hot[g])
    for j in range(3):
        x, y = pixel_xy(me, j)
        for t in range(3):
            cols = slice(128 * t, 128 * t + 128)
            at = [slice(24 * c + 8 * j, 24 * c + 8 * j + 8) for c in range(3)]
            n0, n1, n2, n3, n4, n5 = [motion[k : k + 1, cols] for k in range(6)]
            d = geom[g, at[0], cols]
            a1, a2, a3 = [trio[g, at[c], cols] for c in range(3)]
            corr[8 * j : 8 * j + 8, cols] = (
                a1 * (n1 - y * n2 + d * n3)
                + a2 * (x * n2 - n0 + d * n4)
                - a3 * (y * n0 - x * n1 + d * n5)
            )
    fix[...] += summed(corr[...], hot[g])


def solve(matrix, right):
    factor = {}
    for i in range(6):
        for j in range(i + 1):
            e = matrix(i, j)
            if i == j:
                e = e * 1.1 + 0.001
            for k in range(j):
                e = e - factor[i, k] * factor[j, k]
            factor[i, j] = jnp.sqrt(e) if i == j else e / factor[j, j]
    forward = []
    for i in range(6):
        e = right(i)
        for k in range(i):
            e = e - factor[i, k] * forward[k]
        forward.append(e / factor[i, i])
    z = [None] * 6
    for i in reversed(range(6)):
        e = forward[i]
        for k in range(i + 1, 6):
            e = e - factor[k, i] * z[k]
        z[i] = e / factor[i, i]
    return z


def partner(k):
    row, col = lax.axis_index("row"), lax.axis_index("col")
    z = (row + k // 32) % 4
    y = (col // 8 + (k // 8) % 4) % 4
    x = ((col // 2) % 4 + (k // 2) % 4) % 4
    c = (col + k) % 2
    return z, y * 8 + x * 2 + c


def send_all(copy_to):
    def step(n, carry):
        copy_to(*partner((n * 37) % 128)).start()
        return carry

    lax.fori_loop(1, NDEV, step, 0)


def rows_exchange(send, recv, slot, send_sem, recv_sem):
    def copy_to(row, col):
        d = row * 32 + col
        return pltpu.make_async_remote_copy(
            src_ref=send.at[pl.ds(d, 1), :],
            dst_ref=recv.at[pl.ds(slot, 1), :],
            send_sem=send_sem,
            recv_sem=recv_sem,
            device_id=(row, col),
            device_id_type=MESH,
        )

    send_all(copy_to)


def rows_wait(buf, sem):
    ref = buf.at[pl.ds(0, NDEV - 1), :]
    pltpu.make_async_copy(ref, ref, sem).wait()


def main_kernel(
    packed, out_ref, pose_ref,
    recv, comps, extras, table, hot, geom, rel, both, sums, inverse, trio,
    rows_kh, total, steps, corr, fix,
    send_d, recv_d, send_e, recv_e, send_f, recv_f,
    big_send, big_recv, own_sem, small_send, small_recv,
):
    row, col = lax.axis_index("row"), lax.axis_index("col")
    me = row * 32 + col
    lane = lane_iota()

    def chunk_to(r, c):
        return pltpu.make_async_remote_copy(
            src_ref=packed.at[r * 32 + c],
            dst_ref=recv.at[me],
            send_sem=big_send,
            recv_sem=big_recv.at[me],
            device_id=(r, c),
            device_id_type=MESH,
        )

    own = pltpu.make_async_copy(packed.at[me], recv.at[me], big_recv.at[me])
    own.start()
    send_all(chunk_to)
    table[...] = jnp.zeros_like(table)
    sums[...] = jnp.zeros_like(sums)
    total[...] = jnp.zeros_like(total)
    fix[...] = jnp.zeros_like(fix)
    rows_kh[...] = jnp.zeros_like(rows_kh)

    def loop(body):
        def step(g, carry):
            body(g)
            return carry

        lax.fori_loop(0, GROUPS, step, 0)

    def arrive(g):
        for i in range(8):
            s = 8 * g + i
            pltpu.make_async_copy(packed.at[s], recv.at[s], big_recv.at[s]).wait()
        unpack_group(g, recv, comps, extras, table)

    loop(arrive)
    loop(lambda g: first_pass(g, me, comps, extras, table, hot, geom, rel, both, sums))
    ci = 1.0 / (0.1 + sums[24:48])
    inverse[0:24] = ci
    inverse[24:48] = sums[0:24] * ci
    loop(lambda g: second_pass(g, me, comps, geom, rel, hot, inverse, trio, rows_kh, total))

    send_d[...] = jnp.concatenate(
        [total[:, 0:128], total[:, 128:256], jnp.zeros((64, 128), F32)], 0
    ).T
    recv_d[pl.ds(me, 1), :] = send_d[pl.ds(me, 1), :]
    rows_exchange(send_d, recv_d, me, small_send.at[0], small_recv.at[0])
    rows_wait(recv_d, small_recv.at[0])
    line = jnp.sum(recv_d[...], axis=0, keepdims=True)
    sub = lax.broadcasted_iota(jnp.int32, (8, 128), 0)
    lines = jnp.broadcast_to(line, (8, 128))
    lines = jnp.where(sub == 1, pltpu.roll(lines, 96, 1), lines)
    full = jnp.concatenate([lines, jnp.zeros((120, 128), F32)], 0).T
    z = solve(
        lambda i, j: full[K_INDEX[i, j] : K_INDEX[i, j] + 1, :],
        lambda i: full[H_ROW + i : H_ROW + i + 1, :],
    )
    zs = jnp.concatenate([*z, jnp.zeros((122, 128), F32)], 0)
    pose_ref[...] = zs[0:6, 0:2]
    turned = zs.T
    mine = turned[0:1] + pltpu.roll(turned[0:8], 8, 1)[1:2]
    send_e[...] = jnp.broadcast_to(mine, (8, 128))
    recv_e[pl.ds(me, 1), :] = mine

    def step_to(r, c):
        return pltpu.make_async_remote_copy(
            src_ref=send_e.at[pl.ds(0, 1), :],
            dst_ref=recv_e.at[pl.ds(me, 1), :],
            send_sem=small_send.at[1],
            recv_sem=small_recv.at[1],
            device_id=(r, c),
            device_id_type=MESH,
        )

    send_all(step_to)
    rows_wait(recv_e, small_recv.at[1])
    every = recv_e[...].T
    steps[:, 0:128] = every[0:8]
    steps[:, 128:256] = every[8:16]
    loop(lambda g: third_pass(g, me, geom, trio, hot, steps, corr, fix))
    grad = sums[0:24]
    new = table[0:24] + (grad - fix[...]) * inverse[0:24]
    zero8 = jnp.zeros((8, 128), F32)
    send_f[...] = jnp.concatenate(
        [new[:, 0:128], zero8, new[:, 128:256], zero8, jnp.zeros((64, 128), F32)], 0
    ).T
    slot = (me % 16) * 8 + me // 16
    recv_f[pl.ds(slot, 1), :] = send_f[pl.ds(me, 1), :]
    rows_exchange(send_f, recv_f, slot, small_send.at[2], small_recv.at[2])
    rows_wait(recv_f, small_recv.at[2])
    for f in range(2):
        tiles = [None] * 3
        for i in range(16):
            piece = recv_f[8 * i : 8 * i + 8, :]
            first = 24 * i
            moved = pltpu.roll(piece, (first - 32 * f) % 128, 1)
            for t in range(3):
                a, b = max(first - 128 * t, 0), min(first + 24 - 128 * t, 128)
                if a < b:
                    if tiles[t] is None:
                        tiles[t] = moved
                    else:
                        tiles[t] = jnp.where((lane >= a) & (lane < b), moved, tiles[t])
        for g in range(8):
            for t in range(3):
                at = 384 * g + 128 * t
                out_ref[f : f + 1, at : at + 128] = tiles[t][g : g + 1]

    ref = packed.at[pl.ds(0, NDEV - 1)]
    pltpu.make_async_copy(ref, ref, big_send).wait()
    rows_wait(recv_d, small_send.at[0])
    rows_wait(recv_e, small_send.at[1])
    rows_wait(recv_f, small_send.at[2])


def run_main(packed):
    v = pltpu.VMEM
    return pl.pallas_call(
        main_kernel,
        in_specs=[pl.BlockSpec(memory_space=pl.ANY)],
        out_specs=[pl.BlockSpec(memory_space=pltpu.VMEM)] * 2,
        out_shape=[
            jax.ShapeDtypeStruct((2, PX * NDEV), F32),
            jax.ShapeDtypeStruct((6, 2), F32),
        ],
        scratch_shapes=[
            v((NDEV, 40, 128), F32),
            v((GROUPS, 96, LANES), F32),
            v((GROUPS, 8, LANES), F32),
            v((32, 256), F32),
            v((GROUPS, 256, LANES), BF16),
            v((GROUPS, 96, LANES), F32),
            v((GROUPS, 8, LANES), F32),
            v((48, LANES), F32),
            v((48, 256), F32),
            v((48, 256), F32),
            v((GROUPS, 72, LANES), F32),
            v((32, LANES), F32),
            v((32, 256), F32),
            v((8, 256), F32),
            v((24, LANES), F32),
            v((24, 256), F32),
            v((128, 128), F32),
            v((128, 128), F32),
            v((8, 128), F32),
            v((128, 128), F32),
            v((128, 128), F32),
            v((128, 128), F32),
            pltpu.SemaphoreType.DMA,
            pltpu.SemaphoreType.DMA((NDEV,)),
            pltpu.SemaphoreType.DMA,
            pltpu.SemaphoreType.DMA((3,)),
            pltpu.SemaphoreType.DMA((3,)),
        ],
        compiler_params=pltpu.CompilerParams(
            has_side_effects=True, vmem_limit_bytes=48 * 1024 * 1024
        ),
        name="step",
    )(packed)


def shards(inv_depth, rotation, translation, edge_target, flow_obs, weight):
    pixels = inv_depth.shape[1]
    flow = flow_obs.reshape(2, 48, pixels)
    wts = weight.reshape(2, 48, pixels)
    target = edge_target.reshape(1, 48)
    target = ((target % 2) * 128 + target // 2).astype(F32)
    pose = jnp.repeat(jnp.concatenate([rotation, translation], 0), 24, axis=1)
    extra = jnp.pad(jnp.concatenate([target, pose], 0), ((0, 1), (64, 16)))
    depth8 = jnp.tile(inv_depth, (4, 1))
    return run_main(pack(flow, wts, depth8, extra))


def solution(mesh):
    in_specs = (
        P(("row", "col"), None),
        P(None, ("row", "col")),
        P(None, ("row", "col")),
        P(("row", "col"), None),
        P(None, ("row", "col"), None, None),
        P(None, ("row", "col"), None, None),
    )
    out_specs = (P(("row", "col"), None), P(None, ("row", "col")))
    return jax.shard_map(
        shards, mesh=mesh, in_specs=in_specs, out_specs=out_specs, check_vma=False
    )
```

```python
import contextlib

import jax
import jax.numpy as jnp
from jax import lax
from jax.experimental import pallas as pl
from jax.experimental.pallas import tpu as pltpu
from jax.sharding import PartitionSpec as P

F32 = jnp.float32
BF16 = jnp.bfloat16
NDEV = 128
PX = 24
GROUPS = 16
LANES = 384
MESH = pl.DeviceIdType.MESH
PAIRS = [(a, b) for a in (0, 1, 2, 5) for b in (0, 1, 2, 5) if a <= b]
K_ROWS = [*PAIRS, *[(3, b) for b in range(6)], *[(4, b) for b in (0, 1, 2, 4, 5)]]
K_INDEX = {}
for _n, (_a, _b) in enumerate(K_ROWS):
    K_INDEX[_a, _b] = _n
    K_INDEX[_b, _a] = _n
H_ROW = 21


def lane_iota(shape=(8, 128)):
    return lax.broadcasted_iota(jnp.int32, shape, 1)


def pack_block(n, turn, flow, weight, depth, extra, low, high, out):
    cols = pl.ds(pl.multiple_of(n * LANES, 128), LANES)

    def put(ref, block, value):
        at = pl.multiple_of(((3 * turn + block) % 8) * 16, 16)
        ref[pl.ds(at, 16), :] = value

    for k in range(3):
        put(low, k, flow[0, 16 * k : 16 * k + 16, cols])
        put(low, 3 + k, flow[1, 16 * k : 16 * k + 16, cols])
        put(high, 1 + k, weight[1, 16 * k : 16 * k + 16, cols])
    put(low, 6, weight[0, 0:16, cols])
    put(low, 7, weight[0, 16:32, cols])
    put(high, 0, weight[0, 32:48, cols])
    low_t = low[...].T
    high_t = high[...].T
    where_at = (lane_iota() - 48 * turn + 384) % 128
    for d in range(16):
        base = 24 * d
        to = 16 * n + d
        for j in range(3):
            out[to, 8 * j : 8 * j + 8, :] = low_t[base + 8 * j : base + 8 * j + 8]
        u0 = high_t[base : base + 8]
        u1 = high_t[base + 8 : base + 16]
        u2 = high_t[base + 16 : base + 24]
        out[to, 24:32, :] = jnp.where(where_at < 64, u0, pltpu.roll(u1, 64, 1))
        out[to, 32:40, :] = jnp.where(where_at < 64, u2, extra)


def own_edges(target_ref, rotation_ref, translation_ref, ints, floats):
    lane = lane_iota()
    sub = lax.broadcasted_iota(jnp.int32, (8, 128), 0)
    ints[...] = jnp.zeros_like(ints)
    ints[0:2, 0:24] = target_ref[...]
    both = ints[...]
    target = jnp.where(lane < 24, both[0:1], pltpu.roll(both, 24, 1)[1:2])
    target = ((target % 2) * 128 + target // 2).astype(F32)
    floats[...] = jnp.zeros_like(floats)
    floats[0, 0:2, 0:3] = rotation_ref[...]
    floats[1, 0:2, 0:3] = translation_ref[...]
    pose = floats[0] + pltpu.roll(floats[1], 3, 1)
    column = jnp.concatenate([pose, jnp.zeros((120, 128), F32)], 0).T[0:8]
    spread = jnp.where(lane < 24, column[:, 0:1], column[:, 1:2])
    return jnp.where(sub == 6, target, spread), pose


def pack_tables(depth_ref, pose, unfold, send):
    lane = lane_iota()
    poses = pltpu.roll(pose, 48, 1)[0:1] + pltpu.roll(pose, 56, 1)[1:2]
    for f in range(2):
        for g in range(8):
            unfold[f, g : g + 1, :] = depth_ref[f : f + 1, LANES * g : LANES * g + LANES]
    for i in range(16):
        acc = jnp.broadcast_to(poses, (8, 128))
        for f in range(2):
            for t in range(3):
                a, b = max(24 * i - 128 * t, 0), min(24 * i + 24 - 128 * t, 128)
                if a < b:
                    shift = 24 * f - (24 * i - 128 * t)
                    moved = pltpu.roll(unfold[f, :, 128 * t : 128 * t + 128], shift % 128, 1)
                    acc = jnp.where((lane >= a + shift) & (lane < b + shift), moved, acc)
        send[8 * i : 8 * i + 8, :] = acc


def strip(tiles, lane, offset, width):
    out = []
    for t in range(3):
        acc = None
        for i in range(8):
            start = 48 * i + offset
            for wrap in (0, 384, 768):
                a = max(start - wrap, 128 * t) - 128 * t
                b = min(start + width - wrap, 128 * t + 128) - 128 * t
                if a < b:
                    if acc is None:
                        acc = tiles[i]
                    else:
                        acc = jnp.where((lane >= a) & (lane < b), tiles[i], acc)
        out.append(acc)
    return out


def shifted(tiles, lane, shift):
    whole, part = divmod(shift % 384, 128)
    if part == 0:
        return [tiles[(t - whole) % 3] for t in range(3)]
    rolled = [pltpu.roll(t, part, 1) for t in tiles]
    return [
        jnp.where(lane < part, rolled[(t - whole - 1) % 3], rolled[(t - whole) % 3])
        for t in range(3)
    ]


def split3(x):
    top = x.astype(BF16).astype(F32)
    rest = x - top
    mid = rest.astype(BF16).astype(F32)
    return jnp.concatenate([top, mid, rest - mid], 0).astype(BF16)


def join3(y):
    n = y.shape[0] // 3
    return y[:n] + y[n : 2 * n] + y[2 * n :]


def gathered(table, hot):
    return join3(jnp.dot(split3(table), hot, preferred_element_type=F32))


def summed(values, hot):
    return join3(
        lax.dot_general(
            split3(values), hot, (((1,), (1,)), ((), ())), preferred_element_type=F32
        )
    )


def unpack_group(g, recv, comps, extras):
    lane = lane_iota()
    block_lane = [(lane + 128 * t) % 48 for t in range(3)]
    srcs = [8 * g + i for i in range(8)]
    tile3 = [recv[s, 24:32, :] for s in srcs]
    tile4 = [recv[s, 32:40, :] for s in srcs]
    for j in range(3):
        low = [recv[s, 8 * j : 8 * j + 8, :] for s in srcs]
        high = (tile3, tile3, tile4)[j]
        at = (0, 64, 0)[j]
        first = shifted(strip(low, lane, 96, 32), lane, -96)
        second = shifted(strip(high, lane, at, 16), lane, 32 - at)
        parts = [
            strip(low, lane, 0, 48),
            shifted(strip(low, lane, 48, 48), lane, -48),
            [jnp.where(b < 32, f, s) for b, f, s in zip(block_lane, first, second)],
            shifted(strip(high, lane, at + 16, 48), lane, -16 - at),
        ]
        for c, tiles in enumerate(parts):
            for t in range(3):
                comps[g, 24 * c + 8 * j : 24 * c + 8 * j + 8, 128 * t : 128 * t + 128] = tiles[t]
    for t, tile in enumerate(shifted(strip(tile4, lane, 64, 48), lane, -64)):
        extras[g, :, 128 * t : 128 * t + 128] = tile


def pixel_xy(me, j):
    p = me * PX + 8 * j + lax.broadcasted_iota(jnp.int32, (8, 128), 0)
    x = ((p % 64).astype(F32) + 0.5) / 64 - 0.5
    y = ((p // 64).astype(F32) + 0.5 - 24.0) / 64
    return x, y


def first_pass(g, me, comps, extras, table, hot, geom, rel, both, sums):
    target = extras[g, 6:7, :]
    rows = lax.broadcasted_iota(jnp.int32, (256, LANES), 0).astype(F32)
    hot[g] = jnp.where(rows == target, 1.0, 0.0).astype(BF16)
    near = gathered(table[...], hot[g])
    rel[g] = extras[g] - near[24:32]
    for j in range(3):
        x, y = pixel_xy(me, j)
        for t in range(3):
            cols = slice(128 * t, 128 * t + 128)
            w0, w1, w2, m0, m1, m2 = [rel[g, k : 1 + k, cols] for k in range(6)]
            at = [slice(24 * c + 8 * j, 24 * c + 8 * j + 8) for c in range(4)]
            d = near[8 * j : 8 * j + 8, cols]
            x0 = x + w1 - w2 * y + m0 * d
            x1 = y + w2 * x - w0 + m1 * d
            x2 = 1.0 + w0 * y - w1 * x + m2 * d
            q = 1.0 / x2
            u = x0 * q
            v = x1 * q
            ru = comps[g, at[0], cols] - (u - x)
            rv = comps[g, at[1], cols] - (v - y)
            du = q * (m0 - u * m2)
            dv = q * (m1 - v * m2)
            eu = comps[g, at[2], cols] * du
            ev = comps[g, at[3], cols] * dv
            comps[g, at[0], cols] = ru
            comps[g, at[1], cols] = rv
            geom[g, at[0], cols] = d
            geom[g, at[1], cols] = q
            geom[g, at[2], cols] = u
            geom[g, at[3], cols] = v
            both[8 * j : 8 * j + 8, cols] = eu * ru + ev * rv
            both[24 + 8 * j : 32 + 8 * j, cols] = eu * du + ev * dv
    sums[...] += summed(both[...], hot[g])


def source_columns():
    rows = lax.broadcasted_iota(jnp.int32, (128, LANES), 0)
    frame = lax.broadcasted_iota(jnp.int32, (1, LANES), 1) // 24
    return jnp.where(rows == (frame % 2) * 8 + frame // 2, 1.0, 0.0).astype(BF16)


def second_pass(g, me, comps, geom, rel, hot, own, inverse, trio, rows_kh, total_s, total_t):
    near = gathered(inverse[...], hot[g])
    for t in range(3):
        cols = slice(128 * t, 128 * t + 128)
        acc = [None] * 27
        m0, m1, m2 = [rel[g, 3 + k : 4 + k, cols] for k in range(3)]

        def add(row, value):
            acc[row] = value if acc[row] is None else acc[row] + value

        for j in range(3):
            x, y = pixel_xy(me, j)
            at = [slice(24 * c + 8 * j, 24 * c + 8 * j + 8) for c in range(4)]
            d, q, u, v = [geom[g, at[c], cols] for c in range(4)]
            ru, rv, cu, cv = [comps[g, at[c], cols] for c in range(4)]
            ci = near[8 * j : 8 * j + 8, cols]
            gi = near[24 + 8 * j : 32 + 8 * j, cols]
            du = q * (m0 - u * m2)
            dv = q * (m1 - v * m2)
            eu = cu * du
            ev = cv * dv
            a1 = eu * q
            a2 = ev * q
            trio[g, at[0], cols] = a1
            trio[g, at[1], cols] = a2
            trio[g, at[2], cols] = a1 * u + a2 * v
            qq = q * q
            iu = ci * eu
            alpha = (cu - iu * eu) * qq
            gamma = (iu * ev) * qq
            beta = (cv - ci * ev * ev) * qq
            hu = (cu * ru - eu * gi) * q
            hv = (cv * rv - ev * gi) * q
            nd = -d
            ju = {0: -(u * y), 1: 1.0 + u * x, 2: -y, 5: u * nd}
            jv = {0: -1.0 - v * y, 1: v * x, 2: x, 5: v * nd}
            gd = gamma * d
            pp = {b: alpha * ju[b] - gamma * jv[b] for b in ju}
            qb = {b: beta * jv[b] - gamma * ju[b] for b in ju}
            pp[3], pp[4] = alpha * d, -gd
            qb[4] = beta * d
            for a, b in PAIRS:
                add(K_INDEX[a, b], ju[a] * pp[b] + jv[a] * qb[b])
            for b in range(6):
                add(K_INDEX[3, b], d * pp[b])
            for b in (0, 1, 2, 4, 5):
                add(K_INDEX[4, b], d * qb[b])
            for b in ju:
                add(H_ROW + b, ju[b] * hu + jv[b] * hv)
            add(H_ROW + 3, d * hu)
            add(H_ROW + 4, d * hv)
        for row in range(27):
            rows_kh[row : row + 1, cols] = jnp.sum(acc[row], axis=0, keepdims=True)
    values = rows_kh[...]
    total_t[...] += summed(values, hot[g])
    by_source = summed(values, own[...])
    lane = lane_iota((32, 128))
    for f in range(2):
        at = slice(128 * f, 128 * f + 128)
        moved = pltpu.roll(by_source, (8 * g - 8 * f + 128) % 128, 1)
        total_s[:, at] = jnp.where(lane // 8 == g, moved, total_s[:, at])


def third_pass(g, me, geom, trio, hot, own, steps, corr, fix):
    lane = lane_iota()
    mine = jnp.where(
        lane < 8,
        pltpu.roll(steps[:, 0:128], (128 - 8 * g) % 128, 1),
        pltpu.roll(steps[:, 128:256], (136 - 8 * g) % 128, 1),
    )
    motion = gathered(mine, own[...]) - gathered(steps[...], hot[g])
    for j in range(3):
        x, y = pixel_xy(me, j)
        for t in range(3):
            cols = slice(128 * t, 128 * t + 128)
            at = [slice(24 * c + 8 * j, 24 * c + 8 * j + 8) for c in range(3)]
            n0, n1, n2, n3, n4, n5 = [motion[k : k + 1, cols] for k in range(6)]
            d = geom[g, at[0], cols]
            a1, a2, a3 = [trio[g, at[c], cols] for c in range(3)]
            corr[8 * j : 8 * j + 8, cols] = (
                a1 * (n1 - y * n2 + d * n3)
                + a2 * (x * n2 - n0 + d * n4)
                - a3 * (y * n0 - x * n1 + d * n5)
            )
    fix[...] += summed(corr[...], hot[g])


def solve(matrix, right):
    factor = {}
    for i in range(6):
        for j in range(i + 1):
            e = matrix(i, j)
            if i == j:
                e = e * 1.1 + 0.001
            for k in range(j):
                e = e - factor[i, k] * factor[j, k]
            factor[i, j] = jnp.sqrt(e) if i == j else e / factor[j, j]
    forward = []
    for i in range(6):
        e = right(i)
        for k in range(i):
            e = e - factor[i, k] * forward[k]
        forward.append(e / factor[i, i])
    z = [None] * 6
    for i in reversed(range(6)):
        e = forward[i]
        for k in range(i + 1, 6):
            e = e - factor[k, i] * z[k]
        z[i] = e / factor[i, i]
    return z


def ring_steps(d):
    return min(d, 4 - d)


def far_first():
    offsets = [
        (dz, dy, dx, dc)
        for dz in range(4)
        for dy in range(4)
        for dx in range(4)
        for dc in range(2)
        if (dz, dy, dx, dc) != (0, 0, 0, 0)
    ]
    return sorted(offsets, key=lambda o: -(ring_steps(o[0]) + ring_steps(o[1]) + ring_steps(o[2])))


def group_offset(n):
    return (n // 4 + n) % 4, n % 4


def by_group():
    return [
        (*group_offset(n), dx, dc)
        for n in range(GROUPS)
        for dx in range(4)
        for dc in range(2)
        if (n, dx, dc) != (0, 0, 0)
    ]


def to_all(order, act):
    row, col = lax.axis_index("row"), lax.axis_index("col")
    zs = [((row + d) % 4) * 32 for d in range(4)]
    ys = [((col // 8 + d) % 4) * 8 for d in range(4)]
    xs = [((col // 2 + d) % 4) * 2 for d in range(4)]
    cs = [(col + d) % 2 for d in range(2)]
    for dz, dy, dx, dc in order:
        act(zs[dz] + ys[dy] + xs[dx] + cs[dc])


def slot_of(d):
    return (d % 16) * 8 + d // 16


def rows_exchange(send, recv, source, slot, send_sem, recv_sem):
    def act(d):
        pltpu.make_async_remote_copy(
            src_ref=send.at[pl.ds(source(d), 1), :],
            dst_ref=recv.at[pl.ds(slot, 1), :],
            send_sem=send_sem,
            recv_sem=recv_sem,
            device_id=d,
            device_id_type=pl.DeviceIdType.LOGICAL,
        ).start()

    to_all(far_first(), act)


def rows_wait(buf, sem):
    ref = buf.at[pl.ds(0, NDEV - 1), :]
    pltpu.make_async_copy(ref, ref, sem).wait()


def scope(name):
    return contextlib.nullcontext()


def loop(body):
    def step(g, carry):
        body(g)
        return carry

    lax.fori_loop(0, GROUPS, step, 0)


def main_kernel(
    flow_hbm, weight_hbm, depth_ref, target_ref, rotation_ref, translation_ref,
    out_ref, pose_ref,
    flow, weight, low, high, chunks, ints, floats, unfold,
    recv, comps, extras, table, hot, own, geom, rel, both, sums, inverse, trio,
    rows_kh, total_s, total_t, steps, corr, fix,
    send_t, recv_t, send_d, recv_d, send_e, recv_e, send_f, recv_f,
    in_sem, own_sem, big_send, big_recv, small_send, small_recv,
):
    row, col = lax.axis_index("row"), lax.axis_index("col")
    me = row * 32 + col
    lane = lane_iota()
    barrier = pltpu.get_barrier_semaphore()

    loads = [
        pltpu.make_async_copy(flow_hbm, flow, in_sem.at[0]),
        pltpu.make_async_copy(weight_hbm, weight, in_sem.at[1]),
    ]
    for load in loads:
        load.start()

    def greet(d):
        pl.semaphore_signal(
            barrier, inc=1, device_id=d, device_id_type=pl.DeviceIdType.LOGICAL
        )

    with scope("sc_greet"):
        to_all(far_first(), greet)

    with scope("sc_tables"):
        table[...] = jnp.zeros_like(table)
        sums[...] = jnp.zeros_like(sums)
        total_t[...] = jnp.zeros_like(total_t)
        total_s[...] = jnp.zeros_like(total_s)
        fix[...] = jnp.zeros_like(fix)
        rows_kh[...] = jnp.zeros_like(rows_kh)
        own[...] = source_columns()
        high[...] = jnp.zeros_like(high)
        extra, pose = own_edges(target_ref, rotation_ref, translation_ref, ints, floats)
        pack_tables(depth_ref, pose, unfold, send_t)
        recv_t[pl.ds(me, 1), :] = send_t[pl.ds(slot_of(me), 1), :]
        turn = col % 8
        extra = pltpu.roll(extra, (64 + 48 * turn) % 128, 1)
        for load in loads:
            load.wait()

    def pack(n, carry):
        pack_block(n, turn, flow, weight, depth_ref, extra, low, high, chunks)
        return carry

    with scope("sc_pack"):
        lax.fori_loop(0, 8, pack, 0)
    with scope("sc_barrier"):
        pl.semaphore_wait(barrier, NDEV - 1)

    with scope("sc_sends"):
        rows_exchange(send_t, recv_t, slot_of, me, small_send.at[3], small_recv.at[3])

        def send_chunk(d):
            pltpu.make_async_remote_copy(
                src_ref=chunks.at[d],
                dst_ref=recv.at[me],
                send_sem=big_send,
                recv_sem=big_recv.at[me],
                device_id=d,
                device_id_type=pl.DeviceIdType.LOGICAL,
            ).start()

        to_all(by_group(), send_chunk)
        recv[me] = chunks[me]

    with scope("sc_waitt"):
        rows_wait(recv_t, small_recv.at[3])
        known = recv_t[...].T
        for f in range(2):
            at = slice(128 * f, 128 * f + 128)
            table[0:24, at] = known[24 * f : 24 * f + 24]
            table[24:32, at] = known[48 + 8 * f : 56 + 8 * f]

    def arrive(n):
        dz, dy = group_offset(n)
        g = ((row + 4 - dz) % 4) * 4 + (col // 8 + 4 - dy) % 4
        for i in range(8):
            s = 8 * g + i

            @pl.when(s != me)
            def _():
                pltpu.make_async_copy(chunks.at[s], recv.at[s], big_recv.at[s]).wait()

        unpack_group(g, recv, comps, extras)
        first_pass(g, me, comps, extras, table, hot, geom, rel, both, sums)

    with scope("sc_arrive"):
        loop(arrive)
    with scope("sc_second"):
        ci = 1.0 / (0.1 + sums[24:48])
        inverse[0:24] = ci
        inverse[24:48] = sums[0:24] * ci
        loop(
            lambda g: second_pass(
                g, me, comps, geom, rel, hot, own, inverse, trio, rows_kh, total_s, total_t
            )
        )

    with scope("sc_sendd"):
        kind = lax.broadcasted_iota(jnp.int32, (32, 256), 0)
        total = total_s[...] + jnp.where(kind < H_ROW, total_t[...], -total_t[...])
        send_d[...] = jnp.concatenate(
            [total[:, 0:128], total[:, 128:256], jnp.zeros((64, 128), F32)], 0
        ).T
        recv_d[pl.ds(me, 1), :] = send_d[pl.ds(me, 1), :]
        rows_exchange(send_d, recv_d, lambda d: d, me, small_send.at[0], small_recv.at[0])
    with scope("sc_waitd"):
        rows_wait(recv_d, small_recv.at[0])
    with scope("sc_solve"):
        line = jnp.sum(recv_d[...], axis=0, keepdims=True)
        sub = lax.broadcasted_iota(jnp.int32, (8, 128), 0)
        lines = jnp.broadcast_to(line, (8, 128))
        lines = jnp.where(sub == 1, pltpu.roll(lines, 96, 1), lines)
        full = jnp.concatenate([lines, jnp.zeros((120, 128), F32)], 0).T
        z = solve(
            lambda i, j: full[K_INDEX[i, j] : K_INDEX[i, j] + 1, :],
            lambda i: full[H_ROW + i : H_ROW + i + 1, :],
        )
        zs = jnp.concatenate([*z, jnp.zeros((122, 128), F32)], 0)
        turned = zs.T
        pose_ref[...] = turned[0:2, 0:6]
        mine = turned[0:1] + pltpu.roll(turned[0:8], 8, 1)[1:2]
        send_e[...] = jnp.broadcast_to(mine, (8, 128))
        recv_e[pl.ds(me, 1), :] = mine
    with scope("sc_sende"):
        rows_exchange(send_e, recv_e, lambda d: 0, me, small_send.at[1], small_recv.at[1])
    with scope("sc_waite"):
        rows_wait(recv_e, small_recv.at[1])
    with scope("sc_third"):
        every = recv_e[...].T
        steps[:, 0:128] = every[0:8]
        steps[:, 128:256] = every[8:16]
        loop(lambda g: third_pass(g, me, geom, trio, hot, own, steps, corr, fix))
    with scope("sc_sendf"):
        grad = sums[0:24]
        new = table[0:24] + (grad - fix[...]) * inverse[0:24]
        zero8 = jnp.zeros((8, 128), F32)
        send_f[...] = jnp.concatenate(
            [new[:, 0:128], zero8, new[:, 128:256], zero8, jnp.zeros((64, 128), F32)], 0
        ).T
        slot = slot_of(me)
        recv_f[pl.ds(slot, 1), :] = send_f[pl.ds(me, 1), :]
        rows_exchange(send_f, recv_f, lambda d: d, slot, small_send.at[2], small_recv.at[2])
    with scope("sc_waitf"):
        rows_wait(recv_f, small_recv.at[2])
    for f in range(2):
        tiles = [None] * 3
        for i in range(16):
            piece = recv_f[8 * i : 8 * i + 8, :]
            first = 24 * i
            moved = pltpu.roll(piece, (first - 32 * f) % 128, 1)
            for t in range(3):
                a, b = max(first - 128 * t, 0), min(first + 24 - 128 * t, 128)
                if a < b:
                    if tiles[t] is None:
                        tiles[t] = moved
                    else:
                        tiles[t] = jnp.where((lane >= a) & (lane < b), moved, tiles[t])
        for g in range(8):
            for t in range(3):
                at = 384 * g + 128 * t
                out_ref[f : f + 1, at : at + 128] = tiles[t][g : g + 1]

    ref = chunks.at[pl.ds(0, NDEV - 1)]
    pltpu.make_async_copy(ref, ref, big_send).wait()
    rows_wait(recv_t, small_send.at[3])
    rows_wait(recv_d, small_send.at[0])
    rows_wait(recv_e, small_send.at[1])
    rows_wait(recv_f, small_send.at[2])


def run_main(flow, weight, inv_depth, edge_target, rotation, translation):
    v = pltpu.VMEM
    vmem = pl.BlockSpec(memory_space=pltpu.VMEM)
    hbm = pl.BlockSpec(memory_space=pl.ANY)
    return pl.pallas_call(
        main_kernel,
        in_specs=[hbm, hbm, vmem, vmem, vmem, vmem],
        out_specs=[vmem] * 2,
        out_shape=[
            jax.ShapeDtypeStruct((2, PX * NDEV), F32),
            jax.ShapeDtypeStruct((2, 6), F32),
        ],
        scratch_shapes=[
            v((2, 48, PX * NDEV), F32),
            v((2, 48, PX * NDEV), F32),
            v((128, LANES), F32),
            v((128, LANES), F32),
            v((NDEV, 40, 128), F32),
            v((8, 128), jnp.int32),
            v((2, 8, 128), F32),
            v((2, 8, LANES), F32),
            v((NDEV, 40, 128), F32),
            v((GROUPS, 96, LANES), F32),
            v((GROUPS, 8, LANES), F32),
            v((32, 256), F32),
            v((GROUPS, 256, LANES), BF16),
            v((128, LANES), BF16),
            v((GROUPS, 96, LANES), F32),
            v((GROUPS, 8, LANES), F32),
            v((48, LANES), F32),
            v((48, 256), F32),
            v((48, 256), F32),
            v((GROUPS, 72, LANES), F32),
            v((32, LANES), F32),
            v((32, 256), F32),
            v((32, 256), F32),
            v((8, 256), F32),
            v((24, LANES), F32),
            v((24, 256), F32),
            v((128, 128), F32),
            v((128, 128), F32),
            v((128, 128), F32),
            v((128, 128), F32),
            v((8, 128), F32),
            v((128, 128), F32),
            v((128, 128), F32),
            v((128, 128), F32),
            pltpu.SemaphoreType.DMA((2,)),
            pltpu.SemaphoreType.DMA,
            pltpu.SemaphoreType.DMA,
            pltpu.SemaphoreType.DMA((NDEV,)),
            pltpu.SemaphoreType.DMA((4,)),
            pltpu.SemaphoreType.DMA((4,)),
        ],
        compiler_params=pltpu.CompilerParams(
            collective_id=0, has_side_effects=True, vmem_limit_bytes=56 * 1024 * 1024
        ),
        name="step",
    )(flow, weight, inv_depth, edge_target, rotation, translation)


def shards(inv_depth, rotation, translation, edge_target, flow_obs, weight):
    pixels = inv_depth.shape[1]
    flow = flow_obs.reshape(2, 48, pixels)
    wts = weight.reshape(2, 48, pixels)
    depth, pose = run_main(flow, wts, inv_depth, edge_target, rotation.T, translation.T)
    return depth, pose.T


def solution(mesh):
    in_specs = (
        P(("row", "col"), None),
        P(None, ("row", "col")),
        P(None, ("row", "col")),
        P(("row", "col"), None),
        P(None, ("row", "col"), None, None),
        P(None, ("row", "col"), None, None),
    )
    out_specs = (P(("row", "col"), None), P(None, ("row", "col")))
    return jax.shard_map(
        shards, mesh=mesh, in_specs=in_specs, out_specs=out_specs, check_vma=False
    )
```

```python
import contextlib

import jax
import jax.numpy as jnp
from jax import lax
from jax.experimental import pallas as pl
from jax.experimental.pallas import tpu as pltpu
from jax.sharding import PartitionSpec as P

F32 = jnp.float32
BF16 = jnp.bfloat16
NDEV = 128
PX = 24
GROUPS = 16
LANES = 384
MESH = pl.DeviceIdType.MESH
K_PAIRS = [((a, b), n) for n, (a, b) in enumerate((a, b) for a in range(6) for b in range(a, 6))]
K_INDEX = {**dict(K_PAIRS), **{(b, a): n for (a, b), n in K_PAIRS}}
H_ROW = 21


def lane_iota(shape=(8, 128)):
    return lax.broadcasted_iota(jnp.int32, shape, 1)


def pack_block(n, turn, flow, weight, low, high, out):
    cols = pl.ds(pl.multiple_of(n * LANES, 128), LANES)

    def put(ref, block, value):
        at = pl.multiple_of(((3 * turn + block) % 8) * 16, 16)
        ref[pl.ds(at, 16), :] = value

    for k in range(3):
        put(low, k, flow[0, 16 * k : 16 * k + 16, cols])
        put(low, 3 + k, flow[1, 16 * k : 16 * k + 16, cols])
        put(high, 1 + k, weight[1, 16 * k : 16 * k + 16, cols])
    put(low, 6, weight[0, 0:16, cols])
    put(low, 7, weight[0, 16:32, cols])
    put(high, 0, weight[0, 32:48, cols])
    low_t = low[...].T
    high_t = high[...].T
    where_at = (lane_iota() - 48 * turn + 384) % 128
    for d in range(16):
        base = 24 * d
        to = 16 * n + d
        for j in range(3):
            out[to, 8 * j : 8 * j + 8, :] = low_t[base + 8 * j : base + 8 * j + 8]
        u0 = high_t[base : base + 8]
        u1 = high_t[base + 8 : base + 16]
        u2 = high_t[base + 16 : base + 24]
        out[to, 24:32, :] = jnp.where(where_at < 64, u0, pltpu.roll(u1, 64, 1))
        last = jnp.where(where_at < 64, u2, pltpu.roll(pltpu.roll(u2, 64, 1), 4, 0))
        out[to, 32:36, :] = last[0:4]


def own_edges(target_ref, rotation_ref, translation_ref, ints, floats):
    lane = lane_iota()
    ints[...] = jnp.zeros_like(ints)
    ints[0:2, 0:24] = target_ref[...]
    both = ints[...]
    target = jnp.where(lane < 24, both[0:1], pltpu.roll(both, 24, 1)[1:2])
    x, y, z = (target >> 2) & 3, (target >> 4) & 3, target >> 6
    group = (((z - x) & 3) << 2) + ((y - x) & 3)
    column = ((target & 1) << 7) + (group << 3) + ((target >> 1) & 7)
    floats[...] = jnp.zeros_like(floats)
    floats[0, 0:2, 0:3] = rotation_ref[...]
    floats[1, 0:2, 0:3] = translation_ref[...]
    return column.astype(F32), floats[0] + pltpu.roll(floats[1], 3, 1)


def pack_tables(depth_ref, column, pose, unfold, send):
    lane = lane_iota()
    poses = pltpu.roll(pose, 48, 1)[0:1] + pltpu.roll(pose, 56, 1)[1:2]
    known = jnp.where(lane < 64, poses, pltpu.roll(column, 64, 1)[0:1])
    for f in range(2):
        for g in range(8):
            unfold[f, g : g + 1, :] = depth_ref[f : f + 1, LANES * g : LANES * g + LANES]
    for i in range(16):
        acc = known
        for f in range(2):
            for t in range(3):
                a, b = max(24 * i - 128 * t, 0), min(24 * i + 24 - 128 * t, 128)
                if a < b:
                    shift = 24 * f - (24 * i - 128 * t)
                    moved = pltpu.roll(unfold[f, :, 128 * t : 128 * t + 128], shift % 128, 1)
                    acc = jnp.where((lane >= a + shift) & (lane < b + shift), moved, acc)
        send[8 * i : 8 * i + 8, :] = acc


def strip(tiles, lane, offset, width):
    out = []
    for t in range(3):
        acc = None
        for i in range(8):
            start = 48 * i + offset
            for wrap in (0, 384, 768):
                a = max(start - wrap, 128 * t) - 128 * t
                b = min(start + width - wrap, 128 * t + 128) - 128 * t
                if a < b:
                    if acc is None:
                        acc = tiles[i]
                    else:
                        acc = jnp.where((lane >= a) & (lane < b), tiles[i], acc)
        out.append(acc)
    return out


def shifted(tiles, lane, shift):
    whole, part = divmod(shift % 384, 128)
    if part == 0:
        return [tiles[(t - whole) % 3] for t in range(3)]
    rolled = [pltpu.roll(t, part, 1) for t in tiles]
    return [
        jnp.where(lane < part, rolled[(t - whole - 1) % 3], rolled[(t - whole) % 3])
        for t in range(3)
    ]


def split3(x):
    top = x.astype(BF16).astype(F32)
    rest = x - top
    mid = rest.astype(BF16).astype(F32)
    return jnp.concatenate([top, mid, rest - mid], 0).astype(BF16)


def join3(y):
    n = y.shape[0] // 3
    return y[:n] + y[n : 2 * n] + y[2 * n :]


def gathered(table, hot):
    return join3(jnp.dot(split3(table), hot, preferred_element_type=F32))


def summed(values, hot):
    return join3(
        lax.dot_general(
            split3(values), hot, (((1,), (1,)), ((), ())), preferred_element_type=F32
        )
    )


def unpack_group(g, recv, comps):
    lane = lane_iota()
    upper = lax.broadcasted_iota(jnp.int32, (8, 128), 0) >= 4
    block_lane = [(lane + 128 * t) % 48 for t in range(3)]
    srcs = [8 * g + i for i in range(8)]
    tile3 = [recv[s, 24:32, :] for s in srcs]
    tile4 = [recv[s, 32:40, :] for s in srcs]

    def piece(j, offset, width, to):
        def at(tiles, start):
            return shifted(strip(tiles, lane, start, width), lane, to - start)

        if j < 2:
            return at(tile3, offset + 64 * j)
        first, second = at(tile4, offset), at(tile4, offset + 64)
        return [jnp.where(upper, pltpu.roll(b, 4, 0), a) for a, b in zip(first, second)]

    for j in range(3):
        low = [recv[s, 8 * j : 8 * j + 8, :] for s in srcs]
        first = shifted(strip(low, lane, 96, 32), lane, -96)
        second = piece(j, 0, 16, 32)
        parts = [
            strip(low, lane, 0, 48),
            shifted(strip(low, lane, 48, 48), lane, -48),
            [jnp.where(b < 32, f, s) for b, f, s in zip(block_lane, first, second)],
            piece(j, 16, 48, 0),
        ]
        for c, tiles in enumerate(parts):
            for t in range(3):
                comps[24 * c + 8 * j : 24 * c + 8 * j + 8, 128 * t : 128 * t + 128] = tiles[t]


def group_targets(g, recv_t):
    lane = lane_iota()
    sub = lax.broadcasted_iota(jnp.int32, (8, 128), 0)
    tile = recv_t[pl.ds(pl.multiple_of(8 * g, 8), 8), :]
    out = [jnp.zeros((8, 128), F32)] * 3
    for i in range(8):
        moved = pltpu.roll(tile, (48 * i - 64) % 128, 1)
        for t in range(3):
            a, b = max(48 * i - 128 * t, 0), min(48 * i + 48 - 128 * t, 128)
            if a < b:
                out[t] = jnp.where((sub == i) & (lane >= a) & (lane < b), moved, out[t])
    return jnp.concatenate([jnp.sum(x, axis=0, keepdims=True) for x in out], 1)


def merge(items):
    sub = lax.broadcasted_iota(jnp.int32, (8, 128), 0)
    items = items[::-1]
    for bit in (0, 1, 2):
        step = 1 << bit
        here = (sub & step) != 0
        items = [
            jnp.where(here, a, b) + pltpu.roll(jnp.where(here, b, a), step, 0)
            for a, b in zip(items[0::2], items[1::2])
        ]
    return items[0]


def merged_rows(rows):
    rows = rows + [jnp.zeros((8, 128), F32)] * (32 - len(rows))
    return jnp.concatenate([merge(rows[k : k + 8]) for k in range(0, 32, 8)], 0)


def pixel_xy(me, j):
    p = me * PX + 8 * j + lax.broadcasted_iota(jnp.int32, (8, 128), 0)
    x = ((p % 64).astype(F32) + 0.5) / 64 - 0.5
    y = ((p // 64).astype(F32) + 0.5 - 24.0) / 64
    return x, y


def expanded(rows, g, own):
    lane = lane_iota()
    mine = jnp.where(
        lane < 8,
        pltpu.roll(rows[:, 0:128], (128 - 8 * g) % 128, 1),
        pltpu.roll(rows[:, 128:256], (136 - 8 * g) % 128, 1),
    )
    return gathered(mine, own[...])


def add_up(values, g, hot, own, total_s, total_t):
    total_t[...] += summed(values, hot[g])
    by_source = summed(values, own[...])
    lane = lane_iota((32, 128))
    for f in range(2):
        at = slice(128 * f, 128 * f + 128)
        moved = pltpu.roll(by_source, (8 * g - 8 * f + 128) % 128, 1)
        total_s[:, at] += jnp.where(lane // 8 == g, moved, 0.0)


def first_pass(g, me, comps, recv_t, table, hot, own, coup, sums, total_s, total_t):
    rows = lax.broadcasted_iota(jnp.int32, (256, LANES), 0).astype(F32)
    hot[g] = jnp.where(rows == group_targets(g, recv_t), 1.0, 0.0).astype(BF16)
    near = gathered(table[...], hot[g])
    rel = expanded(table[24:32, :], g, own) - near[24:32]
    grads, curvs, blocks = [], [], []
    for t in range(3):
        cols = slice(128 * t, 128 * t + 128)
        w0, w1, w2, m0, m1, m2 = [rel[k : 1 + k, cols] for k in range(6)]
        acc = [None] * 27
        gs, cs = [], []

        def add(row, value):
            acc[row] = value if acc[row] is None else acc[row] + value

        for j in range(3):
            x, y = pixel_xy(me, j)
            fu, fv, cu, cv = [comps[24 * c + 8 * j : 24 * c + 8 * j + 8, cols] for c in range(4)]
            d = near[8 * j : 8 * j + 8, cols]
            x0 = x + w1 - w2 * y + m0 * d
            x1 = y + w2 * x - w0 + m1 * d
            x2 = 1.0 + w0 * y - w1 * x + m2 * d
            q = 1.0 / x2
            u = x0 * q
            v = x1 * q
            ru = fu - (u - x)
            rv = fv - (v - y)
            du = q * (m0 - u * m2)
            dv = q * (m1 - v * m2)
            eu = cu * du
            ev = cv * dv
            gs.append(eu * ru + ev * rv)
            cs.append(eu * du + ev * dv)
            dq = d * q
            ju = {0: -(u * y) * q, 1: (1.0 + u * x) * q, 2: -y * q, 3: dq, 5: -u * dq}
            jv = {0: (-1.0 - v * y) * q, 1: v * x * q, 2: x * q, 4: dq, 5: -v * dq}
            for a in range(6):
                if a in ju and a in jv:
                    e = ju[a] * eu + jv[a] * ev
                else:
                    e = ju[a] * eu if a in ju else jv[a] * ev
                coup[g, 24 * a + 8 * j : 24 * a + 8 * j + 8, cols] = e
            su = {a: cu * ju[a] for a in ju}
            sv = {a: cv * jv[a] for a in jv}
            for (a, b), row in K_PAIRS:
                if a in ju and b in ju:
                    add(row, su[a] * ju[b])
                if a in jv and b in jv:
                    add(row, sv[a] * jv[b])
            for a in range(6):
                if a in ju:
                    add(H_ROW + a, su[a] * ru)
                if a in jv:
                    add(H_ROW + a, sv[a] * rv)
        acc = [jnp.zeros((8, 128), F32) if x is None else x for x in acc]
        grads.append(jnp.concatenate(gs, 0))
        curvs.append(jnp.concatenate(cs, 0))
        blocks.append(merged_rows(acc))
    both = jnp.concatenate([jnp.concatenate(grads, 1), jnp.concatenate(curvs, 1)], 0)
    sums[...] += summed(both, hot[g])
    add_up(jnp.concatenate(blocks, 1), g, hot, own, total_s, total_t)


def source_columns():
    rows = lax.broadcasted_iota(jnp.int32, (128, LANES), 0)
    frame = lax.broadcasted_iota(jnp.int32, (1, LANES), 1) // 24
    return jnp.where(rows == (frame % 2) * 8 + frame // 2, 1.0, 0.0).astype(BF16)


def second_pass(g, hot, own, coup, inverse, total_s, total_t):
    near = gathered(inverse[...], hot[g])
    blocks = []
    for t in range(3):
        cols = slice(128 * t, 128 * t + 128)
        acc = [None] * 27
        for j in range(3):
            ci = near[8 * j : 8 * j + 8, cols]
            gi = near[24 + 8 * j : 32 + 8 * j, cols]
            e = [coup[g, 24 * a + 8 * j : 24 * a + 8 * j + 8, cols] for a in range(6)]
            for a in range(6):
                scaled = e[a] * ci
                new = [(row, scaled * e[b]) for (k, b), row in K_PAIRS if k == a]
                for row, value in [*new, (H_ROW + a, e[a] * gi)]:
                    acc[row] = value if acc[row] is None else acc[row] + value
        blocks.append(-merged_rows(acc))
    add_up(jnp.concatenate(blocks, 1), g, hot, own, total_s, total_t)


def third_pass(g, hot, own, coup, steps, fix):
    motion = expanded(steps[...], g, own) - gathered(steps[...], hot[g])
    parts = []
    for t in range(3):
        cols = slice(128 * t, 128 * t + 128)
        column = []
        for j in range(3):
            at = [slice(24 * a + 8 * j, 24 * a + 8 * j + 8) for a in range(6)]
            terms = [coup[g, at[a], cols] * motion[a : a + 1, cols] for a in range(6)]
            column.append(((terms[0] + terms[1]) + (terms[2] + terms[3])) + (terms[4] + terms[5]))
        parts.append(jnp.concatenate(column, 0))
    fix[...] += summed(jnp.concatenate(parts, 1), hot[g])


def solve(matrix, right):
    factor = {}
    for i in range(6):
        for j in range(i + 1):
            e = matrix(i, j)
            if i == j:
                e = e * 1.1 + 0.001
            for k in range(j):
                e = e - factor[i, k] * factor[j, k]
            factor[i, j] = jnp.sqrt(e) if i == j else e / factor[j, j]
    forward = []
    for i in range(6):
        e = right(i)
        for k in range(i):
            e = e - factor[i, k] * forward[k]
        forward.append(e / factor[i, i])
    z = [None] * 6
    for i in reversed(range(6)):
        e = forward[i]
        for k in range(i + 1, 6):
            e = e - factor[k, i] * z[k]
        z[i] = e / factor[i, i]
    return z


def ring_steps(d):
    return min(d, 4 - d)


def far_first():
    offsets = [
        (dz, dy, dx, dc)
        for dz in range(4)
        for dy in range(4)
        for dx in range(4)
        for dc in range(2)
        if (dz, dy, dx, dc) != (0, 0, 0, 0)
    ]
    return sorted(offsets, key=lambda o: -(ring_steps(o[0]) + ring_steps(o[1]) + ring_steps(o[2])))


def group_offset(n):
    return (n // 4 + n) % 4, n % 4


def by_group():
    order = []
    for n in range(GROUPS):
        oz, oy = group_offset(n)
        for dx in range(4):
            for dc in range(2):
                order.append(((oz + dx) % 4, (oy + dx) % 4, dx, dc))
    return order[1:]


def to_all(order, act):
    row, col = lax.axis_index("row"), lax.axis_index("col")
    y, x = col // 8, (col // 2) % 4
    zs = [((row + d) % 4) * 32 for d in range(4)]
    ys = [((y + d) % 4) * 8 for d in range(4)]
    xs = [((x + d) % 4) * 2 for d in range(4)]
    cs = [(col + d) % 2 for d in range(2)]
    gz = [((row + 4 - x + d) % 4) * 32 for d in range(4)]
    gy = [((y + 4 - x + d) % 4) * 8 for d in range(4)]
    for dz, dy, dx, dc in order:
        last = xs[dx] + cs[dc]
        act(zs[dz] + ys[dy] + last, gz[(dz - dx) % 4] + gy[(dy - dx) % 4] + last)


def slot_of(d):
    return (d % 16) * 8 + d // 16


def rows_exchange(send, recv, source, slot, send_sem, recv_sem):
    def act(d, place):
        pltpu.make_async_remote_copy(
            src_ref=send.at[pl.ds(source(d, place), 1), :],
            dst_ref=recv.at[pl.ds(slot, 1), :],
            send_sem=send_sem,
            recv_sem=recv_sem,
            device_id=d,
            device_id_type=pl.DeviceIdType.LOGICAL,
        ).start()

    to_all(far_first(), act)


def rows_wait(buf, sem):
    ref = buf.at[pl.ds(0, NDEV - 1), :]
    pltpu.make_async_copy(ref, ref, sem).wait()


def scope(name):
    return contextlib.nullcontext()


def loop(body, times):
    def step(n, carry):
        for k in range(times):
            body(times * n + k)
        return carry

    lax.fori_loop(0, GROUPS // times, step, 0)


def main_kernel(
    flow_hbm, weight_hbm, depth_ref, target_ref, rotation_ref, translation_ref,
    out_ref, pose_ref,
    flow, weight, low, high, chunks, ints, floats, unfold,
    recv, comps, table, hot, own, coup, sums, inverse, total_s, total_t, steps, fix,
    send_t, recv_t, send_d, recv_d, send_e, recv_e, send_f, recv_f,
    in_sem, big_send, big_recv, small_send, small_recv,
):
    row, col = lax.axis_index("row"), lax.axis_index("col")
    me = row * 32 + col
    y, x = col // 8, (col // 2) % 4
    my_gz, my_gy = (row + 4 - x) % 4, (y + 4 - x) % 4
    mine_at = (my_gz * 4 + my_gy) * 8 + col % 8
    lane = lane_iota()
    barrier = pltpu.get_barrier_semaphore()

    loads = [
        pltpu.make_async_copy(flow_hbm, flow, in_sem.at[0]),
        pltpu.make_async_copy(weight_hbm, weight, in_sem.at[1]),
    ]
    for load in loads:
        load.start()

    def greet(d, _):
        pl.semaphore_signal(
            barrier, inc=1, device_id=d, device_id_type=pl.DeviceIdType.LOGICAL
        )

    with scope("sc_greet"):
        to_all(far_first(), greet)

    with scope("sc_tables"):
        table[...] = jnp.zeros_like(table)
        sums[...] = jnp.zeros_like(sums)
        total_t[...] = jnp.zeros_like(total_t)
        total_s[...] = jnp.zeros_like(total_s)
        fix[...] = jnp.zeros_like(fix)
        own[...] = source_columns()
        high[...] = jnp.zeros_like(high)
        column, pose = own_edges(target_ref, rotation_ref, translation_ref, ints, floats)
        pack_tables(depth_ref, column, pose, unfold, send_t)
        recv_t[pl.ds(mine_at, 1), :] = send_t[pl.ds(slot_of(me), 1), :]
        turn = col % 8
        for load in loads:
            load.wait()

    def pack(n, carry):
        pack_block(n, turn, flow, weight, low, high, chunks)
        return carry

    with scope("sc_pack"):
        lax.fori_loop(0, 8, pack, 0)
    with scope("sc_barrier"):
        pl.semaphore_wait(barrier, NDEV - 1)

    with scope("sc_sends"):
        rows_exchange(
            send_t, recv_t, lambda d, _: slot_of(d), mine_at, small_send.at[3], small_recv.at[3]
        )

        def send_chunk(d, _):
            pltpu.make_async_remote_copy(
                src_ref=chunks.at[d, pl.ds(0, 36), :],
                dst_ref=recv.at[mine_at, pl.ds(0, 36), :],
                send_sem=big_send,
                recv_sem=big_recv.at[mine_at],
                device_id=d,
                device_id_type=pl.DeviceIdType.LOGICAL,
            ).start()

        to_all(by_group(), send_chunk)
        recv[mine_at, 0:36, :] = chunks[me, 0:36, :]

    with scope("sc_waitt"):
        rows_wait(recv_t, small_recv.at[3])
        known = recv_t[...].T
        for f in range(2):
            at = slice(128 * f, 128 * f + 128)
            table[0:24, at] = known[24 * f : 24 * f + 24]
            table[24:32, at] = known[48 + 8 * f : 56 + 8 * f]

    def arrive(n):
        oz, oy = group_offset(n)
        g = ((my_gz + 4 - oz) % 4) * 4 + (my_gy + 4 - oy) % 4
        for i in range(8):
            s = 8 * g + i

            @pl.when(s != mine_at)
            def _():
                ref = recv.at[s, pl.ds(0, 36), :]
                pltpu.make_async_copy(ref, ref, big_recv.at[s]).wait()

        unpack_group(g, recv, comps)
        first_pass(g, me, comps, recv_t, table, hot, own, coup, sums, total_s, total_t)

    with scope("sc_arrive"):
        loop(arrive, 1)
    with scope("sc_second"):
        ci = 1.0 / (0.1 + sums[24:48])
        inverse[0:24] = ci
        inverse[24:48] = sums[0:24] * ci
        loop(lambda g: second_pass(g, hot, own, coup, inverse, total_s, total_t), 2)

    with scope("sc_sendd"):
        kind = lax.broadcasted_iota(jnp.int32, (32, 256), 0)
        total = total_s[...] + jnp.where(kind < H_ROW, total_t[...], -total_t[...])
        send_d[...] = jnp.concatenate(
            [total[:, 0:128], total[:, 128:256], jnp.zeros((64, 128), F32)], 0
        ).T
        recv_d[pl.ds(mine_at, 1), :] = send_d[pl.ds(mine_at, 1), :]
        rows_exchange(
            send_d, recv_d, lambda _, place: place, mine_at, small_send.at[0], small_recv.at[0]
        )
    with scope("sc_waitd"):
        rows_wait(recv_d, small_recv.at[0])
    with scope("sc_solve"):
        line = jnp.sum(recv_d[...], axis=0, keepdims=True)
        sub = lax.broadcasted_iota(jnp.int32, (8, 128), 0)
        lines = jnp.broadcast_to(line, (8, 128))
        lines = jnp.where(sub == 1, pltpu.roll(lines, 96, 1), lines)
        full = jnp.concatenate([lines, jnp.zeros((120, 128), F32)], 0).T
        z = solve(
            lambda i, j: full[K_INDEX[i, j] : K_INDEX[i, j] + 1, :],
            lambda i: full[H_ROW + i : H_ROW + i + 1, :],
        )
        zs = jnp.concatenate([*z, jnp.zeros((122, 128), F32)], 0)
        turned = zs.T
        pose_ref[...] = turned[0:2, 0:6]
        mine = turned[0:1] + pltpu.roll(turned[0:8], 8, 1)[1:2]
        send_e[...] = jnp.broadcast_to(mine, (8, 128))
        recv_e[pl.ds(mine_at, 1), :] = mine
    with scope("sc_sende"):
        rows_exchange(
            send_e, recv_e, lambda d, _: 0, mine_at, small_send.at[1], small_recv.at[1]
        )
    with scope("sc_waite"):
        rows_wait(recv_e, small_recv.at[1])
    with scope("sc_third"):
        every = recv_e[...].T
        steps[:, 0:128] = every[0:8]
        steps[:, 128:256] = every[8:16]
        loop(lambda g: third_pass(g, hot, own, coup, steps, fix), 4)
    with scope("sc_sendf"):
        grad = sums[0:24]
        new = table[0:24] + (grad - fix[...]) * inverse[0:24]
        zero8 = jnp.zeros((8, 128), F32)
        send_f[...] = jnp.concatenate(
            [new[:, 0:128], zero8, new[:, 128:256], zero8, jnp.zeros((64, 128), F32)], 0
        ).T
        slot = slot_of(me)
        recv_f[pl.ds(slot, 1), :] = send_f[pl.ds(mine_at, 1), :]
        rows_exchange(
            send_f, recv_f, lambda _, place: place, slot, small_send.at[2], small_recv.at[2]
        )
    with scope("sc_waitf"):
        rows_wait(recv_f, small_recv.at[2])
    for f in range(2):
        tiles = [None] * 3
        for i in range(16):
            piece = recv_f[8 * i : 8 * i + 8, :]
            first = 24 * i
            moved = pltpu.roll(piece, (first - 32 * f) % 128, 1)
            for t in range(3):
                a, b = max(first - 128 * t, 0), min(first + 24 - 128 * t, 128)
                if a < b:
                    if tiles[t] is None:
                        tiles[t] = moved
                    else:
                        tiles[t] = jnp.where((lane >= a) & (lane < b), moved, tiles[t])
        for g in range(8):
            for t in range(3):
                at = 384 * g + 128 * t
                out_ref[f : f + 1, at : at + 128] = tiles[t][g : g + 1]

    ref = chunks.at[pl.ds(0, NDEV - 1), pl.ds(0, 36), :]
    pltpu.make_async_copy(ref, ref, big_send).wait()
    rows_wait(recv_t, small_send.at[3])
    rows_wait(recv_d, small_send.at[0])
    rows_wait(recv_e, small_send.at[1])
    rows_wait(recv_f, small_send.at[2])


def run_main(flow, weight, inv_depth, edge_target, rotation, translation):
    v = pltpu.VMEM
    vmem = pl.BlockSpec(memory_space=pltpu.VMEM)
    hbm = pl.BlockSpec(memory_space=pl.ANY)
    return pl.pallas_call(
        main_kernel,
        in_specs=[hbm, hbm, vmem, vmem, vmem, vmem],
        out_specs=[vmem] * 2,
        out_shape=[
            jax.ShapeDtypeStruct((2, PX * NDEV), F32),
            jax.ShapeDtypeStruct((2, 6), F32),
        ],
        scratch_shapes=[
            v((2, 48, PX * NDEV), F32),
            v((2, 48, PX * NDEV), F32),
            v((128, LANES), F32),
            v((128, LANES), F32),
            v((NDEV, 40, 128), F32),
            v((8, 128), jnp.int32),
            v((2, 8, 128), F32),
            v((2, 8, LANES), F32),
            v((NDEV, 40, 128), F32),
            v((96, LANES), F32),
            v((32, 256), F32),
            v((GROUPS, 256, LANES), BF16),
            v((128, LANES), BF16),
            v((GROUPS, 144, LANES), F32),
            v((48, 256), F32),
            v((48, 256), F32),
            v((32, 256), F32),
            v((32, 256), F32),
            v((8, 256), F32),
            v((24, 256), F32),
            v((128, 128), F32),
            v((128, 128), F32),
            v((128, 128), F32),
            v((128, 128), F32),
            v((8, 128), F32),
            v((128, 128), F32),
            v((128, 128), F32),
            v((128, 128), F32),
            pltpu.SemaphoreType.DMA((2,)),
            pltpu.SemaphoreType.DMA,
            pltpu.SemaphoreType.DMA((NDEV,)),
            pltpu.SemaphoreType.DMA((4,)),
            pltpu.SemaphoreType.DMA((4,)),
        ],
        compiler_params=pltpu.CompilerParams(
            collective_id=0, has_side_effects=True, vmem_limit_bytes=56 * 1024 * 1024
        ),
        name="step",
    )(flow, weight, inv_depth, edge_target, rotation, translation)


def shards(inv_depth, rotation, translation, edge_target, flow_obs, weight):
    pixels = inv_depth.shape[1]
    flow = flow_obs.reshape(2, 48, pixels)
    wts = weight.reshape(2, 48, pixels)
    depth, pose = run_main(flow, wts, inv_depth, edge_target, rotation.T, translation.T)
    return depth, pose.T


def solution(mesh):
    in_specs = (
        P(("row", "col"), None),
        P(None, ("row", "col")),
        P(None, ("row", "col")),
        P(("row", "col"), None),
        P(None, ("row", "col"), None, None),
        P(None, ("row", "col"), None, None),
    )
    out_specs = (P(("row", "col"), None), P(None, ("row", "col")))
    return jax.shard_map(
        shards, mesh=mesh, in_specs=in_specs, out_specs=out_specs, check_vma=False
    )
```

```python
import contextlib
import functools

import jax
import jax.numpy as jnp
from jax import lax
from jax.experimental import pallas as pl
from jax.experimental.pallas import tpu as pltpu
from jax.sharding import PartitionSpec as P

F32 = jnp.float32
BF16 = jnp.bfloat16
NDEV = 128
PX = 24
GROUPS = 16
LANES = 384
MESH = pl.DeviceIdType.MESH
K_PAIRS = [((a, b), n) for n, (a, b) in enumerate((a, b) for a in range(6) for b in range(a, 6))]
K_INDEX = {**dict(K_PAIRS), **{(b, a): n for (a, b), n in K_PAIRS}}
H_ROW = 21
ARRIVE, LAST, THIRD = 2, 4, 8


def lane_iota(shape=(8, 128)):
    return lax.broadcasted_iota(jnp.int32, shape, 1)


def pack_block(n, turn, flow, weight, low, high, out):
    cols = pl.ds(pl.multiple_of(n * LANES, 128), LANES)

    def put(ref, block, value):
        at = pl.multiple_of(((3 * turn + block) % 8) * 16, 16)
        ref[pl.ds(at, 16), :] = value

    for k in range(3):
        put(low, k, flow[0, 16 * k : 16 * k + 16, cols])
        put(low, 3 + k, flow[1, 16 * k : 16 * k + 16, cols])
        put(high, 1 + k, weight[1, 16 * k : 16 * k + 16, cols])
    put(low, 6, weight[0, 0:16, cols])
    put(low, 7, weight[0, 16:32, cols])
    put(high, 0, weight[0, 32:48, cols])
    low_t = low[...].T
    high_t = high[...].T
    where_at = (lane_iota() - 48 * turn + 384) % 128
    for d in range(16):
        for j in range(3):
            at = 24 * d + 8 * j
            out[16 * n + d, j, 0:8, :] = low_t[at : at + 8]
            rest = high_t[at : at + 8]
            turned = pltpu.roll(pltpu.roll(rest, 64, 1), 4, 0)
            out[16 * n + d, j, 8:12, :] = jnp.where(where_at < 64, rest, turned)[0:4]


def own_edges(target_ref, rotation_ref, translation_ref, ints, floats):
    lane = lane_iota()
    ints[...] = jnp.zeros_like(ints)
    ints[0:2, 0:24] = target_ref[...]
    both = ints[...]
    target = jnp.where(lane < 24, both[0:1], pltpu.roll(both, 24, 1)[1:2])
    x, y, z = (target >> 2) & 3, (target >> 4) & 3, target >> 6
    group = (((z - x) & 3) << 2) + ((y - x) & 3)
    column = ((target & 1) << 7) + (group << 3) + ((target >> 1) & 7)
    floats[...] = jnp.zeros_like(floats)
    floats[0, 0:2, 0:3] = rotation_ref[...]
    floats[1, 0:2, 0:3] = translation_ref[...]
    return column.astype(F32), floats[0] + pltpu.roll(floats[1], 3, 1)


def pack_tables(depth_ref, column, pose, unfold, send):
    lane = lane_iota()
    poses = pltpu.roll(pose, 48, 1)[0:1] + pltpu.roll(pose, 56, 1)[1:2]
    known = jnp.where(lane < 64, poses, pltpu.roll(column, 64, 1)[0:1])
    for f in range(2):
        for g in range(8):
            unfold[f, g : g + 1, :] = depth_ref[f : f + 1, LANES * g : LANES * g + LANES]
    for i in range(16):
        acc = known
        for f in range(2):
            for t in range(3):
                a, b = max(24 * i - 128 * t, 0), min(24 * i + 24 - 128 * t, 128)
                if a < b:
                    shift = 24 * f - (24 * i - 128 * t)
                    moved = pltpu.roll(unfold[f, :, 128 * t : 128 * t + 128], shift % 128, 1)
                    acc = jnp.where((lane >= a + shift) & (lane < b + shift), moved, acc)
        send[8 * i : 8 * i + 8, :] = acc


def strip(tiles, lane, offset, width):
    out = []
    for t in range(3):
        acc = None
        for i in range(8):
            start = 48 * i + offset
            for wrap in (0, 384, 768):
                a = max(start - wrap, 128 * t) - 128 * t
                b = min(start + width - wrap, 128 * t + 128) - 128 * t
                if a < b:
                    if acc is None:
                        acc = tiles[i]
                    else:
                        acc = jnp.where((lane >= a) & (lane < b), tiles[i], acc)
        out.append(acc)
    return out


def shifted(tiles, lane, shift):
    whole, part = divmod(shift % 384, 128)
    if part == 0:
        return [tiles[(t - whole) % 3] for t in range(3)]
    rolled = [pltpu.roll(t, part, 1) for t in tiles]
    return [
        jnp.where(lane < part, rolled[(t - whole - 1) % 3], rolled[(t - whole) % 3])
        for t in range(3)
    ]


def split3(x):
    top = x.astype(BF16).astype(F32)
    rest = x - top
    mid = rest.astype(BF16).astype(F32)
    return jnp.concatenate([top, mid, rest - mid], 0).astype(BF16)


def join3(y):
    n = y.shape[0] // 3
    return y[:n] + y[n : 2 * n] + y[2 * n :]


def gathered(table, hot):
    return join3(jnp.dot(split3(table), hot, preferred_element_type=F32))


def summed(values, hot_t):
    return join3(jnp.dot(split3(values), hot_t, preferred_element_type=F32))


def unpack_group(g, j, recv):
    lane = lane_iota()
    upper = lax.broadcasted_iota(jnp.int32, (8, 128), 0) >= 4
    block_lane = [(lane + 128 * t) % 48 for t in range(3)]
    low = [recv[8 * g + i, j, 0:8, :] for i in range(8)]
    high = [recv[8 * g + i, j, 8:16, :] for i in range(8)]

    def at(tiles, start, width, to):
        return shifted(strip(tiles, lane, start, width), lane, to - start)

    def piece(offset, width, to):
        first, second = at(high, offset, width, to), at(high, offset + 64, width, to)
        return [jnp.where(upper, pltpu.roll(b, 4, 0), a) for a, b in zip(first, second)]

    first, second = at(low, 96, 32, 0), piece(0, 16, 32)
    return [
        at(low, 0, 48, 0),
        at(low, 48, 48, 0),
        [jnp.where(b < 32, f, s) for b, f, s in zip(block_lane, first, second)],
        piece(16, 48, 0),
    ]


def group_targets(g, recv_t):
    lane = lane_iota()
    sub = lax.broadcasted_iota(jnp.int32, (8, 128), 0)
    tile = recv_t[pl.ds(pl.multiple_of(8 * g, 8), 8), :]
    out = [jnp.zeros((8, 128), F32)] * 3
    for i in range(8):
        moved = pltpu.roll(tile, (48 * i - 64) % 128, 1)
        for t in range(3):
            a, b = max(48 * i - 128 * t, 0), min(48 * i + 48 - 128 * t, 128)
            if a < b:
                out[t] = jnp.where((sub == i) & (lane >= a) & (lane < b), moved, out[t])
    return jnp.concatenate([jnp.sum(x, axis=0, keepdims=True) for x in out], 1)


def merge(items):
    sub = lax.broadcasted_iota(jnp.int32, (8, 128), 0)
    items = items[::-1]
    for bit in (0, 1, 2):
        step = 1 << bit
        here = (sub & step) != 0
        items = [
            jnp.where(here, a, b) + pltpu.roll(jnp.where(here, b, a), step, 0)
            for a, b in zip(items[0::2], items[1::2])
        ]
    return items[0]


def merged_rows(rows):
    rows = rows + [jnp.zeros((8, 128), F32)] * (32 - len(rows))
    return jnp.concatenate([merge(rows[k : k + 8]) for k in range(0, 32, 8)], 0)


def pixel_xy(me, j):
    p = me * PX + 8 * j + lax.broadcasted_iota(jnp.int32, (8, 128), 0)
    x = ((p % 64).astype(F32) + 0.5) / 64 - 0.5
    y = ((p // 64).astype(F32) + 0.5 - 24.0) / 64
    return x, y


def expand(rows, own, out):
    lane = lane_iota()
    mine = [
        jnp.where(
            lane < 8,
            pltpu.roll(rows[:, 0:128], (128 - 8 * g) % 128, 1),
            pltpu.roll(rows[:, 128:256], (136 - 8 * g) % 128, 1),
        )
        for g in range(GROUPS)
    ]
    out[...] = gathered(jnp.concatenate(mine, 0), own[...])


def rows_of(ref, g):
    return ref[pl.ds(pl.multiple_of(8 * g, 8), 8), :]


def add_up(values, g, hot_t, own_t, total_s, total_t):
    total_t[...] += summed(values, hot_t[g])
    by_source = summed(values, own_t[...])
    lane = lane_iota((32, 128))
    for f in range(2):
        at = slice(128 * f, 128 * f + 128)
        moved = pltpu.roll(by_source, (8 * g - 8 * f + 128) % 128, 1)
        total_s[:, at] += jnp.where(lane // 8 == g, moved, 0.0)


def edge_rows(a, j):
    return slice(24 * a + 8 * j, 24 * a + 8 * j + 8)


def add_block(acc, row, value):
    acc[row] = value if acc[row] is None else acc[row] + value


def source_columns_t():
    frame = lax.broadcasted_iota(jnp.int32, (LANES, 1), 0) // 24
    lanes = lax.broadcasted_iota(jnp.int32, (LANES, 128), 1)
    return jnp.where(lanes == (frame % 2) * 8 + frame // 2, 1.0, 0.0).astype(BF16)


def build_terms(acc, cols, inputs, d, rel, xy, coup, g, j):
    x, y = xy
    fu, fv, cu, cv = inputs
    w0, w1, w2, m0, m1, m2 = [rel[k : 1 + k, cols] for k in range(6)]
    x0 = x + w1 - w2 * y + m0 * d
    x1 = y + w2 * x - w0 + m1 * d
    x2 = 1.0 + w0 * y - w1 * x + m2 * d
    q = 1.0 / x2
    u = x0 * q
    v = x1 * q
    ru = fu - (u - x)
    rv = fv - (v - y)
    du = q * (m0 - u * m2)
    dv = q * (m1 - v * m2)
    eu = cu * du
    ev = cv * dv
    dq = d * q
    ju = {0: -(u * y) * q, 1: (1.0 + u * x) * q, 2: -y * q, 3: dq, 5: -u * dq}
    jv = {0: (-1.0 - v * y) * q, 1: v * x * q, 2: x * q, 4: dq, 5: -v * dq}
    for a in range(6):
        if a in ju and a in jv:
            e = ju[a] * eu + jv[a] * ev
        else:
            e = ju[a] * eu if a in ju else jv[a] * ev
        coup[g, edge_rows(a, j), cols] = e
    su = {a: cu * ju[a] for a in ju}
    sv = {a: cv * jv[a] for a in jv}
    for (a, b), row in K_PAIRS:
        if a in ju and b in ju:
            add_block(acc, row, su[a] * ju[b])
        if a in jv and b in jv:
            add_block(acc, row, sv[a] * jv[b])
    for a in range(6):
        if a in ju:
            add_block(acc, H_ROW + a, su[a] * ru)
        if a in jv:
            add_block(acc, H_ROW + a, sv[a] * rv)
    return eu * ru + ev * rv, eu * du + ev * dv


def take_terms(acc, cols, near, coup, g, j):
    ci, gi = -near[0:8, cols], -near[8:16, cols]
    e = [coup[g, edge_rows(a, j), cols] for a in range(6)]
    for a in range(6):
        scaled = e[a] * ci
        for (k, b), row in K_PAIRS:
            if k == a:
                add_block(acc, row, scaled * e[b])
        add_block(acc, H_ROW + a, e[a] * gi)


def filled(acc):
    return [jnp.zeros((8, 128), F32) if x is None else x for x in acc]


def phase_pass(g, j, me, recv, recv_t, table, hot, hot_t, from_pose, dep, rel, coup, sums, inverse, kh):
    if j == 0:
        rows = lax.broadcasted_iota(jnp.int32, (256, LANES), 0).astype(F32)
        targets = group_targets(g, recv_t)
        hot[g] = jnp.where(rows == targets, 1.0, 0.0).astype(BF16)
        lanes = lane_iota((128, 256)).astype(F32)
        for t in range(3):
            at = slice(128 * t, 128 * t + 128)
            column = jnp.broadcast_to(targets[:, at], (128, 128)).T
            column = jnp.concatenate([column, column], 1)
            hot_t[g, at, :] = jnp.where(lanes == column, 1.0, 0.0).astype(BF16)
        near = gathered(table[...], hot[g])
        dep[g] = near[0:24]
        relative = rows_of(from_pose, g) - near[24:32]
        rel[g] = relative
    else:
        relative = rel[g]
        back = gathered(inverse[j - 1], hot[g])
    parts = unpack_group(g, j, recv)
    grads, curvs, blocks = [], [], []
    xy = pixel_xy(me, j)
    for t in range(3):
        cols = slice(128 * t, 128 * t + 128)
        acc = [None] * 27
        d = dep[g, 8 * j : 8 * j + 8, cols]
        tiles = [part[t] for part in parts]
        gd, cd = build_terms(acc, cols, tiles, d, relative, xy, coup, g, j)
        grads.append(gd)
        curvs.append(cd)
        if j > 0:
            take_terms(acc, cols, back, coup, g, j - 1)
        blocks.append(merged_rows(filled(acc)))
    both = jnp.concatenate([jnp.concatenate(grads, 1), jnp.concatenate(curvs, 1)], 0)
    sums[j] += summed(both, hot_t[g])
    block = jnp.concatenate(blocks, 1)
    kh[g] = block if j == 0 else kh[g] + block


def source_columns():
    rows = lax.broadcasted_iota(jnp.int32, (128, LANES), 0)
    frame = lax.broadcasted_iota(jnp.int32, (1, LANES), 1) // 24
    return jnp.where(rows == (frame % 2) * 8 + frame // 2, 1.0, 0.0).astype(BF16)


def last_pass(g, hot, hot_t, own_t, coup, inverse, kh, total_s, total_t):
    near = gathered(inverse[2], hot[g])
    blocks = []
    for t in range(3):
        acc = [None] * 27
        take_terms(acc, slice(128 * t, 128 * t + 128), near, coup, g, 2)
        blocks.append(merged_rows(acc))
    add_up(kh[g] + jnp.concatenate(blocks, 1), g, hot_t, own_t, total_s, total_t)


def third_pass(g, hot_t, coup, from_steps, fix):
    motion = rows_of(from_steps, g)
    parts = []
    for t in range(3):
        cols = slice(128 * t, 128 * t + 128)
        column = []
        for j in range(3):
            terms = [coup[g, edge_rows(a, j), cols] * motion[a : a + 1, cols] for a in range(6)]
            column.append(((terms[0] + terms[1]) + (terms[2] + terms[3])) + (terms[4] + terms[5]))
        parts.append(jnp.concatenate(column, 0))
    fix[...] += summed(jnp.concatenate(parts, 1), hot_t[g])


def solve(matrix, right):
    factor = {}
    for i in range(6):
        for j in range(i + 1):
            e = matrix(i, j)
            if i == j:
                e = e * 1.1 + 0.001
            for k in range(j):
                e = e - factor[i, k] * factor[j, k]
            factor[i, j] = jnp.sqrt(e) if i == j else e / factor[j, j]
    forward = []
    for i in range(6):
        e = right(i)
        for k in range(i):
            e = e - factor[i, k] * forward[k]
        forward.append(e / factor[i, i])
    z = [None] * 6
    for i in reversed(range(6)):
        e = forward[i]
        for k in range(i + 1, 6):
            e = e - factor[k, i] * z[k]
        z[i] = e / factor[i, i]
    return z


def ring_steps(d):
    return min(d, 4 - d)


def far_first():
    offsets = [
        (dz, dy, dx, dc)
        for dz in range(4)
        for dy in range(4)
        for dx in range(4)
        for dc in range(2)
        if (dz, dy, dx, dc) != (0, 0, 0, 0)
    ]
    return sorted(offsets, key=lambda o: -(ring_steps(o[0]) + ring_steps(o[1]) + ring_steps(o[2])))


def group_offset(n):
    return (n // 4 + n) % 4, n % 4


def by_group():
    order = []
    for n in range(GROUPS):
        oz, oy = group_offset(n)
        for dx in range(4):
            for dc in range(2):
                order.append(((oz + dx) % 4, (oy + dx) % 4, dx, dc))
    return order[1:]


def to_all(order, act):
    row, col = lax.axis_index("row"), lax.axis_index("col")
    y, x = col // 8, (col // 2) % 4
    zs = [((row + d) % 4) * 32 for d in range(4)]
    ys = [((y + d) % 4) * 8 for d in range(4)]
    xs = [((x + d) % 4) * 2 for d in range(4)]
    cs = [(col + d) % 2 for d in range(2)]
    gz = [((row + 4 - x + d) % 4) * 32 for d in range(4)]
    gy = [((y + 4 - x + d) % 4) * 8 for d in range(4)]
    for dz, dy, dx, dc in order:
        last = xs[dx] + cs[dc]
        act(zs[dz] + ys[dy] + last, gz[(dz - dx) % 4] + gy[(dy - dx) % 4] + last)


def slot_of(d):
    return (d % 16) * 8 + d // 16


def rows_exchange(send, recv, source, slot, send_sem, recv_sem):
    def act(d, place):
        pltpu.make_async_remote_copy(
            src_ref=send.at[pl.ds(source(d, place), 1), :],
            dst_ref=recv.at[pl.ds(slot, 1), :],
            send_sem=send_sem,
            recv_sem=recv_sem,
            device_id=d,
            device_id_type=pl.DeviceIdType.LOGICAL,
        ).start()

    to_all(far_first(), act)


def rows_wait(buf, sem):
    ref = buf.at[pl.ds(0, NDEV - 1), :]
    pltpu.make_async_copy(ref, ref, sem).wait()


def scope(name):
    return contextlib.nullcontext()


def loop(body, times):
    def step(n, carry):
        for k in range(times):
            body(times * n + k)
        return carry

    lax.fori_loop(0, GROUPS // times, step, 0)


def main_kernel(
    flow_hbm, weight_hbm, depth_hbm, target_hbm, rotation_hbm, translation_hbm,
    out_ref, pose_ref,
    flow, weight, depth_ref, target_ref, rotation_ref, translation_ref, low, high, chunks, ints, floats, unfold,
    recv, table, hot, hot_t, own, own_t, from_pose, dep, rel, coup, sums, inverse, kh,
    total_s, total_t, at_target, steps, from_steps, fix,
    send_t, recv_t, send_d, recv_d, send_e, recv_e, send_f, recv_f,
    in_sem, big_send, big_recv, small_send, small_recv,
):
    row, col = lax.axis_index("row"), lax.axis_index("col")
    me = row * 32 + col
    y, x = col // 8, (col // 2) % 4
    my_gz, my_gy = (row + 4 - x) % 4, (y + 4 - x) % 4
    my_group = my_gz * 4 + my_gy
    mine_at = my_group * 8 + col % 8
    lane = lane_iota()
    barrier = pltpu.get_barrier_semaphore()

    inputs = [
        (depth_hbm, depth_ref),
        (target_hbm, target_ref),
        (rotation_hbm, rotation_ref),
        (translation_hbm, translation_ref),
        (flow_hbm, flow),
        (weight_hbm, weight),
    ]
    loads = [
        pltpu.make_async_copy(source, to, in_sem.at[k]) for k, (source, to) in enumerate(inputs)
    ]

    def greet(d, _):
        pl.semaphore_signal(
            barrier, inc=1, device_id=d, device_id_type=pl.DeviceIdType.LOGICAL
        )

    with scope("sc_greet"):
        for load in loads:
            load.start()
        to_all(far_first(), greet)

    with scope("sc_tables"):
        table[...] = jnp.zeros_like(table)
        sums[...] = jnp.zeros_like(sums)
        total_t[...] = jnp.zeros_like(total_t)
        total_s[...] = jnp.zeros_like(total_s)
        fix[...] = jnp.zeros_like(fix)
        at_target[...] = jnp.zeros_like(at_target)
        own[...] = source_columns()
        own_t[...] = source_columns_t()
        high[...] = jnp.zeros_like(high)
        for load in loads[:4]:
            load.wait()
        column, pose = own_edges(target_ref, rotation_ref, translation_ref, ints, floats)
        pack_tables(depth_ref, column, pose, unfold, send_t)
        recv_t[pl.ds(mine_at, 1), :] = send_t[pl.ds(slot_of(me), 1), :]
        turn = col % 8
        for load in loads[4:]:
            load.wait()

    def pack(n, carry):
        pack_block(n, turn, flow, weight, low, high, chunks)
        return carry

    with scope("sc_pack"):
        lax.fori_loop(0, 8, pack, 0)
    with scope("sc_barrier"):
        pl.semaphore_wait(barrier, NDEV - 1)

    with scope("sc_sends"):
        rows_exchange(
            send_t, recv_t, lambda d, _: slot_of(d), mine_at, small_send.at[3], small_recv.at[3]
        )

        for j in range(3):

            def send_chunk(d, _):
                pltpu.make_async_remote_copy(
                    src_ref=chunks.at[d, j, pl.ds(0, 12), :],
                    dst_ref=recv.at[mine_at, j, pl.ds(0, 12), :],
                    send_sem=big_send,
                    recv_sem=big_recv.at[j, my_group],
                    device_id=d,
                    device_id_type=pl.DeviceIdType.LOGICAL,
                ).start()

            to_all(by_group(), send_chunk)
        recv[mine_at, :, 0:12, :] = chunks[me, :, 0:12, :]

    with scope("sc_waitt"):
        rows_wait(recv_t, small_recv.at[3])
        known = recv_t[...].T
        for f in range(2):
            at = slice(128 * f, 128 * f + 128)
            table[0:24, at] = known[24 * f : 24 * f + 24]
            table[24:32, at] = known[48 + 8 * f : 56 + 8 * f]
        expand(table[24:32, :], own, from_pose)

    def arrive(n, j):
        oz, oy = group_offset(n)
        g = ((my_gz + 4 - oz) % 4) * 4 + (my_gy + 4 - oy) % 4

        def landed(count):
            ref = recv.at[pl.ds(8 * g, count), j, pl.ds(0, 12), :]
            pltpu.make_async_copy(ref, ref, big_recv.at[j, g]).wait()

        pl.when(n == 0)(lambda: landed(7))
        pl.when(n != 0)(lambda: landed(8))

        phase_pass(
            g, j, me, recv, recv_t, table, hot, hot_t, from_pose, dep, rel, coup, sums,
            inverse, kh,
        )

    for j in range(3):
        with scope(f"sc_arrive{j}"):
            loop(functools.partial(arrive, j=j), ARRIVE)
            ci = 1.0 / (0.1 + sums[j, 8:16])
            inverse[j, 0:8] = ci
            inverse[j, 8:16] = sums[j, 0:8] * ci
    with scope("sc_last"):
        loop(
            lambda g: last_pass(g, hot, hot_t, own_t, coup, inverse, kh, total_s, total_t), LAST
        )

    with scope("sc_sendd"):
        kind = lax.broadcasted_iota(jnp.int32, (32, 256), 0)
        total = total_s[...] + jnp.where(kind < H_ROW, total_t[...], -total_t[...])
        send_d[...] = jnp.concatenate(
            [total[:, 0:128], total[:, 128:256], jnp.zeros((64, 128), F32)], 0
        ).T
        recv_d[pl.ds(mine_at, 1), :] = send_d[pl.ds(mine_at, 1), :]
        rows_exchange(
            send_d, recv_d, lambda _, place: place, mine_at, small_send.at[0], small_recv.at[0]
        )
    with scope("sc_target"):

        def couple(g):
            at_target[...] += summed(coup[g], hot_t[g])

        loop(couple, 2)
    with scope("sc_waitd"):
        rows_wait(recv_d, small_recv.at[0])
    with scope("sc_solve"):
        line = jnp.sum(recv_d[...], axis=0, keepdims=True)
        sub = lax.broadcasted_iota(jnp.int32, (8, 128), 0)
        lines = jnp.broadcast_to(line, (8, 128))
        lines = jnp.where(sub == 1, pltpu.roll(lines, 96, 1), lines)
        full = jnp.concatenate([lines, jnp.zeros((120, 128), F32)], 0).T
        z = solve(
            lambda i, j: full[K_INDEX[i, j] : K_INDEX[i, j] + 1, :],
            lambda i: full[H_ROW + i : H_ROW + i + 1, :],
        )
        zs = jnp.concatenate([*z, jnp.zeros((122, 128), F32)], 0)
        turned = zs.T
        pose_ref[...] = turned[0:2, 0:6]
        mine = turned[0:1] + pltpu.roll(turned[0:8], 8, 1)[1:2]
        send_e[...] = jnp.broadcast_to(mine, (8, 128))
        recv_e[pl.ds(mine_at, 1), :] = mine
    with scope("sc_sende"):
        rows_exchange(
            send_e, recv_e, lambda d, _: 0, mine_at, small_send.at[1], small_recv.at[1]
        )
    with scope("sc_waite"):
        rows_wait(recv_e, small_recv.at[1])
    with scope("sc_third"):
        every = recv_e[...].T
        steps[:, 0:128] = every[0:8]
        steps[:, 128:256] = every[8:16]
        expand(steps[...], own, from_steps)
        loop(lambda g: third_pass(g, hot_t, coup, from_steps, fix), THIRD)
    with scope("sc_sendf"):
        back = at_target[0:24] * steps[0:1]
        for a in range(1, 6):
            back += at_target[24 * a : 24 * a + 24] * steps[a : a + 1]
        grad = jnp.concatenate([sums[j, 0:8] for j in range(3)], 0)
        ci = jnp.concatenate([inverse[j, 0:8] for j in range(3)], 0)
        new = table[0:24] + (grad - (fix[...] - back)) * ci
        zero8 = jnp.zeros((8, 128), F32)
        send_f[...] = jnp.concatenate(
            [new[:, 0:128], zero8, new[:, 128:256], zero8, jnp.zeros((64, 128), F32)], 0
        ).T
        slot = slot_of(me)
        recv_f[pl.ds(slot, 1), :] = send_f[pl.ds(mine_at, 1), :]
        rows_exchange(
            send_f, recv_f, lambda _, place: place, slot, small_send.at[2], small_recv.at[2]
        )
    with scope("sc_waitf"):
        rows_wait(recv_f, small_recv.at[2])
    for f in range(2):
        tiles = [None] * 3
        for i in range(16):
            piece = recv_f[8 * i : 8 * i + 8, :]
            first = 24 * i
            moved = pltpu.roll(piece, (first - 32 * f) % 128, 1)
            for t in range(3):
                a, b = max(first - 128 * t, 0), min(first + 24 - 128 * t, 128)
                if a < b:
                    if tiles[t] is None:
                        tiles[t] = moved
                    else:
                        tiles[t] = jnp.where((lane >= a) & (lane < b), moved, tiles[t])
        for g in range(8):
            for t in range(3):
                at = 384 * g + 128 * t
                out_ref[f : f + 1, at : at + 128] = tiles[t][g : g + 1]

    ref = chunks.at[pl.ds(0, NDEV - 1), :, pl.ds(0, 12), :]
    pltpu.make_async_copy(ref, ref, big_send).wait()
    rows_wait(recv_t, small_send.at[3])
    rows_wait(recv_d, small_send.at[0])
    rows_wait(recv_e, small_send.at[1])
    rows_wait(recv_f, small_send.at[2])


def run_main(flow, weight, inv_depth, edge_target, rotation, translation):
    v = pltpu.VMEM
    vmem = pl.BlockSpec(memory_space=pltpu.VMEM)
    hbm = pl.BlockSpec(memory_space=pl.ANY)
    return pl.pallas_call(
        main_kernel,
        in_specs=[hbm] * 6,
        out_specs=[vmem] * 2,
        out_shape=[
            jax.ShapeDtypeStruct((2, PX * NDEV), F32),
            jax.ShapeDtypeStruct((2, 6), F32),
        ],
        scratch_shapes=[
            v((2, 48, PX * NDEV), F32),
            v((2, 48, PX * NDEV), F32),
            v((2, PX * NDEV), F32),
            v((2, 24), jnp.int32),
            v((2, 3), F32),
            v((2, 3), F32),
            v((128, LANES), F32),
            v((128, LANES), F32),
            v((NDEV, 3, 16, 128), F32),
            v((8, 128), jnp.int32),
            v((2, 8, 128), F32),
            v((2, 8, LANES), F32),
            v((NDEV, 3, 16, 128), F32),
            v((32, 256), F32),
            v((GROUPS, 256, LANES), BF16),
            v((GROUPS, LANES, 256), BF16),
            v((128, LANES), BF16),
            v((LANES, 128), BF16),
            v((128, LANES), F32),
            v((GROUPS, 24, LANES), F32),
            v((GROUPS, 8, LANES), F32),
            v((GROUPS, 144, LANES), F32),
            v((3, 16, 256), F32),
            v((3, 16, 256), F32),
            v((GROUPS, 32, LANES), F32),
            v((32, 256), F32),
            v((32, 256), F32),
            v((144, 256), F32),
            v((8, 256), F32),
            v((128, LANES), F32),
            v((24, 256), F32),
            v((128, 128), F32),
            v((128, 128), F32),
            v((128, 128), F32),
            v((128, 128), F32),
            v((8, 128), F32),
            v((128, 128), F32),
            v((128, 128), F32),
            v((128, 128), F32),
            pltpu.SemaphoreType.DMA((6,)),
            pltpu.SemaphoreType.DMA,
            pltpu.SemaphoreType.DMA((3, GROUPS)),
            pltpu.SemaphoreType.DMA((4,)),
            pltpu.SemaphoreType.DMA((4,)),
        ],
        compiler_params=pltpu.CompilerParams(
            collective_id=0, has_side_effects=True, vmem_limit_bytes=56 * 1024 * 1024
        ),
        name="step",
    )(flow, weight, inv_depth, edge_target, rotation, translation)


def shards(inv_depth, rotation, translation, edge_target, flow_obs, weight):
    pixels = inv_depth.shape[1]
    flow = flow_obs.reshape(2, 48, pixels)
    wts = weight.reshape(2, 48, pixels)
    depth, pose = run_main(flow, wts, inv_depth, edge_target, rotation.T, translation.T)
    return depth, pose.T


def solution(mesh):
    in_specs = (
        P(("row", "col"), None),
        P(None, ("row", "col")),
        P(None, ("row", "col")),
        P(("row", "col"), None),
        P(None, ("row", "col"), None, None),
        P(None, ("row", "col"), None, None),
    )
    out_specs = (P(("row", "col"), None), P(None, ("row", "col")))
    return jax.shard_map(
        shards, mesh=mesh, in_specs=in_specs, out_specs=out_specs, check_vma=False
    )
```

```python
import contextlib
import functools

import jax
import jax.numpy as jnp
from jax import lax
from jax.experimental import pallas as pl
from jax.experimental.pallas import tpu as pltpu
from jax.sharding import PartitionSpec as P

F32 = jnp.float32
BF16 = jnp.bfloat16
NDEV = 128
PX = 24
GROUPS = 16
LANES = 384
MESH = pl.DeviceIdType.MESH
K_PAIRS = [((a, b), n) for n, (a, b) in enumerate((a, b) for a in range(6) for b in range(a, 6))]
K_INDEX = {**dict(K_PAIRS), **{(b, a): n for (a, b), n in K_PAIRS}}
H_ROW = 21


def lane_iota(shape=(8, 128)):
    return lax.broadcasted_iota(jnp.int32, shape, 1)


def pack_block(n, turn, flow, weight, low, high, out):
    cols = pl.ds(pl.multiple_of(n * LANES, 128), LANES)

    def put(ref, block, value):
        at = pl.multiple_of(((3 * turn + block) % 8) * 16, 16)
        ref[pl.ds(at, 16), :] = value

    for k in range(3):
        put(low, k, flow[0, 16 * k : 16 * k + 16, cols])
        put(low, 3 + k, flow[1, 16 * k : 16 * k + 16, cols])
        put(high, 1 + k, weight[1, 16 * k : 16 * k + 16, cols])
    put(low, 6, weight[0, 0:16, cols])
    put(low, 7, weight[0, 16:32, cols])
    put(high, 0, weight[0, 32:48, cols])
    low_t = low[...].T
    high_t = high[...].T
    where_at = (lane_iota() - 48 * turn + 384) % 128
    for d in range(16):
        for j in range(3):
            at = 24 * d + 8 * j
            out[16 * n + d, j, 0:8, :] = low_t[at : at + 8]
            rest = high_t[at : at + 8]
            turned = pltpu.roll(pltpu.roll(rest, 64, 1), 4, 0)
            out[16 * n + d, j, 8:12, :] = jnp.where(where_at < 64, rest, turned)[0:4]


def own_edges(target_ref, rotation_ref, translation_ref, ints, floats):
    lane = lane_iota()
    ints[...] = jnp.zeros_like(ints)
    ints[0:2, 0:24] = target_ref[...]
    both = ints[...]
    target = jnp.where(lane < 24, both[0:1], pltpu.roll(both, 24, 1)[1:2])
    x, y, z = (target >> 2) & 3, (target >> 4) & 3, target >> 6
    group = (((z - x) & 3) << 2) + ((y - x) & 3)
    column = ((target & 1) << 7) + (group << 3) + ((target >> 1) & 7)
    floats[...] = jnp.zeros_like(floats)
    floats[0, 0:2, 0:3] = rotation_ref[...]
    floats[1, 0:2, 0:3] = translation_ref[...]
    return column.astype(F32), floats[0] + pltpu.roll(floats[1], 3, 1)


def pack_tables(depth_ref, column, pose, unfold, send):
    lane = lane_iota()
    poses = pltpu.roll(pose, 48, 1)[0:1] + pltpu.roll(pose, 56, 1)[1:2]
    known = jnp.where(lane < 64, poses, pltpu.roll(column, 64, 1)[0:1])
    for f in range(2):
        for g in range(8):
            unfold[f, g : g + 1, :] = depth_ref[f : f + 1, LANES * g : LANES * g + LANES]
    for i in range(16):
        acc = known
        for f in range(2):
            for t in range(3):
                a, b = max(24 * i - 128 * t, 0), min(24 * i + 24 - 128 * t, 128)
                if a < b:
                    shift = 24 * f - (24 * i - 128 * t)
                    moved = pltpu.roll(unfold[f, :, 128 * t : 128 * t + 128], shift % 128, 1)
                    acc = jnp.where((lane >= a + shift) & (lane < b + shift), moved, acc)
        send[8 * i : 8 * i + 8, :] = acc


def strip(tiles, lane, offset, width):
    out = []
    for t in range(3):
        acc = None
        for i in range(8):
            start = 48 * i + offset
            for wrap in (0, 384, 768):
                a = max(start - wrap, 128 * t) - 128 * t
                b = min(start + width - wrap, 128 * t + 128) - 128 * t
                if a < b:
                    if acc is None:
                        acc = tiles[i]
                    else:
                        acc = jnp.where((lane >= a) & (lane < b), tiles[i], acc)
        out.append(acc)
    return out


def shifted(tiles, lane, shift):
    whole, part = divmod(shift % 384, 128)
    if part == 0:
        return [tiles[(t - whole) % 3] for t in range(3)]
    rolled = [pltpu.roll(t, part, 1) for t in tiles]
    return [
        jnp.where(lane < part, rolled[(t - whole - 1) % 3], rolled[(t - whole) % 3])
        for t in range(3)
    ]


def split3(x):
    top = x.astype(BF16).astype(F32)
    rest = x - top
    mid = rest.astype(BF16).astype(F32)
    return jnp.concatenate([top, mid, rest - mid], 0).astype(BF16)


def join3(y):
    n = y.shape[0] // 3
    return y[:n] + y[n : 2 * n] + y[2 * n :]


def gathered(parts, hot):
    return join3(jnp.dot(parts, hot, preferred_element_type=F32))


def summed(values, hot_t):
    return join3(jnp.dot(split3(values), hot_t, preferred_element_type=F32))


def unpack_group(g, j, recv):
    lane = lane_iota()
    upper = lax.broadcasted_iota(jnp.int32, (8, 128), 0) >= 4
    block_lane = [(lane + 128 * t) % 48 for t in range(3)]
    low = [recv[8 * g + i, j, 0:8, :] for i in range(8)]
    high = [recv[8 * g + i, j, 8:16, :] for i in range(8)]

    def at(tiles, start, width, to):
        return shifted(strip(tiles, lane, start, width), lane, to - start)

    def piece(offset, width, to):
        first, second = at(high, offset, width, to), at(high, offset + 64, width, to)
        return [jnp.where(upper, pltpu.roll(b, 4, 0), a) for a, b in zip(first, second)]

    first, second = at(low, 96, 32, 0), piece(0, 16, 32)
    return [
        at(low, 0, 48, 0),
        at(low, 48, 48, 0),
        [jnp.where(b < 32, f, s) for b, f, s in zip(block_lane, first, second)],
        piece(16, 48, 0),
    ]


def group_targets(g, recv_t):
    lane = lane_iota()
    sub = lax.broadcasted_iota(jnp.int32, (8, 128), 0)
    tile = recv_t[pl.ds(pl.multiple_of(8 * g, 8), 8), :]
    out = [jnp.zeros((8, 128), F32)] * 3
    for i in range(8):
        moved = pltpu.roll(tile, (48 * i - 64) % 128, 1)
        for t in range(3):
            a, b = max(48 * i - 128 * t, 0), min(48 * i + 48 - 128 * t, 128)
            if a < b:
                out[t] = jnp.where((sub == i) & (lane >= a) & (lane < b), moved, out[t])
    return jnp.concatenate([jnp.sum(x, axis=0, keepdims=True) for x in out], 1)


def merge(items):
    sub = lax.broadcasted_iota(jnp.int32, (8, 128), 0)
    items = items[::-1]
    for bit in (0, 1, 2):
        step = 1 << bit
        here = (sub & step) != 0
        items = [
            jnp.where(here, a, b) + pltpu.roll(jnp.where(here, b, a), step, 0)
            for a, b in zip(items[0::2], items[1::2])
        ]
    return items[0]


def merged_rows(rows):
    rows = rows + [jnp.zeros((8, 128), F32)] * (32 - len(rows))
    return jnp.concatenate([merge(rows[k : k + 8]) for k in range(0, 32, 8)], 0)


def pixel_xy(me, j):
    p = me * PX + 8 * j + lax.broadcasted_iota(jnp.int32, (8, 128), 0)
    x = ((p % 64).astype(F32) + 0.5) / 64 - 0.5
    y = ((p // 64).astype(F32) + 0.5 - 24.0) / 64
    return x, y


def expand(rows, own, out):
    lane = lane_iota()
    mine = [
        jnp.where(
            lane < 8,
            pltpu.roll(rows[:, 0:128], (128 - 8 * g) % 128, 1),
            pltpu.roll(rows[:, 128:256], (136 - 8 * g) % 128, 1),
        )
        for g in range(GROUPS)
    ]
    out[...] = gathered(split3(jnp.concatenate(mine, 0)), own[...])


def rows_of(ref, g):
    return ref[pl.ds(pl.multiple_of(8 * g, 8), 8), :]


def edge_rows(a, j):
    return slice(24 * a + 8 * j, 24 * a + 8 * j + 8)


def add_block(acc, row, value):
    acc[row] = value if acc[row] is None else acc[row] + value


def source_columns():
    rows = lax.broadcasted_iota(jnp.int32, (128, LANES), 0)
    frame = lax.broadcasted_iota(jnp.int32, (1, LANES), 1) // 24
    return jnp.where(rows == (frame % 2) * 8 + frame // 2, 1.0, 0.0).astype(BF16)


def source_columns_t():
    edge = lax.broadcasted_iota(jnp.int32, (8 * LANES, 1), 0)
    frame = (edge % LANES) // 24
    lanes = lax.broadcasted_iota(jnp.int32, (8 * LANES, 128), 1)
    at = (edge // LANES) * 16 + (frame % 2) * 8 + frame // 2
    return jnp.where(lanes == at, 1.0, 0.0).astype(BF16)


def build_terms(acc, cols, inputs, d, rel, xy, coup, m, j):
    x, y = xy
    fu, fv, cu, cv = inputs
    w0, w1, w2, m0, m1, m2 = [rel[k : 1 + k, cols] for k in range(6)]
    x0 = x + w1 - w2 * y + m0 * d
    x1 = y + w2 * x - w0 + m1 * d
    x2 = 1.0 + w0 * y - w1 * x + m2 * d
    q = 1.0 / x2
    u = x0 * q
    v = x1 * q
    ru = fu - (u - x)
    rv = fv - (v - y)
    du = q * (m0 - u * m2)
    dv = q * (m1 - v * m2)
    eu = cu * du
    ev = cv * dv
    dq = d * q
    ju = {0: -(u * y) * q, 1: (1.0 + u * x) * q, 2: -y * q, 3: dq, 5: -u * dq}
    jv = {0: (-1.0 - v * y) * q, 1: v * x * q, 2: x * q, 4: dq, 5: -v * dq}
    for a in range(6):
        if a in ju and a in jv:
            e = ju[a] * eu + jv[a] * ev
        else:
            e = ju[a] * eu if a in ju else jv[a] * ev
        coup[m, edge_rows(a, j), cols] = e
    su = {a: cu * ju[a] for a in ju}
    sv = {a: cv * jv[a] for a in jv}
    for (a, b), row in K_PAIRS:
        if a in ju and b in ju:
            add_block(acc, row, su[a] * ju[b])
        if a in jv and b in jv:
            add_block(acc, row, sv[a] * jv[b])
    for a in range(6):
        if a in ju:
            add_block(acc, H_ROW + a, su[a] * ru)
        if a in jv:
            add_block(acc, H_ROW + a, sv[a] * rv)
    return eu * ru + ev * rv, eu * du + ev * dv


def take_terms(acc, cols, near, coup, m, j):
    ci, gi = -near[0], -near[1]
    e = [coup[m, edge_rows(a, j), cols] for a in range(6)]
    for a in range(6):
        scaled = e[a] * ci
        for (k, b), row in K_PAIRS:
            if k == a:
                add_block(acc, row, scaled * e[b])
        add_block(acc, H_ROW + a, e[a] * gi)


def filled(acc):
    return [jnp.zeros((8, 128), F32) if x is None else x for x in acc]


def tile_cols(t):
    return slice(128 * t, 128 * t + 128)


def pair_at(m, count=1):
    size = 2 * LANES * count
    return pl.ds(pl.multiple_of(size * m, 128), size)


def phase_pass(
    m, j, gs, me, recv, recv_t, table3, hot, hot_t, from_pose, dep, rel, coup, sums, inverse3, kh
):
    at = pair_at(m)
    if j == 0:
        rows = lax.broadcasted_iota(jnp.int32, (256, 2 * LANES), 0).astype(F32)
        targets = jnp.concatenate([group_targets(g, recv_t) for g in gs], 1)
        hot[:, at] = jnp.where(rows == targets, 1.0, 0.0).astype(BF16)
        lanes = lane_iota((128, 256)).astype(F32)
        for t in range(6):
            column = jnp.broadcast_to(targets[:, tile_cols(t)], (128, 128)).T
            column = jnp.concatenate([column, column], 1)
            to = pl.ds(pl.multiple_of(2 * LANES * m + 128 * t, 128), 128)
            hot_t[to, :] = jnp.where(lanes == column, 1.0, 0.0).astype(BF16)
        near = gathered(table3[...], hot[:, at])
        dep[m] = near[0:24]
        relative = jnp.concatenate([rows_of(from_pose, g) for g in gs], 1) - near[24:32]
        rel[m] = relative
    else:
        relative = rel[m]
        back = gathered(inverse3[j - 1], hot[:, at])
    parts = [unpack_group(g, j, recv) for g in gs]
    grads, curvs, blocks = [], [], []
    xy = pixel_xy(me, j)
    for t in range(6):
        cols = tile_cols(t)
        acc = [None] * 27
        d = dep[m, 8 * j : 8 * j + 8, cols]
        tiles = [part[t % 3] for part in parts[t // 3]]
        gd, cd = build_terms(acc, cols, tiles, d, relative, xy, coup, m, j)
        grads.append(gd)
        curvs.append(cd)
        if j > 0:
            take_terms(acc, cols, (back[0:8, cols], back[8:16, cols]), coup, m, j - 1)
        blocks.append(merged_rows(filled(acc)))
    both = jnp.concatenate([jnp.concatenate(grads, 1), jnp.concatenate(curvs, 1)], 0)
    sums[j] += summed(both, hot_t[at, :])
    block = jnp.concatenate(blocks, 1)
    kh[m] = block if j == 0 else kh[m] + block


def last_pass(h, hot, hot_t, own_t, coup, inverse3, kh, total_s, total_t):
    at = pair_at(h, 4)
    near = gathered(inverse3[2], hot[:, at])
    blocks = []
    for t in range(24):
        m = 4 * h + t // 6
        acc = [None] * 27
        cols = tile_cols(t)
        take_terms(acc, tile_cols(t % 6), (near[0:8, cols], near[8:16, cols]), coup, m, 2)
        blocks.append(kh[m, :, tile_cols(t % 6)] + merged_rows(acc))
    parts = split3(jnp.concatenate(blocks, 1))
    total_t[...] += join3(jnp.dot(parts, hot_t[at, :], preferred_element_type=F32))
    total_s[h] = join3(jnp.dot(parts, own_t[...], preferred_element_type=F32))


def third_pass(h, gs, hot_t, coup, from_steps, fix):
    parts = []
    for t in range(24):
        m, cols = 4 * h + t // 6, tile_cols(t % 6)
        motion = rows_of(from_steps, gs[t // 3])
        column = []
        for j in range(3):
            terms = [
                coup[m, edge_rows(a, j), cols] * motion[a : a + 1, tile_cols(t % 3)]
                for a in range(6)
            ]
            column.append(((terms[0] + terms[1]) + (terms[2] + terms[3])) + (terms[4] + terms[5]))
        parts.append(jnp.concatenate(column, 0))
    fix[...] += summed(jnp.concatenate(parts, 1), hot_t[pair_at(h, 4), :])


def solve(matrix, right):
    factor = {}
    for i in range(6):
        for j in range(i + 1):
            e = matrix(i, j)
            if i == j:
                e = e * 1.1 + 0.001
            for k in range(j):
                e = e - factor[i, k] * factor[j, k]
            factor[i, j] = jnp.sqrt(e) if i == j else e / factor[j, j]
    forward = []
    for i in range(6):
        e = right(i)
        for k in range(i):
            e = e - factor[i, k] * forward[k]
        forward.append(e / factor[i, i])
    z = [None] * 6
    for i in reversed(range(6)):
        e = forward[i]
        for k in range(i + 1, 6):
            e = e - factor[k, i] * z[k]
        z[i] = e / factor[i, i]
    return z


def ring_steps(d):
    return min(d, 4 - d)


def far_first():
    offsets = [
        (dz, dy, dx, dc)
        for dz in range(4)
        for dy in range(4)
        for dx in range(4)
        for dc in range(2)
        if (dz, dy, dx, dc) != (0, 0, 0, 0)
    ]
    return sorted(offsets, key=lambda o: -(ring_steps(o[0]) + ring_steps(o[1]) + ring_steps(o[2])))


def group_offset(n):
    return (n // 4 + n) % 4, n % 4


def by_group():
    order = []
    for n in range(GROUPS):
        oz, oy = group_offset(n)
        for dx in range(4):
            for dc in range(2):
                order.append(((oz + dx) % 4, (oy + dx) % 4, dx, dc))
    return order[1:]


def to_all(order, act):
    row, col = lax.axis_index("row"), lax.axis_index("col")
    y, x = col // 8, (col // 2) % 4
    zs = [((row + d) % 4) * 32 for d in range(4)]
    ys = [((y + d) % 4) * 8 for d in range(4)]
    xs = [((x + d) % 4) * 2 for d in range(4)]
    cs = [(col + d) % 2 for d in range(2)]
    gz = [((row + 4 - x + d) % 4) * 32 for d in range(4)]
    gy = [((y + 4 - x + d) % 4) * 8 for d in range(4)]
    for dz, dy, dx, dc in order:
        last = xs[dx] + cs[dc]
        act(zs[dz] + ys[dy] + last, gz[(dz - dx) % 4] + gy[(dy - dx) % 4] + last)


def slot_of(d):
    return (d % 16) * 8 + d // 16


def rows_exchange(send, recv, source, slot, send_sem, recv_sem):
    def act(d, place):
        pltpu.make_async_remote_copy(
            src_ref=send.at[pl.ds(source(d, place), 1), :],
            dst_ref=recv.at[pl.ds(slot, 1), :],
            send_sem=send_sem,
            recv_sem=recv_sem,
            device_id=d,
            device_id_type=pl.DeviceIdType.LOGICAL,
        ).start()

    to_all(far_first(), act)


def rows_wait(buf, sem):
    ref = buf.at[pl.ds(0, NDEV - 1), :]
    pltpu.make_async_copy(ref, ref, sem).wait()


def scope(name):
    return contextlib.nullcontext()


def loop(body, count):
    def step(n, carry):
        body(n)
        return carry

    lax.fori_loop(0, count, step, 0)


def main_kernel(
    flow_hbm, weight_hbm, depth_hbm, target_hbm, rotation_hbm, translation_hbm,
    out_ref, pose_ref,
    flow, weight, depth_ref, target_ref, rotation_ref, translation_ref, low, high, chunks, ints, floats, unfold,
    recv, table, table3, hot, hot_t, own, own_t, from_pose, dep, rel, coup, sums, inverse,
    inverse3, kh,
    total_s, total_t, at_target, steps, from_steps, fix,
    send_t, recv_t, send_d, recv_d, send_e, recv_e, send_f, recv_f,
    in_sem, big_send, big_recv, small_send, small_recv,
):
    row, col = lax.axis_index("row"), lax.axis_index("col")
    me = row * 32 + col
    y, x = col // 8, (col // 2) % 4
    my_gz, my_gy = (row + 4 - x) % 4, (y + 4 - x) % 4
    my_group = my_gz * 4 + my_gy
    mine_at = my_group * 8 + col % 8
    lane = lane_iota()
    barrier = pltpu.get_barrier_semaphore()

    inputs = [
        (depth_hbm, depth_ref),
        (target_hbm, target_ref),
        (rotation_hbm, rotation_ref),
        (translation_hbm, translation_ref),
        (flow_hbm, flow),
        (weight_hbm, weight),
    ]
    loads = [
        pltpu.make_async_copy(source, to, in_sem.at[k]) for k, (source, to) in enumerate(inputs)
    ]

    def greet(d, _):
        pl.semaphore_signal(
            barrier, inc=1, device_id=d, device_id_type=pl.DeviceIdType.LOGICAL
        )

    with scope("sc_greet"):
        for load in loads:
            load.start()
        to_all(far_first(), greet)

    with scope("sc_tables"):
        high[...] = jnp.zeros_like(high)
        for load in loads[:4]:
            load.wait()
        column, pose = own_edges(target_ref, rotation_ref, translation_ref, ints, floats)
        pack_tables(depth_ref, column, pose, unfold, send_t)
        recv_t[pl.ds(mine_at, 1), :] = send_t[pl.ds(slot_of(me), 1), :]
        turn = col % 8
        for load in loads[4:]:
            load.wait()

    def pack(n, carry):
        pack_block(n, turn, flow, weight, low, high, chunks)
        return carry

    with scope("sc_pack"):
        lax.fori_loop(0, 8, pack, 0)
    with scope("sc_barrier"):
        pl.semaphore_wait(barrier, NDEV - 1)

    with scope("sc_sends"):
        rows_exchange(
            send_t, recv_t, lambda d, _: slot_of(d), mine_at, small_send.at[3], small_recv.at[3]
        )

        for j in range(3):

            def send_chunk(d, _):
                pltpu.make_async_remote_copy(
                    src_ref=chunks.at[d, j, pl.ds(0, 12), :],
                    dst_ref=recv.at[mine_at, j, pl.ds(0, 12), :],
                    send_sem=big_send,
                    recv_sem=big_recv.at[j, my_group],
                    device_id=d,
                    device_id_type=pl.DeviceIdType.LOGICAL,
                ).start()

            to_all(by_group(), send_chunk)
        recv[mine_at, :, 0:12, :] = chunks[me, :, 0:12, :]

    with scope("sc_waitt"):
        for ref in (sums, total_t, fix, at_target):
            ref[...] = jnp.zeros_like(ref)
        own[...] = source_columns()
        own_t[...] = source_columns_t()
        rows_wait(recv_t, small_recv.at[3])
        known = recv_t[...].T
        for f in range(2):
            at = slice(128 * f, 128 * f + 128)
            table[0:24, at] = known[24 * f : 24 * f + 24]
            table[24:32, at] = known[48 + 8 * f : 56 + 8 * f]
        table3[...] = split3(table[...])
        expand(table[24:32, :], own, from_pose)

    def group_at(n):
        oz, oy = group_offset(n)
        return ((my_gz + 4 - oz) % 4) * 4 + (my_gy + 4 - oy) % 4

    def arrive(m, j):
        gs = [group_at(2 * m), group_at(2 * m + 1)]

        def landed(g, count):
            ref = recv.at[pl.ds(8 * g, count), j, pl.ds(0, 12), :]
            pltpu.make_async_copy(ref, ref, big_recv.at[j, g]).wait()

        pl.when(m == 0)(lambda: landed(gs[0], 7))
        pl.when(m != 0)(lambda: landed(gs[0], 8))
        landed(gs[1], 8)
        phase_pass(
            m, j, gs, me, recv, recv_t, table3, hot, hot_t, from_pose, dep, rel, coup, sums,
            inverse3, kh,
        )

    for j in range(3):
        with scope(f"sc_arrive{j}"):
            loop(functools.partial(arrive, j=j), 8)
            ci = 1.0 / (0.1 + sums[j, 8:16])
            both = jnp.concatenate([ci, sums[j, 0:8] * ci], 0)
            inverse[j] = both
            inverse3[j] = split3(both)
    with scope("sc_last"):
        loop(lambda h: last_pass(h, hot, hot_t, own_t, coup, inverse3, kh, total_s, total_t), 2)

    with scope("sc_sendd"):
        kind = lax.broadcasted_iota(jnp.int32, (32, 256), 0)
        total = jnp.where(kind < H_ROW, total_t[...], -total_t[...])
        send_d[...] = jnp.concatenate(
            [total[:, 0:128], total[:, 128:256], jnp.zeros((64, 128), F32)], 0
        ).T
        for h in range(2):
            by_source = jnp.concatenate([total_s[h], jnp.zeros((96, 128), F32)], 0).T
            for k in range(8):
                to = pl.ds(pl.multiple_of(8 * group_at(8 * h + k), 8), 8)
                first, second = by_source[16 * k : 16 * k + 8], by_source[16 * k + 8 : 16 * k + 16]
                send_d[to, :] += first + pltpu.roll(second, 32, 1)
        recv_d[pl.ds(mine_at, 1), :] = send_d[pl.ds(mine_at, 1), :]
        rows_exchange(
            send_d, recv_d, lambda _, place: place, mine_at, small_send.at[0], small_recv.at[0]
        )
    with scope("sc_target"):

        def couple(m):
            at_target[...] += summed(coup[m], hot_t[pair_at(m), :])

        loop(couple, 8)
    with scope("sc_waitd"):
        rows_wait(recv_d, small_recv.at[0])
    with scope("sc_solve"):
        line = jnp.sum(recv_d[...], axis=0, keepdims=True)
        sub = lax.broadcasted_iota(jnp.int32, (8, 128), 0)
        lines = jnp.broadcast_to(line, (8, 128))
        lines = jnp.where(sub == 1, pltpu.roll(lines, 96, 1), lines)
        full = jnp.concatenate([lines, jnp.zeros((120, 128), F32)], 0).T
        z = solve(
            lambda i, j: full[K_INDEX[i, j] : K_INDEX[i, j] + 1, :],
            lambda i: full[H_ROW + i : H_ROW + i + 1, :],
        )
        zs = jnp.concatenate([*z, jnp.zeros((122, 128), F32)], 0)
        turned = zs.T
        pose_ref[...] = turned[0:2, 0:6]
        mine = turned[0:1] + pltpu.roll(turned[0:8], 8, 1)[1:2]
        send_e[...] = jnp.broadcast_to(mine, (8, 128))
        recv_e[pl.ds(mine_at, 1), :] = mine
    with scope("sc_sende"):
        rows_exchange(
            send_e, recv_e, lambda d, _: 0, mine_at, small_send.at[1], small_recv.at[1]
        )
    with scope("sc_waite"):
        rows_wait(recv_e, small_recv.at[1])
    with scope("sc_third"):
        every = recv_e[...].T
        steps[:, 0:128] = every[0:8]
        steps[:, 128:256] = every[8:16]
        expand(steps[...], own, from_steps)
        loop(
            lambda h: third_pass(
                h, [group_at(8 * h + k) for k in range(8)], hot_t, coup, from_steps, fix
            ),
            2,
        )
    with scope("sc_sendf"):
        back = at_target[0:24] * steps[0:1]
        for a in range(1, 6):
            back += at_target[24 * a : 24 * a + 24] * steps[a : a + 1]
        grad = jnp.concatenate([sums[j, 0:8] for j in range(3)], 0)
        ci = jnp.concatenate([inverse[j, 0:8] for j in range(3)], 0)
        new = table[0:24] + (grad - (fix[...] - back)) * ci
        zero8 = jnp.zeros((8, 128), F32)
        send_f[...] = jnp.concatenate(
            [new[:, 0:128], zero8, new[:, 128:256], zero8, jnp.zeros((64, 128), F32)], 0
        ).T
        slot = slot_of(me)
        recv_f[pl.ds(slot, 1), :] = send_f[pl.ds(mine_at, 1), :]
        rows_exchange(
            send_f, recv_f, lambda _, place: place, slot, small_send.at[2], small_recv.at[2]
        )
    with scope("sc_waitf"):
        rows_wait(recv_f, small_recv.at[2])
    for f in range(2):
        tiles = [None] * 3
        for i in range(16):
            piece = recv_f[8 * i : 8 * i + 8, :]
            first = 24 * i
            moved = pltpu.roll(piece, (first - 32 * f) % 128, 1)
            for t in range(3):
                a, b = max(first - 128 * t, 0), min(first + 24 - 128 * t, 128)
                if a < b:
                    if tiles[t] is None:
                        tiles[t] = moved
                    else:
                        tiles[t] = jnp.where((lane >= a) & (lane < b), moved, tiles[t])
        for g in range(8):
            for t in range(3):
                at = 384 * g + 128 * t
                out_ref[f : f + 1, at : at + 128] = tiles[t][g : g + 1]

    ref = chunks.at[pl.ds(0, NDEV - 1), :, pl.ds(0, 12), :]
    pltpu.make_async_copy(ref, ref, big_send).wait()
    rows_wait(recv_t, small_send.at[3])
    rows_wait(recv_d, small_send.at[0])
    rows_wait(recv_e, small_send.at[1])
    rows_wait(recv_f, small_send.at[2])


def run_main(flow, weight, inv_depth, edge_target, rotation, translation):
    v = pltpu.VMEM
    vmem = pl.BlockSpec(memory_space=pltpu.VMEM)
    hbm = pl.BlockSpec(memory_space=pltpu.HBM)
    return pl.pallas_call(
        main_kernel,
        in_specs=[hbm] * 6,
        out_specs=[vmem] * 2,
        out_shape=[
            jax.ShapeDtypeStruct((2, PX * NDEV), F32),
            jax.ShapeDtypeStruct((2, 6), F32),
        ],
        scratch_shapes=[
            v((2, 48, PX * NDEV), F32),
            v((2, 48, PX * NDEV), F32),
            v((2, PX * NDEV), F32),
            v((2, 24), jnp.int32),
            v((2, 3), F32),
            v((2, 3), F32),
            v((128, LANES), F32),
            v((128, LANES), F32),
            v((NDEV, 3, 16, 128), F32),
            v((8, 128), jnp.int32),
            v((2, 8, 128), F32),
            v((2, 8, LANES), F32),
            v((NDEV, 3, 16, 128), F32),
            v((32, 256), F32),
            v((96, 256), BF16),
            v((256, GROUPS * LANES), BF16),
            v((GROUPS * LANES, 256), BF16),
            v((128, LANES), BF16),
            v((8 * LANES, 128), BF16),
            v((128, LANES), F32),
            v((8, 24, 2 * LANES), F32),
            v((8, 8, 2 * LANES), F32),
            v((8, 144, 2 * LANES), F32),
            v((3, 16, 256), F32),
            v((3, 16, 256), F32),
            v((3, 48, 256), BF16),
            v((8, 32, 2 * LANES), F32),
            v((2, 32, 128), F32),
            v((32, 256), F32),
            v((144, 256), F32),
            v((8, 256), F32),
            v((128, LANES), F32),
            v((24, 256), F32),
            v((128, 128), F32),
            v((128, 128), F32),
            v((128, 128), F32),
            v((128, 128), F32),
            v((8, 128), F32),
            v((128, 128), F32),
            v((128, 128), F32),
            v((128, 128), F32),
            pltpu.SemaphoreType.DMA((6,)),
            pltpu.SemaphoreType.DMA,
            pltpu.SemaphoreType.DMA((3, GROUPS)),
            pltpu.SemaphoreType.DMA((4,)),
            pltpu.SemaphoreType.DMA((4,)),
        ],
        compiler_params=pltpu.CompilerParams(
            collective_id=0, has_side_effects=True, vmem_limit_bytes=56 * 1024 * 1024
        ),
        name="step",
    )(flow, weight, inv_depth, edge_target, rotation, translation)


def shards(inv_depth, rotation, translation, edge_target, flow_obs, weight):
    pixels = inv_depth.shape[1]
    flow = flow_obs.reshape(2, 48, pixels)
    wts = weight.reshape(2, 48, pixels)
    depth, pose = run_main(flow, wts, inv_depth, edge_target, rotation.T, translation.T)
    return depth, pose.T


def solution(mesh):
    in_specs = (
        P(("row", "col"), None),
        P(None, ("row", "col")),
        P(None, ("row", "col")),
        P(("row", "col"), None),
        P(None, ("row", "col"), None, None),
        P(None, ("row", "col"), None, None),
    )
    out_specs = (P(("row", "col"), None), P(None, ("row", "col")))
    return jax.shard_map(
        shards, mesh=mesh, in_specs=in_specs, out_specs=out_specs, check_vma=False
    )
```

```python
import contextlib
import functools

import jax
import jax.numpy as jnp
from jax import lax
from jax.experimental import pallas as pl
from jax.experimental.pallas import tpu as pltpu
from jax.sharding import PartitionSpec as P

F32 = jnp.float32
BF16 = jnp.bfloat16
NDEV = 128
PX = 24
GROUPS = 16
LANES = 384
MESH = pl.DeviceIdType.MESH
K_PAIRS = [((a, b), n) for n, (a, b) in enumerate((a, b) for a in range(6) for b in range(a, 6))]
K_INDEX = {**dict(K_PAIRS), **{(b, a): n for (a, b), n in K_PAIRS}}
H_ROW = 21


def lane_iota(shape=(8, 128)):
    return lax.broadcasted_iota(jnp.int32, shape, 1)


def pack_block(n, turn, flow, weight, low, high, out):
    cols = pl.ds(pl.multiple_of(n * LANES, 128), LANES)

    def put(ref, block, value):
        at = pl.multiple_of(((3 * turn + block) % 8) * 16, 16)
        ref[pl.ds(at, 16), :] = value

    for k in range(3):
        put(low, k, flow[0, 16 * k : 16 * k + 16, cols])
        put(low, 3 + k, flow[1, 16 * k : 16 * k + 16, cols])
        put(high, 1 + k, weight[1, 16 * k : 16 * k + 16, cols])
    put(low, 6, weight[0, 0:16, cols])
    put(low, 7, weight[0, 16:32, cols])
    put(high, 0, weight[0, 32:48, cols])
    low_t = low[...].T
    high_t = high[...].T
    where_at = (lane_iota() - 48 * turn + 384) % 128
    for d in range(16):
        for j in range(3):
            at = 24 * d + 8 * j
            out[16 * n + d, j, 0:8, :] = low_t[at : at + 8]
            rest = high_t[at : at + 8]
            turned = pltpu.roll(pltpu.roll(rest, 64, 1), 4, 0)
            out[16 * n + d, j, 8:12, :] = jnp.where(where_at < 64, rest, turned)[0:4]


def own_edges(target_ref, rotation_ref, translation_ref, ints, floats):
    lane = lane_iota()
    ints[...] = jnp.zeros_like(ints)
    ints[0:2, 0:24] = target_ref[...]
    both = ints[...]
    target = jnp.where(lane < 24, both[0:1], pltpu.roll(both, 24, 1)[1:2])
    x, y, z = (target >> 2) & 3, (target >> 4) & 3, target >> 6
    group = (((z - x) & 3) << 2) + ((y - x) & 3)
    column = ((target & 1) << 7) + (group << 3) + ((target >> 1) & 7)
    floats[...] = jnp.zeros_like(floats)
    floats[0, 0:2, 0:3] = rotation_ref[...]
    floats[1, 0:2, 0:3] = translation_ref[...]
    return column.astype(F32), floats[0] + pltpu.roll(floats[1], 3, 1)


def pack_tables(depth_ref, column, pose, unfold, send):
    lane = lane_iota()
    poses = pltpu.roll(pose, 48, 1)[0:1] + pltpu.roll(pose, 56, 1)[1:2]
    known = jnp.where(lane < 64, poses, pltpu.roll(column, 64, 1)[0:1])
    for f in range(2):
        for g in range(8):
            unfold[f, g : g + 1, :] = depth_ref[f : f + 1, LANES * g : LANES * g + LANES]
    for i in range(16):
        acc = known
        for f in range(2):
            for t in range(3):
                a, b = max(24 * i - 128 * t, 0), min(24 * i + 24 - 128 * t, 128)
                if a < b:
                    shift = 24 * f - (24 * i - 128 * t)
                    moved = pltpu.roll(unfold[f, :, 128 * t : 128 * t + 128], shift % 128, 1)
                    acc = jnp.where((lane >= a + shift) & (lane < b + shift), moved, acc)
        send[8 * i : 8 * i + 8, :] = acc


def strip(tiles, lane, offset, width):
    out = []
    for t in range(3):
        acc = None
        for i in range(8):
            start = 48 * i + offset
            for wrap in (0, 384, 768):
                a = max(start - wrap, 128 * t) - 128 * t
                b = min(start + width - wrap, 128 * t + 128) - 128 * t
                if a < b:
                    if acc is None:
                        acc = tiles[i]
                    else:
                        acc = jnp.where((lane >= a) & (lane < b), tiles[i], acc)
        out.append(acc)
    return out


def shifted(tiles, lane, shift):
    whole, part = divmod(shift % 384, 128)
    if part == 0:
        return [tiles[(t - whole) % 3] for t in range(3)]
    rolled = [pltpu.roll(t, part, 1) for t in tiles]
    return [
        jnp.where(lane < part, rolled[(t - whole - 1) % 3], rolled[(t - whole) % 3])
        for t in range(3)
    ]


def split3(x):
    top = x.astype(BF16).astype(F32)
    rest = x - top
    mid = rest.astype(BF16).astype(F32)
    return jnp.concatenate([top, mid, rest - mid], 0).astype(BF16)


def join3(y):
    n = y.shape[0] // 3
    return y[:n] + y[n : 2 * n] + y[2 * n :]


def gathered(parts, hot):
    return join3(jnp.dot(parts, hot, preferred_element_type=F32))


def summed(values, hot_t):
    return join3(jnp.dot(split3(values), hot_t, preferred_element_type=F32))


def unpack_group(g, j, recv):
    lane = lane_iota()
    upper = lax.broadcasted_iota(jnp.int32, (8, 128), 0) >= 4
    block_lane = [(lane + 128 * t) % 48 for t in range(3)]
    low = [recv[8 * g + i, j, 0:8, :] for i in range(8)]
    high = [recv[8 * g + i, j, 8:16, :] for i in range(8)]

    def at(tiles, start, width, to):
        return shifted(strip(tiles, lane, start, width), lane, to - start)

    def piece(offset, width, to):
        first, second = at(high, offset, width, to), at(high, offset + 64, width, to)
        return [jnp.where(upper, pltpu.roll(b, 4, 0), a) for a, b in zip(first, second)]

    first, second = at(low, 96, 32, 0), piece(0, 16, 32)
    return [
        at(low, 0, 48, 0),
        at(low, 48, 48, 0),
        [jnp.where(b < 32, f, s) for b, f, s in zip(block_lane, first, second)],
        piece(16, 48, 0),
    ]


def group_targets(g, recv_t):
    lane = lane_iota()
    sub = lax.broadcasted_iota(jnp.int32, (8, 128), 0)
    tile = recv_t[pl.ds(pl.multiple_of(8 * g, 8), 8), :]
    out = [jnp.zeros((8, 128), F32)] * 3
    for i in range(8):
        moved = pltpu.roll(tile, (48 * i - 64) % 128, 1)
        for t in range(3):
            a, b = max(48 * i - 128 * t, 0), min(48 * i + 48 - 128 * t, 128)
            if a < b:
                out[t] = jnp.where((sub == i) & (lane >= a) & (lane < b), moved, out[t])
    return jnp.concatenate([jnp.sum(x, axis=0, keepdims=True) for x in out], 1)


def merge(items):
    sub = lax.broadcasted_iota(jnp.int32, (8, 128), 0)
    items = items[::-1]
    for bit in (0, 1, 2):
        step = 1 << bit
        here = (sub & step) != 0
        items = [
            jnp.where(here, a, b) + pltpu.roll(jnp.where(here, b, a), step, 0)
            for a, b in zip(items[0::2], items[1::2])
        ]
    return items[0]


def merged_rows(rows):
    rows = rows + [jnp.zeros((8, 128), F32)] * (32 - len(rows))
    return jnp.concatenate([merge(rows[k : k + 8]) for k in range(0, 32, 8)], 0)


def pixel_xy(me, j):
    p = me * PX + 8 * j + lax.broadcasted_iota(jnp.int32, (8, 128), 0)
    x = ((p % 64).astype(F32) + 0.5) / 64 - 0.5
    y = ((p // 64).astype(F32) + 0.5 - 24.0) / 64
    return x, y


def expand(rows, own, out):
    lane = lane_iota()
    mine = [
        jnp.where(
            lane < 8,
            pltpu.roll(rows[:, 0:128], (128 - 8 * g) % 128, 1),
            pltpu.roll(rows[:, 128:256], (136 - 8 * g) % 128, 1),
        )
        for g in range(GROUPS)
    ]
    out[...] = gathered(split3(jnp.concatenate(mine, 0)), own[...])


def rows_of(ref, g):
    return ref[pl.ds(pl.multiple_of(8 * g, 8), 8), :]


def edge_rows(a, j):
    return slice(24 * a + 8 * j, 24 * a + 8 * j + 8)


def add_block(acc, row, value):
    acc[row] = value if acc[row] is None else acc[row] + value


def source_columns():
    rows = lax.broadcasted_iota(jnp.int32, (128, LANES), 0)
    frame = lax.broadcasted_iota(jnp.int32, (1, LANES), 1) // 24
    return jnp.where(rows == (frame % 2) * 8 + frame // 2, 1.0, 0.0).astype(BF16)


def source_columns_t():
    edge = lax.broadcasted_iota(jnp.int32, (8 * LANES, 1), 0)
    frame = (edge % LANES) // 24
    lanes = lax.broadcasted_iota(jnp.int32, (8 * LANES, 128), 1)
    at = (edge // LANES) * 16 + (frame % 2) * 8 + frame // 2
    return jnp.where(lanes == at, 1.0, 0.0).astype(BF16)


def build_terms(acc, cols, inputs, d, rel, xy, coup, m, j):
    x, y = xy
    fu, fv, cu, cv = inputs
    w0, w1, w2, m0, m1, m2 = [rel[k : 1 + k, cols] for k in range(6)]
    x0 = x + w1 - w2 * y + m0 * d
    x1 = y + w2 * x - w0 + m1 * d
    x2 = 1.0 + w0 * y - w1 * x + m2 * d
    q = 1.0 / x2
    u = x0 * q
    v = x1 * q
    ru = fu - (u - x)
    rv = fv - (v - y)
    du = q * (m0 - u * m2)
    dv = q * (m1 - v * m2)
    eu = cu * du
    ev = cv * dv
    dq = d * q
    ju = {0: -(u * y) * q, 1: (1.0 + u * x) * q, 2: -y * q, 3: dq, 5: -u * dq}
    jv = {0: (-1.0 - v * y) * q, 1: v * x * q, 2: x * q, 4: dq, 5: -v * dq}
    for a in range(6):
        if a in ju and a in jv:
            e = ju[a] * eu + jv[a] * ev
        else:
            e = ju[a] * eu if a in ju else jv[a] * ev
        coup[m, edge_rows(a, j), cols] = e
    su = {a: cu * ju[a] for a in ju}
    sv = {a: cv * jv[a] for a in jv}
    for (a, b), row in K_PAIRS:
        if a in ju and b in ju:
            add_block(acc, row, su[a] * ju[b])
        if a in jv and b in jv:
            add_block(acc, row, sv[a] * jv[b])
    for a in range(6):
        if a in ju:
            add_block(acc, H_ROW + a, su[a] * ru)
        if a in jv:
            add_block(acc, H_ROW + a, sv[a] * rv)
    return eu * ru + ev * rv, eu * du + ev * dv


def take_terms(acc, cols, near, coup, m, j):
    ci, gi = -near[0], -near[1]
    e = [coup[m, edge_rows(a, j), cols] for a in range(6)]
    for a in range(6):
        scaled = e[a] * ci
        for (k, b), row in K_PAIRS:
            if k == a:
                add_block(acc, row, scaled * e[b])
        add_block(acc, H_ROW + a, e[a] * gi)


def filled(acc):
    return [jnp.zeros((8, 128), F32) if x is None else x for x in acc]


def tile_cols(t):
    return slice(128 * t, 128 * t + 128)


def pair_at(m, count=1):
    size = 2 * LANES * count
    return pl.ds(pl.multiple_of(size * m, 128), size)


def phase_pass(
    m, j, gs, me, recv, recv_t, table3, hot, hot_t, from_pose, dep, rel, coup, sums, inverse3, kh
):
    at = pair_at(m)
    if j == 0:
        rows = lax.broadcasted_iota(jnp.int32, (256, 2 * LANES), 0).astype(F32)
        targets = jnp.concatenate([group_targets(g, recv_t) for g in gs], 1)
        hot[:, at] = jnp.where(rows == targets, 1.0, 0.0).astype(BF16)
        lanes = lane_iota((128, 256)).astype(F32)
        for t in range(6):
            column = jnp.broadcast_to(targets[:, tile_cols(t)], (128, 128)).T
            column = jnp.concatenate([column, column], 1)
            to = pl.ds(pl.multiple_of(2 * LANES * m + 128 * t, 128), 128)
            hot_t[to, :] = jnp.where(lanes == column, 1.0, 0.0).astype(BF16)
        near = gathered(table3[...], hot[:, at])
        dep[m] = near[0:24]
        relative = jnp.concatenate([rows_of(from_pose, g) for g in gs], 1) - near[24:32]
        rel[m] = relative
    else:
        relative = rel[m]
        back = gathered(inverse3[j - 1], hot[:, at])
    parts = [unpack_group(g, j, recv) for g in gs]
    grads, curvs, blocks = [], [], []
    xy = pixel_xy(me, j)
    for t in range(6):
        cols = tile_cols(t)
        acc = [None] * 27
        d = dep[m, 8 * j : 8 * j + 8, cols]
        tiles = [part[t % 3] for part in parts[t // 3]]
        gd, cd = build_terms(acc, cols, tiles, d, relative, xy, coup, m, j)
        grads.append(gd)
        curvs.append(cd)
        if j > 0:
            take_terms(acc, cols, (back[0:8, cols], back[8:16, cols]), coup, m, j - 1)
        blocks.append(merged_rows(filled(acc)))
    both = jnp.concatenate([jnp.concatenate(grads, 1), jnp.concatenate(curvs, 1)], 0)
    sums[j] += summed(both, hot_t[at, :])
    block = jnp.concatenate(blocks, 1)
    kh[m] = block if j == 0 else kh[m] + block


def last_pass(h, hot, hot_t, own_t, coup, inverse3, kh, total_s, total_t):
    at = pair_at(h, 4)
    near = gathered(inverse3[2], hot[:, at])
    blocks = []
    for t in range(24):
        m = 4 * h + t // 6
        acc = [None] * 27
        cols = tile_cols(t)
        take_terms(acc, tile_cols(t % 6), (near[0:8, cols], near[8:16, cols]), coup, m, 2)
        blocks.append(kh[m, :, tile_cols(t % 6)] + merged_rows(acc))
    parts = split3(jnp.concatenate(blocks, 1))
    total_t[...] += join3(jnp.dot(parts, hot_t[at, :], preferred_element_type=F32))
    total_s[h] = join3(jnp.dot(parts, own_t[...], preferred_element_type=F32))


def third_pass(h, gs, hot_t, coup, from_steps, fix):
    parts = []
    for t in range(24):
        m, cols = 4 * h + t // 6, tile_cols(t % 6)
        motion = rows_of(from_steps, gs[t // 3])
        column = []
        for j in range(3):
            terms = [
                coup[m, edge_rows(a, j), cols] * motion[a : a + 1, tile_cols(t % 3)]
                for a in range(6)
            ]
            column.append(((terms[0] + terms[1]) + (terms[2] + terms[3])) + (terms[4] + terms[5]))
        parts.append(jnp.concatenate(column, 0))
    fix[...] += summed(jnp.concatenate(parts, 1), hot_t[pair_at(h, 4), :])


def solve(matrix, right):
    factor = {}
    for i in range(6):
        for j in range(i + 1):
            e = matrix(i, j)
            if i == j:
                e = e * 1.1 + 0.001
            for k in range(j):
                e = e - factor[i, k] * factor[j, k]
            factor[i, j] = jnp.sqrt(e) if i == j else e / factor[j, j]
    forward = []
    for i in range(6):
        e = right(i)
        for k in range(i):
            e = e - factor[i, k] * forward[k]
        forward.append(e / factor[i, i])
    z = [None] * 6
    for i in reversed(range(6)):
        e = forward[i]
        for k in range(i + 1, 6):
            e = e - factor[k, i] * z[k]
        z[i] = e / factor[i, i]
    return z


def ring_steps(d):
    return min(d, 4 - d)


def hops(offset):
    return ring_steps(offset[0]) + ring_steps(offset[1]) + ring_steps(offset[2])


def far_first():
    offsets = [
        (dz, dy, dx, dc)
        for dz in range(4)
        for dy in range(4)
        for dx in range(4)
        for dc in range(2)
        if (dz, dy, dx, dc) != (0, 0, 0, 0)
    ]
    return sorted(offsets, key=lambda o: -hops(o))


def group_offset(n):
    return (n // 4 + n) % 4, n % 4


def by_group(far_ahead=False):
    order = []
    for n in range(GROUPS):
        oz, oy = group_offset(n)
        members = [
            ((oz + dx) % 4, (oy + dx) % 4, dx, dc) for dx in range(4) for dc in range(2)
        ]
        order += sorted(members, key=lambda o: -hops(o)) if far_ahead else members
    return [o for o in order if o != (0, 0, 0, 0)]


def to_all(order, act):
    row, col = lax.axis_index("row"), lax.axis_index("col")
    y, x = col // 8, (col // 2) % 4
    zs = [((row + d) % 4) * 32 for d in range(4)]
    ys = [((y + d) % 4) * 8 for d in range(4)]
    xs = [((x + d) % 4) * 2 for d in range(4)]
    cs = [(col + d) % 2 for d in range(2)]
    gz = [((row + 4 - x + d) % 4) * 32 for d in range(4)]
    gy = [((y + 4 - x + d) % 4) * 8 for d in range(4)]
    for dz, dy, dx, dc in order:
        last = xs[dx] + cs[dc]
        act(zs[dz] + ys[dy] + last, gz[(dz - dx) % 4] + gy[(dy - dx) % 4] + last)


def slot_of(d):
    return (d % 16) * 8 + d // 16


def rows_exchange(send, recv, source, slot, send_sem, recv_sem):
    def act(d, place):
        pltpu.make_async_remote_copy(
            src_ref=send.at[pl.ds(source(d, place), 1), :],
            dst_ref=recv.at[pl.ds(slot, 1), :],
            send_sem=send_sem,
            recv_sem=recv_sem,
            device_id=d,
            device_id_type=pl.DeviceIdType.LOGICAL,
        ).start()

    to_all(far_first(), act)


def steps_exchange(order, send, source, recv, slot, send_sem, recv_sem):
    def act(d, _):
        pltpu.make_async_remote_copy(
            src_ref=send.at[pl.ds(source, 1), :],
            dst_ref=recv.at[pl.ds(slot, 1), :],
            send_sem=send_sem,
            recv_sem=recv_sem,
            device_id=d,
            device_id_type=pl.DeviceIdType.LOGICAL,
        ).start()

    to_all(order, act)


def rows_wait(buf, sem, count=NDEV - 1):
    ref = buf.at[pl.ds(0, count), :]
    pltpu.make_async_copy(ref, ref, sem).wait()


def scope(name):
    return contextlib.nullcontext()


def loop(body, count):
    def step(n, carry):
        body(n)
        return carry

    lax.fori_loop(0, count, step, 0)


def main_kernel(
    flow_hbm, weight_hbm, depth_hbm, target_hbm, rotation_hbm, translation_hbm,
    out_ref, pose_ref,
    flow, weight, depth_ref, target_ref, rotation_ref, translation_ref, low, high, chunks, ints, floats, unfold,
    recv, table, table3, hot, hot_t, own, own_t, from_pose, dep, rel, coup, sums, inverse,
    inverse3, kh,
    total_s, total_t, at_target, steps, from_steps, fix,
    send_t, recv_t, sum_d, send_d, recv_d, send_e, recv_e, send_f, recv_f,
    in_sem, big_send, big_recv, small_send, small_recv,
):
    row, col = lax.axis_index("row"), lax.axis_index("col")
    me = row * 32 + col
    y, x = col // 8, (col // 2) % 4
    my_gz, my_gy = (row + 4 - x) % 4, (y + 4 - x) % 4
    my_group = my_gz * 4 + my_gy
    mine_at = my_group * 8 + col % 8
    other_at = my_group * 8 + (col + 4) % 8
    lane = lane_iota()
    barrier = pltpu.get_barrier_semaphore()

    inputs = [
        (depth_hbm, depth_ref),
        (target_hbm, target_ref),
        (rotation_hbm, rotation_ref),
        (translation_hbm, translation_ref),
        (flow_hbm, flow),
        (weight_hbm, weight),
    ]
    loads = [
        pltpu.make_async_copy(source, to, in_sem.at[k]) for k, (source, to) in enumerate(inputs)
    ]

    def greet(d, _):
        pl.semaphore_signal(
            barrier, inc=1, device_id=d, device_id_type=pl.DeviceIdType.LOGICAL
        )

    with scope("sc_greet"):
        for load in loads:
            load.start()
        to_all(far_first(), greet)

    with scope("sc_tables"):
        high[...] = jnp.zeros_like(high)
        for load in loads[:4]:
            load.wait()
        column, pose = own_edges(target_ref, rotation_ref, translation_ref, ints, floats)
        pack_tables(depth_ref, column, pose, unfold, send_t)
        recv_t[pl.ds(mine_at, 1), :] = send_t[pl.ds(slot_of(me), 1), :]
        turn = col % 8
        for load in loads[4:]:
            load.wait()

    def pack(n, carry):
        pack_block(n, turn, flow, weight, low, high, chunks)
        return carry

    with scope("sc_pack"):
        lax.fori_loop(0, 8, pack, 0)
    with scope("sc_barrier"):
        pl.semaphore_wait(barrier, NDEV - 1)

    with scope("sc_sends"):
        rows_exchange(
            send_t, recv_t, lambda d, _: slot_of(d), mine_at, small_send.at[3], small_recv.at[3]
        )

        for j in range(3):

            def send_chunk(d, _):
                pltpu.make_async_remote_copy(
                    src_ref=chunks.at[d, j, pl.ds(0, 12), :],
                    dst_ref=recv.at[mine_at, j, pl.ds(0, 12), :],
                    send_sem=big_send,
                    recv_sem=big_recv.at[j, my_group],
                    device_id=d,
                    device_id_type=pl.DeviceIdType.LOGICAL,
                ).start()

            to_all(by_group(far_ahead=j == 2), send_chunk)
        recv[mine_at, :, 0:12, :] = chunks[me, :, 0:12, :]

    with scope("sc_waitt"):
        for ref in (sums, total_t, fix, at_target):
            ref[...] = jnp.zeros_like(ref)
        own[...] = source_columns()
        own_t[...] = source_columns_t()
        rows_wait(recv_t, small_recv.at[3])
        known = recv_t[...].T
        for f in range(2):
            at = slice(128 * f, 128 * f + 128)
            table[0:24, at] = known[24 * f : 24 * f + 24]
            table[24:32, at] = known[48 + 8 * f : 56 + 8 * f]
        table3[...] = split3(table[...])
        expand(table[24:32, :], own, from_pose)

    def group_at(n):
        oz, oy = group_offset(n)
        return ((my_gz + 4 - oz) % 4) * 4 + (my_gy + 4 - oy) % 4

    def arrive(m, j):
        gs = [group_at(2 * m), group_at(2 * m + 1)]

        def landed(g, count):
            ref = recv.at[pl.ds(8 * g, count), j, pl.ds(0, 12), :]
            pltpu.make_async_copy(ref, ref, big_recv.at[j, g]).wait()

        pl.when(m == 0)(lambda: landed(gs[0], 7))
        pl.when(m != 0)(lambda: landed(gs[0], 8))
        landed(gs[1], 8)
        phase_pass(
            m, j, gs, me, recv, recv_t, table3, hot, hot_t, from_pose, dep, rel, coup, sums,
            inverse3, kh,
        )

    for j in range(3):
        with scope(f"sc_arrive{j}"):
            loop(functools.partial(arrive, j=j), 8)
            ci = 1.0 / (0.1 + sums[j, 8:16])
            both = jnp.concatenate([ci, sums[j, 0:8] * ci], 0)
            inverse[j] = both
            inverse3[j] = split3(both)
    with scope("sc_last"):
        loop(lambda h: last_pass(h, hot, hot_t, own_t, coup, inverse3, kh, total_s, total_t), 2)

    with scope("sc_sendd"):
        kind = lax.broadcasted_iota(jnp.int32, (32, 256), 0)
        total = jnp.where(kind < H_ROW, total_t[...], -total_t[...])
        by_target = jnp.concatenate(
            [total[:, 0:128], total[:, 128:256], jnp.zeros((64, 128), F32)], 0
        ).T
        for h in range(2):
            by_source = jnp.concatenate([total_s[h], jnp.zeros((96, 128), F32)], 0).T
            for k in range(8):
                to = pl.ds(pl.multiple_of(8 * group_at(8 * h + k), 8), 8)
                first, second = by_source[16 * k : 16 * k + 8], by_source[16 * k + 8 : 16 * k + 16]
                sum_d[to, :] = first + pltpu.roll(second, 32, 1)
        rows = by_target + sum_d[...]
        opposite = [pltpu.roll(rows[8 * g : 8 * g + 8], 4, 0) for g in range(GROUPS)]
        send_d[...] = rows + pltpu.roll(jnp.concatenate(opposite, 0), 64, 1)
        recv_d[pl.ds(mine_at, 1), :] = send_d[pl.ds(mine_at, 1), :]
        rows_exchange(
            send_d, recv_d, lambda _, place: place, mine_at, small_send.at[0], small_recv.at[0]
        )
    with scope("sc_target"):

        def couple(m):
            at_target[...] += summed(coup[m], hot_t[pair_at(m), :])

        loop(couple, 8)
    with scope("sc_waitd"):
        rows_wait(recv_d, small_recv.at[0])
    with scope("sc_solve"):
        line = jnp.sum(recv_d[...], axis=0, keepdims=True)
        sub = lax.broadcasted_iota(jnp.int32, (8, 128), 0)
        lines = jnp.broadcast_to(line, (8, 128))
        for f in range(1, 4):
            lines = jnp.where(sub == f, pltpu.roll(lines, 128 - 32 * f, 1), lines)
        full = jnp.concatenate([lines, jnp.zeros((120, 128), F32)], 0).T
        z = solve(
            lambda i, j: full[K_INDEX[i, j] : K_INDEX[i, j] + 1, :],
            lambda i: full[H_ROW + i : H_ROW + i + 1, :],
        )
        zs = jnp.concatenate([*z, jnp.zeros((122, 128), F32)], 0)
        turned = zs.T
        pose_ref[...] = turned[0:2, 0:6]
        later = pltpu.roll(turned[0:8], 8, 1)
        mine, other = turned[0:1] + later[1:2], turned[2:3] + later[3:4]
        send_e[...] = jnp.where(sub == 0, mine, other)
        recv_e[pl.ds(mine_at, 1), :] = mine
        recv_e[pl.ds(other_at, 1), :] = other
    with scope("sc_sende"):
        near = [o for o in far_first() if hops(o) <= 3]
        steps_exchange(near, send_e, 0, recv_e, mine_at, small_send.at[1], small_recv.at[1])
        near = [o for o in near if hops(o) <= 2]
        steps_exchange(near, send_e, 1, recv_e, other_at, small_send.at[1], small_recv.at[1])
    with scope("sc_waite"):
        rows_wait(recv_e, small_recv.at[1], NDEV - 2)
    with scope("sc_third"):
        every = recv_e[...].T
        steps[:, 0:128] = every[0:8]
        steps[:, 128:256] = every[8:16]
        expand(steps[...], own, from_steps)
        loop(
            lambda h: third_pass(
                h, [group_at(8 * h + k) for k in range(8)], hot_t, coup, from_steps, fix
            ),
            2,
        )
    with scope("sc_sendf"):
        back = at_target[0:24] * steps[0:1]
        for a in range(1, 6):
            back += at_target[24 * a : 24 * a + 24] * steps[a : a + 1]
        grad = jnp.concatenate([sums[j, 0:8] for j in range(3)], 0)
        ci = jnp.concatenate([inverse[j, 0:8] for j in range(3)], 0)
        new = table[0:24] + (grad - (fix[...] - back)) * ci
        zero8 = jnp.zeros((8, 128), F32)
        send_f[...] = jnp.concatenate(
            [new[:, 0:128], zero8, new[:, 128:256], zero8, jnp.zeros((64, 128), F32)], 0
        ).T
        slot = slot_of(me)
        recv_f[pl.ds(slot, 1), :] = send_f[pl.ds(mine_at, 1), :]
        rows_exchange(
            send_f, recv_f, lambda _, place: place, slot, small_send.at[2], small_recv.at[2]
        )
    with scope("sc_waitf"):
        rows_wait(recv_f, small_recv.at[2])
    for f in range(2):
        tiles = [None] * 3
        for i in range(16):
            piece = recv_f[8 * i : 8 * i + 8, :]
            first = 24 * i
            moved = pltpu.roll(piece, (first - 32 * f) % 128, 1)
            for t in range(3):
                a, b = max(first - 128 * t, 0), min(first + 24 - 128 * t, 128)
                if a < b:
                    if tiles[t] is None:
                        tiles[t] = moved
                    else:
                        tiles[t] = jnp.where((lane >= a) & (lane < b), moved, tiles[t])
        for g in range(8):
            for t in range(3):
                at = 384 * g + 128 * t
                out_ref[f : f + 1, at : at + 128] = tiles[t][g : g + 1]

    ref = chunks.at[pl.ds(0, NDEV - 1), :, pl.ds(0, 12), :]
    pltpu.make_async_copy(ref, ref, big_send).wait()
    rows_wait(recv_t, small_send.at[3])
    rows_wait(recv_d, small_send.at[0])
    rows_wait(recv_e, small_send.at[1], NDEV - 2)
    rows_wait(recv_f, small_send.at[2])


def run_main(flow, weight, inv_depth, edge_target, rotation, translation):
    v = pltpu.VMEM
    vmem = pl.BlockSpec(memory_space=pltpu.VMEM)
    hbm = pl.BlockSpec(memory_space=pltpu.HBM)
    return pl.pallas_call(
        main_kernel,
        in_specs=[hbm] * 6,
        out_specs=[vmem] * 2,
        out_shape=[
            jax.ShapeDtypeStruct((2, PX * NDEV), F32),
            jax.ShapeDtypeStruct((2, 6), F32),
        ],
        scratch_shapes=[
            v((2, 48, PX * NDEV), F32),
            v((2, 48, PX * NDEV), F32),
            v((2, PX * NDEV), F32),
            v((2, 24), jnp.int32),
            v((2, 3), F32),
            v((2, 3), F32),
            v((128, LANES), F32),
            v((128, LANES), F32),
            v((NDEV, 3, 16, 128), F32),
            v((8, 128), jnp.int32),
            v((2, 8, 128), F32),
            v((2, 8, LANES), F32),
            v((NDEV, 3, 16, 128), F32),
            v((32, 256), F32),
            v((96, 256), BF16),
            v((256, GROUPS * LANES), BF16),
            v((GROUPS * LANES, 256), BF16),
            v((128, LANES), BF16),
            v((8 * LANES, 128), BF16),
            v((128, LANES), F32),
            v((8, 24, 2 * LANES), F32),
            v((8, 8, 2 * LANES), F32),
            v((8, 144, 2 * LANES), F32),
            v((3, 16, 256), F32),
            v((3, 16, 256), F32),
            v((3, 48, 256), BF16),
            v((8, 32, 2 * LANES), F32),
            v((2, 32, 128), F32),
            v((32, 256), F32),
            v((144, 256), F32),
            v((8, 256), F32),
            v((128, LANES), F32),
            v((24, 256), F32),
            v((128, 128), F32),
            v((128, 128), F32),
            v((128, 128), F32),
            v((128, 128), F32),
            v((128, 128), F32),
            v((8, 128), F32),
            v((128, 128), F32),
            v((128, 128), F32),
            v((128, 128), F32),
            pltpu.SemaphoreType.DMA((6,)),
            pltpu.SemaphoreType.DMA,
            pltpu.SemaphoreType.DMA((3, GROUPS)),
            pltpu.SemaphoreType.DMA((4,)),
            pltpu.SemaphoreType.DMA((4,)),
        ],
        compiler_params=pltpu.CompilerParams(
            collective_id=0, has_side_effects=True, vmem_limit_bytes=56 * 1024 * 1024
        ),
        name="step",
    )(flow, weight, inv_depth, edge_target, rotation, translation)


def hand_over(*results):
    def kernel(depth, pose, depth_out, pose_out):
        depth_out[...] = depth[...]
        pose_out[...] = pose[...]

    vmem = pl.BlockSpec(memory_space=pltpu.VMEM)
    return pl.pallas_call(
        kernel,
        in_specs=[vmem] * 2,
        out_specs=[vmem] * 2,
        out_shape=[jax.ShapeDtypeStruct(r.shape, r.dtype) for r in results],
        compiler_params=pltpu.CompilerParams(vmem_limit_bytes=56 * 1024 * 1024),
        name="hand_over",
    )(*results)


def shards(inv_depth, rotation, translation, edge_target, flow_obs, weight):
    pixels = inv_depth.shape[1]
    flow = flow_obs.reshape(2, 48, pixels)
    wts = weight.reshape(2, 48, pixels)
    depth, pose = hand_over(
        *run_main(flow, wts, inv_depth, edge_target, rotation.T, translation.T)
    )
    return depth, pose.T


def solution(mesh):
    in_specs = (
        P(("row", "col"), None),
        P(None, ("row", "col")),
        P(None, ("row", "col")),
        P(("row", "col"), None),
        P(None, ("row", "col"), None, None),
        P(None, ("row", "col"), None, None),
    )
    out_specs = (P(("row", "col"), None), P(None, ("row", "col")))
    return jax.shard_map(
        shards, mesh=mesh, in_specs=in_specs, out_specs=out_specs, check_vma=False
    )
```

```python
import contextlib
import functools

import jax
import jax.numpy as jnp
from jax import lax
from jax.experimental import pallas as pl
from jax.experimental.pallas import tpu as pltpu
from jax.sharding import PartitionSpec as P

F32 = jnp.float32
BF16 = jnp.bfloat16
NDEV = 128
PX = 24
GROUPS = 16
LANES = 384
MESH = pl.DeviceIdType.MESH
K_PAIRS = [((a, b), n) for n, (a, b) in enumerate((a, b) for a in range(6) for b in range(a, 6))]
K_INDEX = {**dict(K_PAIRS), **{(b, a): n for (a, b), n in K_PAIRS}}
H_ROW = 21


def lane_iota(shape=(8, 128)):
    return lax.broadcasted_iota(jnp.int32, shape, 1)


def pack_half(b, j, turn, flow, weight, low, high, out):
    cols = pl.ds(pl.multiple_of((2 * j + b) * 512, 512), 512)

    def put(ref, block, value):
        at = pl.multiple_of(((3 * turn + block) % 8) * 16, 16)
        ref[pl.ds(at, 16), :] = value

    for k in range(3):
        put(low, k, flow[0, 16 * k : 16 * k + 16, cols])
        put(low, 3 + k, flow[1, 16 * k : 16 * k + 16, cols])
        put(high, 1 + k, weight[1, 16 * k : 16 * k + 16, cols])
    put(low, 6, weight[0, 0:16, cols])
    put(low, 7, weight[0, 16:32, cols])
    put(high, 0, weight[0, 32:48, cols])
    low_t = low[...].T
    high_t = high[...].T
    where_at = (lane_iota() - 48 * turn + 384) % 128
    for d in range(64):
        out[64 * b + d, j, 0:8, :] = low_t[8 * d : 8 * d + 8]
        rest = high_t[8 * d : 8 * d + 8]
        turned = pltpu.roll(pltpu.roll(rest, 64, 1), 4, 0)
        out[64 * b + d, j, 8:12, :] = jnp.where(where_at < 64, rest, turned)[0:4]


def own_edges(target_ref, rotation_ref, translation_ref, ints, floats):
    lane = lane_iota()
    ints[...] = jnp.zeros_like(ints)
    ints[0:2, 0:24] = target_ref[...]
    both = ints[...]
    target = jnp.where(lane < 24, both[0:1], pltpu.roll(both, 24, 1)[1:2])
    x, y, z = (target >> 2) & 3, (target >> 4) & 3, target >> 6
    group = (((z - x) & 3) << 2) + ((y - x) & 3)
    column = ((target & 1) << 7) + (group << 3) + ((target >> 1) & 7)
    floats[...] = jnp.zeros_like(floats)
    floats[0, 0:2, 0:3] = rotation_ref[...]
    floats[1, 0:2, 0:3] = translation_ref[...]
    return column.astype(F32), floats[0] + pltpu.roll(floats[1], 3, 1)


def pack_tables(depth_ref, column, pose, unfold, send):
    lane = lane_iota()
    poses = pltpu.roll(pose, 48, 1)[0:1] + pltpu.roll(pose, 56, 1)[1:2]
    known = jnp.where(lane < 64, poses, pltpu.roll(column, 64, 1)[0:1])
    for f in range(2):
        for j in range(3):
            for g in range(8):
                at = 128 * (8 * j + g)
                unfold[f, j, g : g + 1, :] = depth_ref[f : f + 1, at : at + 128]
    for i in range(16):
        acc = known
        for f in range(2):
            for j in range(3):
                to = 24 * f + 8 * j
                moved = pltpu.roll(unfold[f, j], (to - 8 * i) % 128, 1)
                acc = jnp.where((lane >= to) & (lane < to + 8), moved, acc)
        send[8 * i : 8 * i + 8, :] = acc


def strip(tiles, lane, offset, width):
    out = []
    for t in range(3):
        acc = None
        for i in range(8):
            start = 48 * i + offset
            for wrap in (0, 384, 768):
                a = max(start - wrap, 128 * t) - 128 * t
                b = min(start + width - wrap, 128 * t + 128) - 128 * t
                if a < b:
                    if acc is None:
                        acc = tiles[i]
                    else:
                        acc = jnp.where((lane >= a) & (lane < b), tiles[i], acc)
        out.append(acc)
    return out


def shifted(tiles, lane, shift):
    whole, part = divmod(shift % 384, 128)
    if part == 0:
        return [tiles[(t - whole) % 3] for t in range(3)]
    rolled = [pltpu.roll(t, part, 1) for t in tiles]
    return [
        jnp.where(lane < part, rolled[(t - whole - 1) % 3], rolled[(t - whole) % 3])
        for t in range(3)
    ]


def split3(x):
    top = x.astype(BF16).astype(F32)
    rest = x - top
    mid = rest.astype(BF16).astype(F32)
    return jnp.concatenate([top, mid, rest - mid], 0).astype(BF16)


def join3(y):
    n = y.shape[0] // 3
    return y[:n] + y[n : 2 * n] + y[2 * n :]


def gathered(parts, hot):
    return join3(jnp.dot(parts, hot, preferred_element_type=F32))


def summed(values, hot_t):
    return join3(jnp.dot(split3(values), hot_t, preferred_element_type=F32))


def unpack_group(g, j, recv):
    lane = lane_iota()
    upper = lax.broadcasted_iota(jnp.int32, (8, 128), 0) >= 4
    block_lane = [(lane + 128 * t) % 48 for t in range(3)]
    low = [recv[8 * g + i, j, 0:8, :] for i in range(8)]
    high = [recv[8 * g + i, j, 8:16, :] for i in range(8)]

    def at(tiles, start, width, to):
        return shifted(strip(tiles, lane, start, width), lane, to - start)

    def piece(offset, width, to):
        first, second = at(high, offset, width, to), at(high, offset + 64, width, to)
        return [jnp.where(upper, pltpu.roll(b, 4, 0), a) for a, b in zip(first, second)]

    first, second = at(low, 96, 32, 0), piece(0, 16, 32)
    return [
        at(low, 0, 48, 0),
        at(low, 48, 48, 0),
        [jnp.where(b < 32, f, s) for b, f, s in zip(block_lane, first, second)],
        piece(16, 48, 0),
    ]


def group_targets(g, recv_t):
    lane = lane_iota()
    sub = lax.broadcasted_iota(jnp.int32, (8, 128), 0)
    tile = recv_t[pl.ds(pl.multiple_of(8 * g, 8), 8), :]
    out = [jnp.zeros((8, 128), F32)] * 3
    for i in range(8):
        moved = pltpu.roll(tile, (48 * i - 64) % 128, 1)
        for t in range(3):
            a, b = max(48 * i - 128 * t, 0), min(48 * i + 48 - 128 * t, 128)
            if a < b:
                out[t] = jnp.where((sub == i) & (lane >= a) & (lane < b), moved, out[t])
    return jnp.concatenate([jnp.sum(x, axis=0, keepdims=True) for x in out], 1)


def merge(items):
    sub = lax.broadcasted_iota(jnp.int32, (8, 128), 0)
    items = items[::-1]
    for bit in (0, 1, 2):
        step = 1 << bit
        here = (sub & step) != 0
        items = [
            jnp.where(here, a, b) + pltpu.roll(jnp.where(here, b, a), step, 0)
            for a, b in zip(items[0::2], items[1::2])
        ]
    return items[0]


def merged_rows(rows):
    rows = rows + [jnp.zeros((8, 128), F32)] * (32 - len(rows))
    return jnp.concatenate([merge(rows[k : k + 8]) for k in range(0, 32, 8)], 0)


def pixel_xy(me, j):
    p = 8 * NDEV * j + 8 * me + lax.broadcasted_iota(jnp.int32, (8, 128), 0)
    x = ((p % 64).astype(F32) + 0.5) / 64 - 0.5
    y = ((p // 64).astype(F32) + 0.5 - 24.0) / 64
    return x, y


def expand(rows, own, out):
    lane = lane_iota()
    mine = [
        jnp.where(
            lane < 8,
            pltpu.roll(rows[:, 0:128], (128 - 8 * g) % 128, 1),
            pltpu.roll(rows[:, 128:256], (136 - 8 * g) % 128, 1),
        )
        for g in range(GROUPS)
    ]
    out[...] = gathered(split3(jnp.concatenate(mine, 0)), own[...])


def rows_of(ref, g):
    return ref[pl.ds(pl.multiple_of(8 * g, 8), 8), :]


def edge_rows(a, j):
    return slice(24 * a + 8 * j, 24 * a + 8 * j + 8)


def add_block(acc, row, value):
    acc[row] = value if acc[row] is None else acc[row] + value


def source_columns():
    rows = lax.broadcasted_iota(jnp.int32, (128, LANES), 0)
    frame = lax.broadcasted_iota(jnp.int32, (1, LANES), 1) // 24
    return jnp.where(rows == (frame % 2) * 8 + frame // 2, 1.0, 0.0).astype(BF16)


def source_columns_t():
    edge = lax.broadcasted_iota(jnp.int32, (8 * LANES, 1), 0)
    frame = (edge % LANES) // 24
    lanes = lax.broadcasted_iota(jnp.int32, (8 * LANES, 128), 1)
    at = (edge // LANES) * 16 + (frame % 2) * 8 + frame // 2
    return jnp.where(lanes == at, 1.0, 0.0).astype(BF16)


def build_terms(acc, cols, inputs, d, rel, xy, coup, m, j):
    x, y = xy
    fu, fv, cu, cv = inputs
    w0, w1, w2, m0, m1, m2 = [rel[k : 1 + k, cols] for k in range(6)]
    x0 = x + w1 - w2 * y + m0 * d
    x1 = y + w2 * x - w0 + m1 * d
    x2 = 1.0 + w0 * y - w1 * x + m2 * d
    q = 1.0 / x2
    u = x0 * q
    v = x1 * q
    ru = fu - (u - x)
    rv = fv - (v - y)
    du = q * (m0 - u * m2)
    dv = q * (m1 - v * m2)
    eu = cu * du
    ev = cv * dv
    dq = d * q
    ju = {0: -(u * y) * q, 1: (1.0 + u * x) * q, 2: -y * q, 3: dq, 5: -u * dq}
    jv = {0: (-1.0 - v * y) * q, 1: v * x * q, 2: x * q, 4: dq, 5: -v * dq}
    for a in range(6):
        if a in ju and a in jv:
            e = ju[a] * eu + jv[a] * ev
        else:
            e = ju[a] * eu if a in ju else jv[a] * ev
        coup[m, edge_rows(a, j), cols] = e
    su = {a: cu * ju[a] for a in ju}
    sv = {a: cv * jv[a] for a in jv}
    for (a, b), row in K_PAIRS:
        if a in ju and b in ju:
            add_block(acc, row, su[a] * ju[b])
        if a in jv and b in jv:
            add_block(acc, row, sv[a] * jv[b])
    for a in range(6):
        if a in ju:
            add_block(acc, H_ROW + a, su[a] * ru)
        if a in jv:
            add_block(acc, H_ROW + a, sv[a] * rv)
    return eu * ru + ev * rv, eu * du + ev * dv


def take_terms(acc, cols, near, coup, m, j):
    ci, gi = -near[0], -near[1]
    e = [coup[m, edge_rows(a, j), cols] for a in range(6)]
    for a in range(6):
        scaled = e[a] * ci
        for (k, b), row in K_PAIRS:
            if k == a:
                add_block(acc, row, scaled * e[b])
        add_block(acc, H_ROW + a, e[a] * gi)


def filled(acc):
    return [jnp.zeros((8, 128), F32) if x is None else x for x in acc]


def tile_cols(t):
    return slice(128 * t, 128 * t + 128)


def pair_at(m, count=1):
    size = 2 * LANES * count
    return pl.ds(pl.multiple_of(size * m, 128), size)


def phase_pass(
    m, j, gs, me, recv, recv_t, table3, hot, hot_t, from_pose, dep, rel, coup, sums, inverse3, kh
):
    at = pair_at(m)
    if j == 0:
        rows = lax.broadcasted_iota(jnp.int32, (256, 2 * LANES), 0).astype(F32)
        targets = jnp.concatenate([group_targets(g, recv_t) for g in gs], 1)
        hot[:, at] = jnp.where(rows == targets, 1.0, 0.0).astype(BF16)
        lanes = lane_iota((128, 256)).astype(F32)
        for t in range(6):
            column = jnp.broadcast_to(targets[:, tile_cols(t)], (128, 128)).T
            column = jnp.concatenate([column, column], 1)
            to = pl.ds(pl.multiple_of(2 * LANES * m + 128 * t, 128), 128)
            hot_t[to, :] = jnp.where(lanes == column, 1.0, 0.0).astype(BF16)
        near = gathered(table3[...], hot[:, at])
        dep[m] = near[0:24]
        relative = jnp.concatenate([rows_of(from_pose, g) for g in gs], 1) - near[24:32]
        rel[m] = relative
    else:
        relative = rel[m]
        back = gathered(inverse3[j - 1], hot[:, at])
    parts = [unpack_group(g, j, recv) for g in gs]
    grads, curvs, blocks = [], [], []
    xy = pixel_xy(me, j)
    for t in range(6):
        cols = tile_cols(t)
        acc = [None] * 27
        d = dep[m, 8 * j : 8 * j + 8, cols]
        tiles = [part[t % 3] for part in parts[t // 3]]
        gd, cd = build_terms(acc, cols, tiles, d, relative, xy, coup, m, j)
        grads.append(gd)
        curvs.append(cd)
        if j > 0:
            take_terms(acc, cols, (back[0:8, cols], back[8:16, cols]), coup, m, j - 1)
        blocks.append(merged_rows(filled(acc)))
    both = jnp.concatenate([jnp.concatenate(grads, 1), jnp.concatenate(curvs, 1)], 0)
    sums[j] += summed(both, hot_t[at, :])
    block = jnp.concatenate(blocks, 1)
    kh[m] = block if j == 0 else kh[m] + block


def last_pass(h, hot, hot_t, own_t, coup, inverse3, kh, total_s, total_t):
    at = pair_at(h, 4)
    near = gathered(inverse3[2], hot[:, at])
    blocks = []
    for t in range(24):
        m = 4 * h + t // 6
        acc = [None] * 27
        cols = tile_cols(t)
        take_terms(acc, tile_cols(t % 6), (near[0:8, cols], near[8:16, cols]), coup, m, 2)
        blocks.append(kh[m, :, tile_cols(t % 6)] + merged_rows(acc))
    parts = split3(jnp.concatenate(blocks, 1))
    total_t[...] += join3(jnp.dot(parts, hot_t[at, :], preferred_element_type=F32))
    total_s[h] = join3(jnp.dot(parts, own_t[...], preferred_element_type=F32))


def third_pass(h, gs, hot_t, coup, from_steps, fix):
    parts = []
    for t in range(24):
        m, cols = 4 * h + t // 6, tile_cols(t % 6)
        motion = rows_of(from_steps, gs[t // 3])
        column = []
        for j in range(3):
            terms = [
                coup[m, edge_rows(a, j), cols] * motion[a : a + 1, tile_cols(t % 3)]
                for a in range(6)
            ]
            column.append(((terms[0] + terms[1]) + (terms[2] + terms[3])) + (terms[4] + terms[5]))
        parts.append(jnp.concatenate(column, 0))
    fix[...] += summed(jnp.concatenate(parts, 1), hot_t[pair_at(h, 4), :])


def solve(matrix, right):
    factor = {}
    for i in range(6):
        for j in range(i + 1):
            e = matrix(i, j)
            if i == j:
                e = e * 1.1 + 0.001
            for k in range(j):
                e = e - factor[i, k] * factor[j, k]
            factor[i, j] = jnp.sqrt(e) if i == j else e / factor[j, j]
    forward = []
    for i in range(6):
        e = right(i)
        for k in range(i):
            e = e - factor[i, k] * forward[k]
        forward.append(e / factor[i, i])
    z = [None] * 6
    for i in reversed(range(6)):
        e = forward[i]
        for k in range(i + 1, 6):
            e = e - factor[k, i] * z[k]
        z[i] = e / factor[i, i]
    return z


def ring_steps(d):
    return min(d, 4 - d)


def hops(offset):
    return ring_steps(offset[0]) + ring_steps(offset[1]) + ring_steps(offset[2])


def far_first():
    offsets = [
        (dz, dy, dx, dc)
        for dz in range(4)
        for dy in range(4)
        for dx in range(4)
        for dc in range(2)
        if (dz, dy, dx, dc) != (0, 0, 0, 0)
    ]
    return sorted(offsets, key=lambda o: -hops(o))


def group_offset(n):
    return (n // 4 + n) % 4, n % 4


def pair_order(m, far_ahead):
    order = []
    for n in (2 * m, 2 * m + 1):
        oz, oy = group_offset(n)
        members = [
            ((oz + dx) % 4, (oy + dx) % 4, dx, dc) for dx in range(4) for dc in range(2)
        ]
        order += sorted(members, key=lambda o: -hops(o)) if far_ahead else members
    return [o for o in order if o != (0, 0, 0, 0)]


def to_all(order, act):
    row, col = lax.axis_index("row"), lax.axis_index("col")
    y, x = col // 8, (col // 2) % 4
    zs = [((row + d) % 4) * 32 for d in range(4)]
    ys = [((y + d) % 4) * 8 for d in range(4)]
    xs = [((x + d) % 4) * 2 for d in range(4)]
    cs = [(col + d) % 2 for d in range(2)]
    gz = [((row + 4 - x + d) % 4) * 32 for d in range(4)]
    gy = [((y + 4 - x + d) % 4) * 8 for d in range(4)]
    for dz, dy, dx, dc in order:
        last = xs[dx] + cs[dc]
        act(zs[dz] + ys[dy] + last, gz[(dz - dx) % 4] + gy[(dy - dx) % 4] + last)


def slot_of(d):
    return (d % 16) * 8 + d // 16


def rows_exchange(send, recv, source, slot, send_sem, recv_sem):
    def act(d, place):
        pltpu.make_async_remote_copy(
            src_ref=send.at[pl.ds(source(d, place), 1), :],
            dst_ref=recv.at[pl.ds(slot, 1), :],
            send_sem=send_sem,
            recv_sem=recv_sem,
            device_id=d,
            device_id_type=pl.DeviceIdType.LOGICAL,
        ).start()

    to_all(far_first(), act)


def steps_exchange(order, send, source, recv, slot, send_sem, recv_sem):
    def act(d, _):
        pltpu.make_async_remote_copy(
            src_ref=send.at[pl.ds(source, 1), :],
            dst_ref=recv.at[pl.ds(slot, 1), :],
            send_sem=send_sem,
            recv_sem=recv_sem,
            device_id=d,
            device_id_type=pl.DeviceIdType.LOGICAL,
        ).start()

    to_all(order, act)


def rows_wait(buf, sem, count=NDEV - 1):
    ref = buf.at[pl.ds(0, count), :]
    pltpu.make_async_copy(ref, ref, sem).wait()


def scope(name):
    return contextlib.nullcontext()


def loop(body, count):
    def step(n, carry):
        body(n)
        return carry

    lax.fori_loop(0, count, step, 0)


def main_kernel(
    flow_hbm, weight_hbm, depth_hbm, target_hbm, rotation_hbm, translation_hbm,
    out_ref, pose_ref,
    flow, weight, depth_ref, target_ref, rotation_ref, translation_ref, low, high, chunks, ints, floats, unfold,
    recv, table, table3, hot, hot_t, own, own_t, from_pose, dep, rel, coup, sums, inverse,
    inverse3, kh,
    total_s, total_t, at_target, steps, from_steps, fix,
    send_t, recv_t, sum_d, send_d, recv_d, send_e, recv_e, send_f, recv_f,
    in_sem, big_send, big_recv, small_send, small_recv,
):
    row, col = lax.axis_index("row"), lax.axis_index("col")
    me = row * 32 + col
    y, x = col // 8, (col // 2) % 4
    my_gz, my_gy = (row + 4 - x) % 4, (y + 4 - x) % 4
    my_group = my_gz * 4 + my_gy
    mine_at = my_group * 8 + col % 8
    other_at = my_group * 8 + (col + 4) % 8
    lane = lane_iota()
    barrier = pltpu.get_barrier_semaphore()

    inputs = [
        (depth_hbm, depth_ref),
        (target_hbm, target_ref),
        (rotation_hbm, rotation_ref),
        (translation_hbm, translation_ref),
        (flow_hbm, flow),
        (weight_hbm, weight),
    ]
    loads = [
        pltpu.make_async_copy(source, to, in_sem.at[k]) for k, (source, to) in enumerate(inputs)
    ]

    def greet(d, _):
        pl.semaphore_signal(
            barrier, inc=1, device_id=d, device_id_type=pl.DeviceIdType.LOGICAL
        )

    with scope("sc_greet"):
        for load in loads:
            load.start()
        to_all(far_first(), greet)

    with scope("sc_tables"):
        high[...] = jnp.zeros_like(high)
        for load in loads[:4]:
            load.wait()
        column, pose = own_edges(target_ref, rotation_ref, translation_ref, ints, floats)
        pack_tables(depth_ref, column, pose, unfold, send_t)
        recv_t[pl.ds(mine_at, 1), :] = send_t[pl.ds(slot_of(me), 1), :]
        turn = col % 8
        for load in loads[4:]:
            load.wait()

    def pack(j):
        def step(b, carry):
            pack_half(b, j, turn, flow, weight, low, high, chunks)
            return carry

        lax.fori_loop(0, 2, step, 0)

    with scope("sc_pack"):
        pack(0)
    with scope("sc_barrier"):
        pl.semaphore_wait(barrier, NDEV - 1)

    with scope("sc_sends"):
        rows_exchange(
            send_t, recv_t, lambda d, _: slot_of(d), mine_at, small_send.at[3], small_recv.at[3]
        )

        def send_phase(j):
            for m in range(8):

                def send_chunk(d, _):
                    pltpu.make_async_remote_copy(
                        src_ref=chunks.at[d, j, pl.ds(0, 12), :],
                        dst_ref=recv.at[mine_at, j, pl.ds(0, 12), :],
                        send_sem=big_send,
                        recv_sem=big_recv.at[j, m],
                        device_id=d,
                        device_id_type=pl.DeviceIdType.LOGICAL,
                    ).start()

                to_all(pair_order(m, j == 2), send_chunk)

        send_phase(0)
        pack(1)
        pack(2)
        send_phase(1)
        send_phase(2)
        recv[mine_at, :, 0:12, :] = chunks[me, :, 0:12, :]

    with scope("sc_waitt"):
        for ref in (sums, total_t, fix, at_target):
            ref[...] = jnp.zeros_like(ref)
        own[...] = source_columns()
        own_t[...] = source_columns_t()
        rows_wait(recv_t, small_recv.at[3])
        known = recv_t[...].T
        for f in range(2):
            at = slice(128 * f, 128 * f + 128)
            table[0:24, at] = known[24 * f : 24 * f + 24]
            table[24:32, at] = known[48 + 8 * f : 56 + 8 * f]
        table3[...] = split3(table[...])
        expand(table[24:32, :], own, from_pose)

    def group_at(n):
        oz, oy = group_offset(n)
        return ((my_gz + 4 - oz) % 4) * 4 + (my_gy + 4 - oy) % 4

    def arrive(m, j):
        gs = [group_at(2 * m), group_at(2 * m + 1)]

        def landed(count):
            ref = recv.at[pl.ds(0, count), j, pl.ds(0, 12), :]
            pltpu.make_async_copy(ref, ref, big_recv.at[j, m]).wait()

        pl.when(m == 0)(lambda: landed(15))
        pl.when(m != 0)(lambda: landed(16))
        phase_pass(
            m, j, gs, me, recv, recv_t, table3, hot, hot_t, from_pose, dep, rel, coup, sums,
            inverse3, kh,
        )

    for j in range(3):
        with scope(f"sc_arrive{j}"):
            loop(functools.partial(arrive, j=j), 8)
            ci = 1.0 / (0.1 + sums[j, 8:16])
            both = jnp.concatenate([ci, sums[j, 0:8] * ci], 0)
            inverse[j] = both
            inverse3[j] = split3(both)
    with scope("sc_last"):
        loop(lambda h: last_pass(h, hot, hot_t, own_t, coup, inverse3, kh, total_s, total_t), 2)

    with scope("sc_sendd"):
        kind = lax.broadcasted_iota(jnp.int32, (32, 256), 0)
        total = jnp.where(kind < H_ROW, total_t[...], -total_t[...])
        by_target = jnp.concatenate(
            [total[:, 0:128], total[:, 128:256], jnp.zeros((64, 128), F32)], 0
        ).T
        for h in range(2):
            by_source = jnp.concatenate([total_s[h], jnp.zeros((96, 128), F32)], 0).T
            for k in range(8):
                to = pl.ds(pl.multiple_of(8 * group_at(8 * h + k), 8), 8)
                first, second = by_source[16 * k : 16 * k + 8], by_source[16 * k + 8 : 16 * k + 16]
                sum_d[to, :] = first + pltpu.roll(second, 32, 1)
        rows = by_target + sum_d[...]
        opposite = [pltpu.roll(rows[8 * g : 8 * g + 8], 4, 0) for g in range(GROUPS)]
        send_d[...] = rows + pltpu.roll(jnp.concatenate(opposite, 0), 64, 1)
        recv_d[pl.ds(mine_at, 1), :] = send_d[pl.ds(mine_at, 1), :]
        rows_exchange(
            send_d, recv_d, lambda _, place: place, mine_at, small_send.at[0], small_recv.at[0]
        )
    with scope("sc_target"):

        def couple(m):
            at_target[...] += summed(coup[m], hot_t[pair_at(m), :])

        loop(couple, 8)
    with scope("sc_waitd"):
        rows_wait(recv_d, small_recv.at[0])
    with scope("sc_solve"):
        line = jnp.sum(recv_d[...], axis=0, keepdims=True)
        sub = lax.broadcasted_iota(jnp.int32, (8, 128), 0)
        lines = jnp.broadcast_to(line, (8, 128))
        for f in range(1, 4):
            lines = jnp.where(sub == f, pltpu.roll(lines, 128 - 32 * f, 1), lines)
        full = jnp.concatenate([lines, jnp.zeros((120, 128), F32)], 0).T
        z = solve(
            lambda i, j: full[K_INDEX[i, j] : K_INDEX[i, j] + 1, :],
            lambda i: full[H_ROW + i : H_ROW + i + 1, :],
        )
        zs = jnp.concatenate([*z, jnp.zeros((122, 128), F32)], 0)
        turned = zs.T
        pose_ref[...] = turned[0:2, 0:6]
        later = pltpu.roll(turned[0:8], 8, 1)
        mine, other = turned[0:1] + later[1:2], turned[2:3] + later[3:4]
        send_e[...] = jnp.where(sub == 0, mine, other)
        recv_e[pl.ds(mine_at, 1), :] = mine
        recv_e[pl.ds(other_at, 1), :] = other
    with scope("sc_sende"):
        near = [o for o in far_first() if hops(o) <= 3]
        steps_exchange(near, send_e, 0, recv_e, mine_at, small_send.at[1], small_recv.at[1])
        near = [o for o in near if hops(o) <= 2]
        steps_exchange(near, send_e, 1, recv_e, other_at, small_send.at[1], small_recv.at[1])
    with scope("sc_waite"):
        rows_wait(recv_e, small_recv.at[1], NDEV - 2)
    with scope("sc_third"):
        every = recv_e[...].T
        steps[:, 0:128] = every[0:8]
        steps[:, 128:256] = every[8:16]
        expand(steps[...], own, from_steps)
        loop(
            lambda h: third_pass(
                h, [group_at(8 * h + k) for k in range(8)], hot_t, coup, from_steps, fix
            ),
            2,
        )
    with scope("sc_sendf"):
        back = at_target[0:24] * steps[0:1]
        for a in range(1, 6):
            back += at_target[24 * a : 24 * a + 24] * steps[a : a + 1]
        grad = jnp.concatenate([sums[j, 0:8] for j in range(3)], 0)
        ci = jnp.concatenate([inverse[j, 0:8] for j in range(3)], 0)
        new = table[0:24] + (grad - (fix[...] - back)) * ci
        zero8 = jnp.zeros((8, 128), F32)
        send_f[...] = jnp.concatenate(
            [new[:, 0:128], zero8, new[:, 128:256], zero8, jnp.zeros((64, 128), F32)], 0
        ).T
        slot = slot_of(me)
        recv_f[pl.ds(slot, 1), :] = send_f[pl.ds(mine_at, 1), :]
        rows_exchange(
            send_f, recv_f, lambda _, place: place, slot, small_send.at[2], small_recv.at[2]
        )
    with scope("sc_waitf"):
        rows_wait(recv_f, small_recv.at[2])
    for f in range(2):
        for j in range(3):
            tile = None
            for i in range(16):
                shift = 8 * i - 32 * f - 8 * j
                moved = pltpu.roll(recv_f[8 * i : 8 * i + 8, :], shift % 128, 1)
                tile = moved if i == 0 else jnp.where(lane >= 8 * i, moved, tile)
            for g in range(8):
                at = 128 * (8 * j + g)
                out_ref[f : f + 1, at : at + 128] = tile[g : g + 1]

    ref = chunks.at[pl.ds(0, NDEV - 1), :, pl.ds(0, 12), :]
    pltpu.make_async_copy(ref, ref, big_send).wait()
    rows_wait(recv_t, small_send.at[3])
    rows_wait(recv_d, small_send.at[0])
    rows_wait(recv_e, small_send.at[1], NDEV - 2)
    rows_wait(recv_f, small_send.at[2])


def run_main(flow, weight, inv_depth, edge_target, rotation, translation):
    v = pltpu.VMEM
    vmem = pl.BlockSpec(memory_space=pltpu.VMEM)
    hbm = pl.BlockSpec(memory_space=pltpu.HBM)
    return pl.pallas_call(
        main_kernel,
        in_specs=[hbm] * 6,
        out_specs=[vmem] * 2,
        out_shape=[
            jax.ShapeDtypeStruct((2, PX * NDEV), F32),
            jax.ShapeDtypeStruct((2, 6), F32),
        ],
        scratch_shapes=[
            v((2, 48, PX * NDEV), F32),
            v((2, 48, PX * NDEV), F32),
            v((2, PX * NDEV), F32),
            v((2, 24), jnp.int32),
            v((2, 3), F32),
            v((2, 3), F32),
            v((128, 512), F32),
            v((128, 512), F32),
            v((NDEV, 3, 16, 128), F32),
            v((8, 128), jnp.int32),
            v((2, 8, 128), F32),
            v((2, 3, 8, 128), F32),
            v((NDEV, 3, 16, 128), F32),
            v((32, 256), F32),
            v((96, 256), BF16),
            v((256, GROUPS * LANES), BF16),
            v((GROUPS * LANES, 256), BF16),
            v((128, LANES), BF16),
            v((8 * LANES, 128), BF16),
            v((128, LANES), F32),
            v((8, 24, 2 * LANES), F32),
            v((8, 8, 2 * LANES), F32),
            v((8, 144, 2 * LANES), F32),
            v((3, 16, 256), F32),
            v((3, 16, 256), F32),
            v((3, 48, 256), BF16),
            v((8, 32, 2 * LANES), F32),
            v((2, 32, 128), F32),
            v((32, 256), F32),
            v((144, 256), F32),
            v((8, 256), F32),
            v((128, LANES), F32),
            v((24, 256), F32),
            v((128, 128), F32),
            v((128, 128), F32),
            v((128, 128), F32),
            v((128, 128), F32),
            v((128, 128), F32),
            v((8, 128), F32),
            v((128, 128), F32),
            v((128, 128), F32),
            v((128, 128), F32),
            pltpu.SemaphoreType.DMA((6,)),
            pltpu.SemaphoreType.DMA,
            pltpu.SemaphoreType.DMA((3, GROUPS // 2)),
            pltpu.SemaphoreType.DMA((4,)),
            pltpu.SemaphoreType.DMA((4,)),
        ],
        compiler_params=pltpu.CompilerParams(
            collective_id=0, has_side_effects=True, vmem_limit_bytes=56 * 1024 * 1024
        ),
        name="step",
    )(flow, weight, inv_depth, edge_target, rotation, translation)


def hand_over(*results):
    def kernel(depth, pose, depth_out, pose_out):
        depth_out[...] = depth[...]
        pose_out[...] = pose[...]

    vmem = pl.BlockSpec(memory_space=pltpu.VMEM)
    return pl.pallas_call(
        kernel,
        in_specs=[vmem] * 2,
        out_specs=[vmem] * 2,
        out_shape=[jax.ShapeDtypeStruct(r.shape, r.dtype) for r in results],
        compiler_params=pltpu.CompilerParams(vmem_limit_bytes=56 * 1024 * 1024),
        name="hand_over",
    )(*results)


def shards(inv_depth, rotation, translation, edge_target, flow_obs, weight):
    pixels = inv_depth.shape[1]
    flow = flow_obs.reshape(2, 48, pixels)
    wts = weight.reshape(2, 48, pixels)
    depth, pose = hand_over(
        *run_main(flow, wts, inv_depth, edge_target, rotation.T, translation.T)
    )
    return depth, pose.T


def solution(mesh):
    in_specs = (
        P(("row", "col"), None),
        P(None, ("row", "col")),
        P(None, ("row", "col")),
        P(("row", "col"), None),
        P(None, ("row", "col"), None, None),
        P(None, ("row", "col"), None, None),
    )
    out_specs = (P(("row", "col"), None), P(None, ("row", "col")))
    return jax.shard_map(
        shards, mesh=mesh, in_specs=in_specs, out_specs=out_specs, check_vma=False
    )
```

```python
import contextlib
import functools

import jax
import jax.numpy as jnp
from jax import lax
from jax.experimental import pallas as pl
from jax.experimental.pallas import tpu as pltpu
from jax.sharding import PartitionSpec as P

F32 = jnp.float32
BF16 = jnp.bfloat16
NDEV = 128
PX = 24
GROUPS = 16
LANES = 384
MESH = pl.DeviceIdType.MESH
K_PAIRS = [((a, b), n) for n, (a, b) in enumerate((a, b) for a in range(6) for b in range(a, 6))]
K_INDEX = {**dict(K_PAIRS), **{(b, a): n for (a, b), n in K_PAIRS}}
H_ROW = 21


def lane_iota(shape=(8, 128)):
    return lax.broadcasted_iota(jnp.int32, shape, 1)


def pack_half(b, j, turn, flow, weight, low, high, out):
    cols = pl.ds(pl.multiple_of((2 * j + b) * 512, 512), 512)

    def put(ref, block, value):
        at = pl.multiple_of(((3 * turn + block) % 8) * 16, 16)
        ref[pl.ds(at, 16), :] = value

    for k in range(3):
        put(low, k, flow[0, 16 * k : 16 * k + 16, cols])
        put(low, 3 + k, flow[1, 16 * k : 16 * k + 16, cols])
        put(high, 1 + k, weight[1, 16 * k : 16 * k + 16, cols])
    put(low, 6, weight[0, 0:16, cols])
    put(low, 7, weight[0, 16:32, cols])
    put(high, 0, weight[0, 32:48, cols])
    low_t = low[...].T
    high_t = high[...].T
    where_at = (lane_iota() - 48 * turn + 384) % 128
    for d in range(64):
        out[64 * b + d, j, 0:8, :] = low_t[8 * d : 8 * d + 8]
        rest = high_t[8 * d : 8 * d + 8]
        turned = pltpu.roll(pltpu.roll(rest, 64, 1), 4, 0)
        out[64 * b + d, j, 8:12, :] = jnp.where(where_at < 64, rest, turned)[0:4]


def own_edges(target_ref, rotation_ref, translation_ref, ints, floats):
    lane = lane_iota()
    ints[...] = jnp.zeros_like(ints)
    ints[0:2, 0:24] = target_ref[...]
    both = ints[...]
    target = jnp.where(lane < 24, both[0:1], pltpu.roll(both, 24, 1)[1:2])
    x, y, z = (target >> 2) & 3, (target >> 4) & 3, target >> 6
    group = (((z - x) & 3) << 2) + ((y - x) & 3)
    column = ((target & 1) << 7) + (group << 3) + ((target >> 1) & 7)
    floats[...] = jnp.zeros_like(floats)
    floats[0, 0:2, 0:3] = rotation_ref[...]
    floats[1, 0:2, 0:3] = translation_ref[...]
    return column.astype(F32), floats[0] + pltpu.roll(floats[1], 3, 1)


def pack_tables(depth_ref, column, pose, unfold, send):
    lane = lane_iota()
    poses = pltpu.roll(pose, 48, 1)[0:1] + pltpu.roll(pose, 56, 1)[1:2]
    known = jnp.where(lane < 64, poses, pltpu.roll(column, 64, 1)[0:1])
    for f in range(2):
        for j in range(3):
            for g in range(8):
                at = 128 * (8 * j + g)
                unfold[f, j, g : g + 1, :] = depth_ref[f : f + 1, at : at + 128]
    for i in range(16):
        acc = known
        for f in range(2):
            for j in range(3):
                to = 24 * f + 8 * j
                moved = pltpu.roll(unfold[f, j], (to - 8 * i) % 128, 1)
                acc = jnp.where((lane >= to) & (lane < to + 8), moved, acc)
        send[8 * i : 8 * i + 8, :] = acc


def strip(tiles, lane, offset, width):
    out = []
    for t in range(3):
        acc = None
        for i in range(8):
            start = 48 * i + offset
            for wrap in (0, 384, 768):
                a = max(start - wrap, 128 * t) - 128 * t
                b = min(start + width - wrap, 128 * t + 128) - 128 * t
                if a < b:
                    if acc is None:
                        acc = tiles[i]
                    else:
                        acc = jnp.where((lane >= a) & (lane < b), tiles[i], acc)
        out.append(acc)
    return out


def shifted(tiles, lane, shift):
    whole, part = divmod(shift % 384, 128)
    if part == 0:
        return [tiles[(t - whole) % 3] for t in range(3)]
    rolled = [pltpu.roll(t, part, 1) for t in tiles]
    return [
        jnp.where(lane < part, rolled[(t - whole - 1) % 3], rolled[(t - whole) % 3])
        for t in range(3)
    ]


def split3(x):
    top = x.astype(BF16).astype(F32)
    rest = x - top
    mid = rest.astype(BF16).astype(F32)
    return jnp.concatenate([top, mid, rest - mid], 0).astype(BF16)


def join3(y):
    n = y.shape[0] // 3
    return y[:n] + y[n : 2 * n] + y[2 * n :]


def gathered(parts, hot):
    return join3(jnp.dot(parts, hot, preferred_element_type=F32))


def summed(values, hot_t):
    return join3(jnp.dot(split3(values), hot_t, preferred_element_type=F32))


def unpack_group(g, j, recv):
    lane = lane_iota()
    upper = lax.broadcasted_iota(jnp.int32, (8, 128), 0) >= 4
    block_lane = [(lane + 128 * t) % 48 for t in range(3)]
    low = [recv[8 * g + i, j, 0:8, :] for i in range(8)]
    high = [recv[8 * g + i, j, 8:16, :] for i in range(8)]

    def at(tiles, start, width, to):
        return shifted(strip(tiles, lane, start, width), lane, to - start)

    def piece(offset, width, to):
        first, second = at(high, offset, width, to), at(high, offset + 64, width, to)
        return [jnp.where(upper, pltpu.roll(b, 4, 0), a) for a, b in zip(first, second)]

    first, second = at(low, 96, 32, 0), piece(0, 16, 32)
    return [
        at(low, 0, 48, 0),
        at(low, 48, 48, 0),
        [jnp.where(b < 32, f, s) for b, f, s in zip(block_lane, first, second)],
        piece(16, 48, 0),
    ]


def group_targets(g, recv_t):
    lane = lane_iota()
    sub = lax.broadcasted_iota(jnp.int32, (8, 128), 0)
    tile = recv_t[pl.ds(pl.multiple_of(8 * g, 8), 8), :]
    out = [jnp.zeros((8, 128), F32)] * 3
    for i in range(8):
        moved = pltpu.roll(tile, (48 * i - 64) % 128, 1)
        for t in range(3):
            a, b = max(48 * i - 128 * t, 0), min(48 * i + 48 - 128 * t, 128)
            if a < b:
                out[t] = jnp.where((sub == i) & (lane >= a) & (lane < b), moved, out[t])
    return jnp.concatenate([jnp.sum(x, axis=0, keepdims=True) for x in out], 1)


def merge(items):
    sub = lax.broadcasted_iota(jnp.int32, (8, 128), 0)
    items = items[::-1]
    for bit in (0, 1, 2):
        step = 1 << bit
        here = (sub & step) != 0
        items = [
            jnp.where(here, a, b) + pltpu.roll(jnp.where(here, b, a), step, 0)
            for a, b in zip(items[0::2], items[1::2])
        ]
    return items[0]


def merged_rows(rows):
    rows = rows + [jnp.zeros((8, 128), F32)] * (32 - len(rows))
    return jnp.concatenate([merge(rows[k : k + 8]) for k in range(0, 32, 8)], 0)


def pixel_xy(me, j):
    p = 8 * NDEV * j + 8 * me + lax.broadcasted_iota(jnp.int32, (8, 128), 0)
    x = ((p % 64).astype(F32) + 0.5) / 64 - 0.5
    y = ((p // 64).astype(F32) + 0.5 - 24.0) / 64
    return x, y


def expand(rows, own, out):
    lane = lane_iota()
    mine = [
        jnp.where(
            lane < 8,
            pltpu.roll(rows[:, 0:128], (128 - 8 * g) % 128, 1),
            pltpu.roll(rows[:, 128:256], (136 - 8 * g) % 128, 1),
        )
        for g in range(GROUPS)
    ]
    out[...] = gathered(split3(jnp.concatenate(mine, 0)), own[...])


def rows_of(ref, g):
    return ref[pl.ds(pl.multiple_of(8 * g, 8), 8), :]


def edge_rows(a, j):
    return slice(24 * a + 8 * j, 24 * a + 8 * j + 8)


def add_block(acc, row, value):
    acc[row] = value if acc[row] is None else acc[row] + value


def source_columns():
    rows = lax.broadcasted_iota(jnp.int32, (128, LANES), 0)
    frame = lax.broadcasted_iota(jnp.int32, (1, LANES), 1) // 24
    return jnp.where(rows == (frame % 2) * 8 + frame // 2, 1.0, 0.0).astype(BF16)


def source_columns_t():
    edge = lax.broadcasted_iota(jnp.int32, (8 * LANES, 1), 0)
    frame = (edge % LANES) // 24
    lanes = lax.broadcasted_iota(jnp.int32, (8 * LANES, 128), 1)
    at = (edge // LANES) * 16 + (frame % 2) * 8 + frame // 2
    return jnp.where(lanes == at, 1.0, 0.0).astype(BF16)


def build_terms(acc, cols, inputs, d, rel, xy, coup, m, j):
    x, y = xy
    fu, fv, cu, cv = inputs
    w0, w1, w2, m0, m1, m2 = [rel[k : 1 + k, cols] for k in range(6)]
    x0 = x + w1 - w2 * y + m0 * d
    x1 = y + w2 * x - w0 + m1 * d
    x2 = 1.0 + w0 * y - w1 * x + m2 * d
    q = 1.0 / x2
    u = x0 * q
    v = x1 * q
    ru = fu - (u - x)
    rv = fv - (v - y)
    du = q * (m0 - u * m2)
    dv = q * (m1 - v * m2)
    eu = cu * du
    ev = cv * dv
    dq = d * q
    ju = {0: -(u * y) * q, 1: (1.0 + u * x) * q, 2: -y * q, 3: dq, 5: -u * dq}
    jv = {0: (-1.0 - v * y) * q, 1: v * x * q, 2: x * q, 4: dq, 5: -v * dq}
    for a in range(6):
        if a in ju and a in jv:
            e = ju[a] * eu + jv[a] * ev
        else:
            e = ju[a] * eu if a in ju else jv[a] * ev
        coup[m, edge_rows(a, j), cols] = e
    su = {a: cu * ju[a] for a in ju}
    sv = {a: cv * jv[a] for a in jv}
    for (a, b), row in K_PAIRS:
        if a in ju and b in ju:
            add_block(acc, row, su[a] * ju[b])
        if a in jv and b in jv:
            add_block(acc, row, sv[a] * jv[b])
    for a in range(6):
        if a in ju:
            add_block(acc, H_ROW + a, su[a] * ru)
        if a in jv:
            add_block(acc, H_ROW + a, sv[a] * rv)
    return eu * ru + ev * rv, eu * du + ev * dv


def take_terms(acc, cols, near, coup, m, j):
    ci, gi = -near[0], -near[1]
    e = [coup[m, edge_rows(a, j), cols] for a in range(6)]
    for a in range(6):
        scaled = e[a] * ci
        for (k, b), row in K_PAIRS:
            if k == a:
                add_block(acc, row, scaled * e[b])
        add_block(acc, H_ROW + a, e[a] * gi)


def filled(acc):
    return [jnp.zeros((8, 128), F32) if x is None else x for x in acc]


def tile_cols(t):
    return slice(128 * t, 128 * t + 128)


def pair_at(m, count=1):
    size = 2 * LANES * count
    return pl.ds(pl.multiple_of(size * m, 128), size)


def phase_pass(
    m, j, gs, me, recv, recv_t, table3, hot, hot_t, from_pose, dep, rel, coup, sums, inverse3, kh
):
    at = pair_at(m)
    if j == 0:
        rows = lax.broadcasted_iota(jnp.int32, (256, 2 * LANES), 0).astype(F32)
        targets = jnp.concatenate([group_targets(g, recv_t) for g in gs], 1)
        hot[:, at] = jnp.where(rows == targets, 1.0, 0.0).astype(BF16)
        lanes = lane_iota((128, 256)).astype(F32)
        for t in range(6):
            column = jnp.broadcast_to(targets[:, tile_cols(t)], (128, 128)).T
            column = jnp.concatenate([column, column], 1)
            to = pl.ds(pl.multiple_of(2 * LANES * m + 128 * t, 128), 128)
            hot_t[to, :] = jnp.where(lanes == column, 1.0, 0.0).astype(BF16)
        near = gathered(table3[...], hot[:, at])
        dep[m] = near[0:24]
        relative = jnp.concatenate([rows_of(from_pose, g) for g in gs], 1) - near[24:32]
        rel[m] = relative
    else:
        relative = rel[m]
        back = gathered(inverse3[j - 1], hot[:, at])
    parts = [unpack_group(g, j, recv) for g in gs]
    grads, curvs, blocks = [], [], []
    xy = pixel_xy(me, j)
    for t in range(6):
        cols = tile_cols(t)
        acc = [None] * 27
        d = dep[m, 8 * j : 8 * j + 8, cols]
        tiles = [part[t % 3] for part in parts[t // 3]]
        gd, cd = build_terms(acc, cols, tiles, d, relative, xy, coup, m, j)
        grads.append(gd)
        curvs.append(cd)
        if j > 0:
            take_terms(acc, cols, (back[0:8, cols], back[8:16, cols]), coup, m, j - 1)
        blocks.append(merged_rows(filled(acc)))
    both = jnp.concatenate([jnp.concatenate(grads, 1), jnp.concatenate(curvs, 1)], 0)
    sums[j] += summed(both, hot_t[at, :])
    block = jnp.concatenate(blocks, 1)
    kh[m] = block if j == 0 else kh[m] + block


def last_pass(h, hot, hot_t, own_t, coup, inverse3, kh, total_s, total_t):
    at = pair_at(h, 4)
    near = gathered(inverse3[2], hot[:, at])
    blocks = []
    for t in range(24):
        m = 4 * h + t // 6
        acc = [None] * 27
        cols = tile_cols(t)
        take_terms(acc, tile_cols(t % 6), (near[0:8, cols], near[8:16, cols]), coup, m, 2)
        blocks.append(kh[m, :, tile_cols(t % 6)] + merged_rows(acc))
    parts = split3(jnp.concatenate(blocks, 1))
    total_t[...] += join3(jnp.dot(parts, hot_t[at, :], preferred_element_type=F32))
    total_s[h] = join3(jnp.dot(parts, own_t[...], preferred_element_type=F32))


def third_pass(h, gs, hot_t, coup, from_steps, fix):
    parts = []
    for t in range(24):
        m, cols = 4 * h + t // 6, tile_cols(t % 6)
        motion = rows_of(from_steps, gs[t // 3])
        column = []
        for j in range(3):
            terms = [
                coup[m, edge_rows(a, j), cols] * motion[a : a + 1, tile_cols(t % 3)]
                for a in range(6)
            ]
            column.append(((terms[0] + terms[1]) + (terms[2] + terms[3])) + (terms[4] + terms[5]))
        parts.append(jnp.concatenate(column, 0))
    fix[...] += summed(jnp.concatenate(parts, 1), hot_t[pair_at(h, 4), :])


def solve(matrix, right):
    factor = {}
    for i in range(6):
        for j in range(i + 1):
            e = matrix(i, j)
            if i == j:
                e = e * 1.1 + 0.001
            for k in range(j):
                e = e - factor[i, k] * factor[j, k]
            factor[i, j] = jnp.sqrt(e) if i == j else e / factor[j, j]
    forward = []
    for i in range(6):
        e = right(i)
        for k in range(i):
            e = e - factor[i, k] * forward[k]
        forward.append(e / factor[i, i])
    z = [None] * 6
    for i in reversed(range(6)):
        e = forward[i]
        for k in range(i + 1, 6):
            e = e - factor[k, i] * z[k]
        z[i] = e / factor[i, i]
    return z


def ring_steps(d):
    return min(d, 4 - d)


def hops(offset):
    return ring_steps(offset[0]) + ring_steps(offset[1]) + ring_steps(offset[2])


def far_first():
    offsets = [
        (dz, dy, dx, dc)
        for dz in range(4)
        for dy in range(4)
        for dx in range(4)
        for dc in range(2)
        if (dz, dy, dx, dc) != (0, 0, 0, 0)
    ]
    return sorted(offsets, key=lambda o: -hops(o))


def group_offset(n):
    return (n // 4 + n) % 4, n % 4


def pair_order(m, far_ahead):
    order = []
    for n in (2 * m, 2 * m + 1):
        oz, oy = group_offset(n)
        members = [
            ((oz + dx) % 4, (oy + dx) % 4, dx, dc) for dx in range(4) for dc in range(2)
        ]
        order += sorted(members, key=lambda o: -hops(o)) if far_ahead else members
    return [o for o in order if o != (0, 0, 0, 0)]


def to_all(order, act):
    row, col = lax.axis_index("row"), lax.axis_index("col")
    y, x = col // 8, (col // 2) % 4
    zs = [((row + d) % 4) * 32 for d in range(4)]
    ys = [((y + d) % 4) * 8 for d in range(4)]
    xs = [((x + d) % 4) * 2 for d in range(4)]
    cs = [(col + d) % 2 for d in range(2)]
    gz = [((row + 4 - x + d) % 4) * 32 for d in range(4)]
    gy = [((y + 4 - x + d) % 4) * 8 for d in range(4)]
    for dz, dy, dx, dc in order:
        last = xs[dx] + cs[dc]
        act(zs[dz] + ys[dy] + last, gz[(dz - dx) % 4] + gy[(dy - dx) % 4] + last)


def slot_of(d):
    return (d % 16) * 8 + d // 16


def rows_exchange(send, recv, source, slot, send_sem, recv_sem):
    def act(d, place):
        pltpu.make_async_remote_copy(
            src_ref=send.at[pl.ds(source(d, place), 1), :],
            dst_ref=recv.at[pl.ds(slot, 1), :],
            send_sem=send_sem,
            recv_sem=recv_sem,
            device_id=d,
            device_id_type=pl.DeviceIdType.LOGICAL,
        ).start()

    to_all(far_first(), act)


def steps_exchange(order, send, source, recv, slot, send_sem, recv_sem):
    def act(d, _):
        pltpu.make_async_remote_copy(
            src_ref=send.at[pl.ds(source, 1), :],
            dst_ref=recv.at[pl.ds(slot, 1), :],
            send_sem=send_sem,
            recv_sem=recv_sem,
            device_id=d,
            device_id_type=pl.DeviceIdType.LOGICAL,
        ).start()

    to_all(order, act)


def rows_wait(buf, sem, count=NDEV - 1):
    ref = buf.at[pl.ds(0, count), :]
    pltpu.make_async_copy(ref, ref, sem).wait()


def scope(name):
    return contextlib.nullcontext()


def loop(body, count):
    def step(n, carry):
        body(n)
        return carry

    lax.fori_loop(0, count, step, 0)


def main_kernel(
    flow_hbm, weight_hbm, depth_hbm, target_hbm, rotation_hbm, translation_hbm,
    recv_f, pose_hbm,
    flow, weight, depth_ref, target_ref, rotation_ref, translation_ref, low, high, chunks, ints, floats, unfold,
    recv, table, table3, hot, hot_t, own, own_t, from_pose, dep, rel, coup, sums, inverse,
    inverse3, kh,
    total_s, total_t, at_target, steps, from_steps, fix,
    send_t, recv_t, sum_d, send_d, recv_d, send_e, recv_e, send_f, pose_ref,
    in_sem, out_sem, big_send, big_recv, small_send, small_recv,
):
    row, col = lax.axis_index("row"), lax.axis_index("col")
    me = row * 32 + col
    y, x = col // 8, (col // 2) % 4
    my_gz, my_gy = (row + 4 - x) % 4, (y + 4 - x) % 4
    my_group = my_gz * 4 + my_gy
    mine_at = my_group * 8 + col % 8
    other_at = my_group * 8 + (col + 4) % 8
    lane = lane_iota()
    barrier = pltpu.get_barrier_semaphore()

    inputs = [
        (depth_hbm, depth_ref),
        (target_hbm, target_ref),
        (rotation_hbm, rotation_ref),
        (translation_hbm, translation_ref),
        (flow_hbm, flow),
        (weight_hbm, weight),
    ]
    loads = [
        pltpu.make_async_copy(source, to, in_sem.at[k]) for k, (source, to) in enumerate(inputs)
    ]

    def greet(d, _):
        pl.semaphore_signal(
            barrier, inc=1, device_id=d, device_id_type=pl.DeviceIdType.LOGICAL
        )

    with scope("sc_greet"):
        for load in loads:
            load.start()
        to_all(far_first(), greet)

    with scope("sc_tables"):
        high[...] = jnp.zeros_like(high)
        for load in loads[:4]:
            load.wait()
        column, pose = own_edges(target_ref, rotation_ref, translation_ref, ints, floats)
        pack_tables(depth_ref, column, pose, unfold, send_t)
        recv_t[pl.ds(mine_at, 1), :] = send_t[pl.ds(slot_of(me), 1), :]
        turn = col % 8
        for load in loads[4:]:
            load.wait()

    def pack(j):
        def step(b, carry):
            pack_half(b, j, turn, flow, weight, low, high, chunks)
            return carry

        lax.fori_loop(0, 2, step, 0)

    with scope("sc_pack"):
        pack(0)
    with scope("sc_barrier"):
        pl.semaphore_wait(barrier, NDEV - 1)

    with scope("sc_sends"):
        rows_exchange(
            send_t, recv_t, lambda d, _: slot_of(d), mine_at, small_send.at[3], small_recv.at[3]
        )

        def send_phase(j):
            for m in range(8):

                def send_chunk(d, _):
                    pltpu.make_async_remote_copy(
                        src_ref=chunks.at[d, j, pl.ds(0, 12), :],
                        dst_ref=recv.at[mine_at, j, pl.ds(0, 12), :],
                        send_sem=big_send,
                        recv_sem=big_recv.at[j, m],
                        device_id=d,
                        device_id_type=pl.DeviceIdType.LOGICAL,
                    ).start()

                to_all(pair_order(m, j == 2), send_chunk)

        send_phase(0)
        pack(1)
        pack(2)
        send_phase(1)
        send_phase(2)
        recv[mine_at, :, 0:12, :] = chunks[me, :, 0:12, :]

    with scope("sc_waitt"):
        for ref in (sums, total_t, fix, at_target):
            ref[...] = jnp.zeros_like(ref)
        own[...] = source_columns()
        own_t[...] = source_columns_t()
        rows_wait(recv_t, small_recv.at[3])
        known = recv_t[...].T
        for f in range(2):
            at = slice(128 * f, 128 * f + 128)
            table[0:24, at] = known[24 * f : 24 * f + 24]
            table[24:32, at] = known[48 + 8 * f : 56 + 8 * f]
        table3[...] = split3(table[...])
        expand(table[24:32, :], own, from_pose)

    def group_at(n):
        oz, oy = group_offset(n)
        return ((my_gz + 4 - oz) % 4) * 4 + (my_gy + 4 - oy) % 4

    def arrive(m, j):
        gs = [group_at(2 * m), group_at(2 * m + 1)]

        def landed(count):
            ref = recv.at[pl.ds(0, count), j, pl.ds(0, 12), :]
            pltpu.make_async_copy(ref, ref, big_recv.at[j, m]).wait()

        pl.when(m == 0)(lambda: landed(15))
        pl.when(m != 0)(lambda: landed(16))
        phase_pass(
            m, j, gs, me, recv, recv_t, table3, hot, hot_t, from_pose, dep, rel, coup, sums,
            inverse3, kh,
        )

    for j in range(3):
        with scope(f"sc_arrive{j}"):
            loop(functools.partial(arrive, j=j), 8)
            ci = 1.0 / (0.1 + sums[j, 8:16])
            both = jnp.concatenate([ci, sums[j, 0:8] * ci], 0)
            inverse[j] = both
            inverse3[j] = split3(both)
    with scope("sc_last"):
        loop(lambda h: last_pass(h, hot, hot_t, own_t, coup, inverse3, kh, total_s, total_t), 2)

    with scope("sc_sendd"):
        kind = lax.broadcasted_iota(jnp.int32, (32, 256), 0)
        total = jnp.where(kind < H_ROW, total_t[...], -total_t[...])
        by_target = jnp.concatenate(
            [total[:, 0:128], total[:, 128:256], jnp.zeros((64, 128), F32)], 0
        ).T
        for h in range(2):
            by_source = jnp.concatenate([total_s[h], jnp.zeros((96, 128), F32)], 0).T
            for k in range(8):
                to = pl.ds(pl.multiple_of(8 * group_at(8 * h + k), 8), 8)
                first, second = by_source[16 * k : 16 * k + 8], by_source[16 * k + 8 : 16 * k + 16]
                sum_d[to, :] = first + pltpu.roll(second, 32, 1)
        rows = by_target + sum_d[...]
        opposite = [pltpu.roll(rows[8 * g : 8 * g + 8], 4, 0) for g in range(GROUPS)]
        send_d[...] = rows + pltpu.roll(jnp.concatenate(opposite, 0), 64, 1)
        recv_d[pl.ds(mine_at, 1), :] = send_d[pl.ds(mine_at, 1), :]
        rows_exchange(
            send_d, recv_d, lambda _, place: place, mine_at, small_send.at[0], small_recv.at[0]
        )
    with scope("sc_target"):

        def couple(m):
            at_target[...] += summed(coup[m], hot_t[pair_at(m), :])

        loop(couple, 8)
    with scope("sc_waitd"):
        rows_wait(recv_d, small_recv.at[0])
    with scope("sc_solve"):
        line = jnp.sum(recv_d[...], axis=0, keepdims=True)
        sub = lax.broadcasted_iota(jnp.int32, (8, 128), 0)
        lines = jnp.broadcast_to(line, (8, 128))
        for f in range(1, 4):
            lines = jnp.where(sub == f, pltpu.roll(lines, 128 - 32 * f, 1), lines)
        full = jnp.concatenate([lines, jnp.zeros((120, 128), F32)], 0).T
        z = solve(
            lambda i, j: full[K_INDEX[i, j] : K_INDEX[i, j] + 1, :],
            lambda i: full[H_ROW + i : H_ROW + i + 1, :],
        )
        zs = jnp.concatenate([*z, jnp.zeros((122, 128), F32)], 0)
        turned = zs.T
        pose_ref[...] = turned[0:2, 0:6]
        pose_out = pltpu.make_async_copy(pose_ref, pose_hbm, out_sem.at[0])
        pose_out.start()
        later = pltpu.roll(turned[0:8], 8, 1)
        mine, other = turned[0:1] + later[1:2], turned[2:3] + later[3:4]
        send_e[...] = jnp.where(sub == 0, mine, other)
        recv_e[pl.ds(mine_at, 1), :] = mine
        recv_e[pl.ds(other_at, 1), :] = other
    with scope("sc_sende"):
        near = [o for o in far_first() if hops(o) <= 3]
        steps_exchange(near, send_e, 0, recv_e, mine_at, small_send.at[1], small_recv.at[1])
        near = [o for o in near if hops(o) <= 2]
        steps_exchange(near, send_e, 1, recv_e, other_at, small_send.at[1], small_recv.at[1])
    with scope("sc_waite"):
        rows_wait(recv_e, small_recv.at[1], NDEV - 2)
    with scope("sc_third"):
        every = recv_e[...].T
        steps[:, 0:128] = every[0:8]
        steps[:, 128:256] = every[8:16]
        expand(steps[...], own, from_steps)
        loop(
            lambda h: third_pass(
                h, [group_at(8 * h + k) for k in range(8)], hot_t, coup, from_steps, fix
            ),
            2,
        )
    with scope("sc_sendf"):
        back = at_target[0:24] * steps[0:1]
        for a in range(1, 6):
            back += at_target[24 * a : 24 * a + 24] * steps[a : a + 1]
        grad = jnp.concatenate([sums[j, 0:8] for j in range(3)], 0)
        ci = jnp.concatenate([inverse[j, 0:8] for j in range(3)], 0)
        new = table[0:24] + (grad - (fix[...] - back)) * ci
        zero8 = jnp.zeros((8, 128), F32)
        send_f[...] = jnp.concatenate(
            [new[:, 0:128], zero8, new[:, 128:256], zero8, jnp.zeros((64, 128), F32)], 0
        ).T
        slot = slot_of(me)
        own_row = pltpu.make_async_copy(
            send_f.at[pl.ds(mine_at, 1), :], recv_f.at[pl.ds(slot, 1), :], out_sem.at[1]
        )
        own_row.start()
        rows_exchange(
            send_f, recv_f, lambda _, place: place, slot, small_send.at[2], small_recv.at[2]
        )
    with scope("sc_waitf"):
        rows_wait(recv_f, small_recv.at[2])
    own_row.wait()
    pose_out.wait()
    ref = chunks.at[pl.ds(0, NDEV - 1), :, pl.ds(0, 12), :]
    pltpu.make_async_copy(ref, ref, big_send).wait()
    rows_wait(recv_t, small_send.at[3])
    rows_wait(recv_d, small_send.at[0])
    rows_wait(recv_e, small_send.at[1], NDEV - 2)
    rows_wait(recv_f, small_send.at[2])


def run_main(flow, weight, inv_depth, edge_target, rotation, translation):
    v = pltpu.VMEM
    hbm = pl.BlockSpec(memory_space=pltpu.HBM)
    return pl.pallas_call(
        main_kernel,
        in_specs=[hbm] * 6,
        out_specs=[hbm] * 2,
        out_shape=[
            jax.ShapeDtypeStruct((NDEV, 128), F32),
            jax.ShapeDtypeStruct((2, 6), F32),
        ],
        scratch_shapes=[
            v((2, 48, PX * NDEV), F32),
            v((2, 48, PX * NDEV), F32),
            v((2, PX * NDEV), F32),
            v((2, 24), jnp.int32),
            v((2, 3), F32),
            v((2, 3), F32),
            v((128, 512), F32),
            v((128, 512), F32),
            v((NDEV, 3, 16, 128), F32),
            v((8, 128), jnp.int32),
            v((2, 8, 128), F32),
            v((2, 3, 8, 128), F32),
            v((NDEV, 3, 16, 128), F32),
            v((32, 256), F32),
            v((96, 256), BF16),
            v((256, GROUPS * LANES), BF16),
            v((GROUPS * LANES, 256), BF16),
            v((128, LANES), BF16),
            v((8 * LANES, 128), BF16),
            v((128, LANES), F32),
            v((8, 24, 2 * LANES), F32),
            v((8, 8, 2 * LANES), F32),
            v((8, 144, 2 * LANES), F32),
            v((3, 16, 256), F32),
            v((3, 16, 256), F32),
            v((3, 48, 256), BF16),
            v((8, 32, 2 * LANES), F32),
            v((2, 32, 128), F32),
            v((32, 256), F32),
            v((144, 256), F32),
            v((8, 256), F32),
            v((128, LANES), F32),
            v((24, 256), F32),
            v((128, 128), F32),
            v((128, 128), F32),
            v((128, 128), F32),
            v((128, 128), F32),
            v((128, 128), F32),
            v((8, 128), F32),
            v((128, 128), F32),
            v((128, 128), F32),
            v((2, 6), F32),
            pltpu.SemaphoreType.DMA((6,)),
            pltpu.SemaphoreType.DMA((2,)),
            pltpu.SemaphoreType.DMA,
            pltpu.SemaphoreType.DMA((3, GROUPS // 2)),
            pltpu.SemaphoreType.DMA((4,)),
            pltpu.SemaphoreType.DMA((4,)),
        ],
        compiler_params=pltpu.CompilerParams(
            collective_id=0, has_side_effects=True, vmem_limit_bytes=56 * 1024 * 1024
        ),
        name="step",
    )(flow, weight, inv_depth, edge_target, rotation, translation)


def hand_over(parts, pose):
    def kernel(recv_f, pose_ref, out_ref, pose_out):
        lane = lane_iota()
        pose_out[...] = pose_ref[...]
        for f in range(2):
            for j in range(3):
                tile = None
                for i in range(16):
                    shift = 8 * i - 32 * f - 8 * j
                    moved = pltpu.roll(recv_f[8 * i : 8 * i + 8, :], shift % 128, 1)
                    tile = moved if i == 0 else jnp.where(lane >= 8 * i, moved, tile)
                for g in range(8):
                    at = 128 * (8 * j + g)
                    out_ref[f : f + 1, at : at + 128] = tile[g : g + 1]

    vmem = pl.BlockSpec(memory_space=pltpu.VMEM)
    return pl.pallas_call(
        kernel,
        in_specs=[vmem] * 2,
        out_specs=[vmem] * 2,
        out_shape=[
            jax.ShapeDtypeStruct((2, PX * NDEV), F32),
            jax.ShapeDtypeStruct((2, 6), F32),
        ],
        compiler_params=pltpu.CompilerParams(vmem_limit_bytes=56 * 1024 * 1024),
        name="hand_over",
    )(parts, pose)


def shards(inv_depth, rotation, translation, edge_target, flow_obs, weight):
    pixels = inv_depth.shape[1]
    flow = flow_obs.reshape(2, 48, pixels)
    wts = weight.reshape(2, 48, pixels)
    depth, pose = hand_over(
        *run_main(flow, wts, inv_depth, edge_target, rotation.T, translation.T)
    )
    return depth, pose.T


def solution(mesh):
    in_specs = (
        P(("row", "col"), None),
        P(None, ("row", "col")),
        P(None, ("row", "col")),
        P(("row", "col"), None),
        P(None, ("row", "col"), None, None),
        P(None, ("row", "col"), None, None),
    )
    out_specs = (P(("row", "col"), None), P(None, ("row", "col")))
    return jax.shard_map(
        shards, mesh=mesh, in_specs=in_specs, out_specs=out_specs, check_vma=False
    )
```

```python
import contextlib
import functools

import jax
import jax.numpy as jnp
from jax import lax
from jax.experimental import pallas as pl
from jax.experimental.pallas import tpu as pltpu
from jax.sharding import PartitionSpec as P

F32 = jnp.float32
BF16 = jnp.bfloat16
NDEV = 128
PX = 24
GROUPS = 16
LANES = 384
MESH = pl.DeviceIdType.MESH
K_PAIRS = [((a, b), n) for n, (a, b) in enumerate((a, b) for a in range(6) for b in range(a, 6))]
K_INDEX = {**dict(K_PAIRS), **{(b, a): n for (a, b), n in K_PAIRS}}
H_ROW = 21


def lane_iota(shape=(8, 128)):
    return lax.broadcasted_iota(jnp.int32, shape, 1)


def pack_half(b, j, turn, flow, weight, low, high, out):
    cols = pl.ds(pl.multiple_of((2 * j + b) * 512, 512), 512)

    def put(ref, block, value):
        at = pl.multiple_of(((3 * turn + block) % 8) * 16, 16)
        ref[pl.ds(at, 16), :] = value

    for k in range(3):
        put(low, k, flow[0, 16 * k : 16 * k + 16, cols])
        put(low, 3 + k, flow[1, 16 * k : 16 * k + 16, cols])
        put(high, 1 + k, weight[1, 16 * k : 16 * k + 16, cols])
    put(low, 6, weight[0, 0:16, cols])
    put(low, 7, weight[0, 16:32, cols])
    put(high, 0, weight[0, 32:48, cols])
    low_t = low[...].T
    high_t = high[...].T
    where_at = (lane_iota() - 48 * turn + 384) % 128
    for d in range(64):
        out[64 * b + d, j, 0:8, :] = low_t[8 * d : 8 * d + 8]
        rest = high_t[8 * d : 8 * d + 8]
        turned = pltpu.roll(pltpu.roll(rest, 64, 1), 4, 0)
        out[64 * b + d, j, 8:12, :] = jnp.where(where_at < 64, rest, turned)[0:4]


def own_edges(target_ref, rotation_ref, translation_ref, ints, floats):
    lane = lane_iota()
    ints[...] = jnp.zeros_like(ints)
    ints[0:2, 0:24] = target_ref[...]
    both = ints[...]
    target = jnp.where(lane < 24, both[0:1], pltpu.roll(both, 24, 1)[1:2])
    x, y, z = (target >> 2) & 3, (target >> 4) & 3, target >> 6
    group = (((z - x) & 3) << 2) + ((y - x) & 3)
    column = ((target & 1) << 7) + (group << 3) + ((target >> 1) & 7)
    floats[...] = jnp.zeros_like(floats)
    floats[0, 0:2, 0:3] = rotation_ref[...]
    floats[1, 0:2, 0:3] = translation_ref[...]
    return column.astype(F32), floats[0] + pltpu.roll(floats[1], 3, 1)


def pack_tables(depth_ref, column, pose, unfold, send):
    lane = lane_iota()
    poses = pltpu.roll(pose, 48, 1)[0:1] + pltpu.roll(pose, 56, 1)[1:2]
    known = jnp.where(lane < 64, poses, pltpu.roll(column, 64, 1)[0:1])
    for f in range(2):
        for j in range(3):
            for g in range(8):
                at = 128 * (8 * j + g)
                unfold[f, j, g : g + 1, :] = depth_ref[f : f + 1, at : at + 128]
    for i in range(16):
        acc = known
        for f in range(2):
            for j in range(3):
                to = 24 * f + 8 * j
                moved = pltpu.roll(unfold[f, j], (to - 8 * i) % 128, 1)
                acc = jnp.where((lane >= to) & (lane < to + 8), moved, acc)
        send[8 * i : 8 * i + 8, :] = acc


def strip(tiles, lane, offset, width):
    out = []
    for t in range(3):
        acc = None
        for i in range(8):
            start = 48 * i + offset
            for wrap in (0, 384, 768):
                a = max(start - wrap, 128 * t) - 128 * t
                b = min(start + width - wrap, 128 * t + 128) - 128 * t
                if a < b:
                    if acc is None:
                        acc = tiles[i]
                    else:
                        acc = jnp.where((lane >= a) & (lane < b), tiles[i], acc)
        out.append(acc)
    return out


def shifted(tiles, lane, shift):
    whole, part = divmod(shift % 384, 128)
    if part == 0:
        return [tiles[(t - whole) % 3] for t in range(3)]
    rolled = [pltpu.roll(t, part, 1) for t in tiles]
    return [
        jnp.where(lane < part, rolled[(t - whole - 1) % 3], rolled[(t - whole) % 3])
        for t in range(3)
    ]


def split3(x):
    top = x.astype(BF16).astype(F32)
    rest = x - top
    mid = rest.astype(BF16).astype(F32)
    return jnp.concatenate([top, mid, rest - mid], 0).astype(BF16)


def join3(y):
    n = y.shape[0] // 3
    return y[:n] + y[n : 2 * n] + y[2 * n :]


def gathered(parts, hot):
    return join3(jnp.dot(parts, hot, preferred_element_type=F32))


def summed(values, hot_t):
    return join3(jnp.dot(split3(values), hot_t, preferred_element_type=F32))


def unpack_group(g, j, recv):
    lane = lane_iota()
    upper = lax.broadcasted_iota(jnp.int32, (8, 128), 0) >= 4
    block_lane = [(lane + 128 * t) % 48 for t in range(3)]
    low = [recv[8 * g + i, j, 0:8, :] for i in range(8)]
    high = [recv[8 * g + i, j, 8:16, :] for i in range(8)]

    def at(tiles, start, width, to):
        return shifted(strip(tiles, lane, start, width), lane, to - start)

    def piece(offset, width, to):
        first, second = at(high, offset, width, to), at(high, offset + 64, width, to)
        return [jnp.where(upper, pltpu.roll(b, 4, 0), a) for a, b in zip(first, second)]

    first, second = at(low, 96, 32, 0), piece(0, 16, 32)
    return [
        at(low, 0, 48, 0),
        at(low, 48, 48, 0),
        [jnp.where(b < 32, f, s) for b, f, s in zip(block_lane, first, second)],
        piece(16, 48, 0),
    ]


def group_targets(g, recv_t):
    lane = lane_iota()
    sub = lax.broadcasted_iota(jnp.int32, (8, 128), 0)
    tile = recv_t[pl.ds(pl.multiple_of(8 * g, 8), 8), :]
    out = [jnp.zeros((8, 128), F32)] * 3
    for i in range(8):
        moved = pltpu.roll(tile, (48 * i - 64) % 128, 1)
        for t in range(3):
            a, b = max(48 * i - 128 * t, 0), min(48 * i + 48 - 128 * t, 128)
            if a < b:
                out[t] = jnp.where((sub == i) & (lane >= a) & (lane < b), moved, out[t])
    return jnp.concatenate([jnp.sum(x, axis=0, keepdims=True) for x in out], 1)


def merge(items):
    sub = lax.broadcasted_iota(jnp.int32, (8, 128), 0)
    items = items[::-1]
    for bit in (0, 1, 2):
        step = 1 << bit
        here = (sub & step) != 0
        items = [
            jnp.where(here, a, b) + pltpu.roll(jnp.where(here, b, a), step, 0)
            for a, b in zip(items[0::2], items[1::2])
        ]
    return items[0]


def merged_rows(rows):
    rows = rows + [jnp.zeros((8, 128), F32)] * (32 - len(rows))
    return jnp.concatenate([merge(rows[k : k + 8]) for k in range(0, 32, 8)], 0)


def pixel_xy(me, j):
    p = 8 * NDEV * j + 8 * me + lax.broadcasted_iota(jnp.int32, (8, 128), 0)
    x = ((p % 64).astype(F32) + 0.5) / 64 - 0.5
    y = ((p // 64).astype(F32) + 0.5 - 24.0) / 64
    return x, y


def expand(rows, own, out):
    lane = lane_iota()
    mine = [
        jnp.where(
            lane < 8,
            pltpu.roll(rows[:, 0:128], (128 - 8 * g) % 128, 1),
            pltpu.roll(rows[:, 128:256], (136 - 8 * g) % 128, 1),
        )
        for g in range(GROUPS)
    ]
    out[...] = gathered(split3(jnp.concatenate(mine, 0)), own[...])


def rows_of(ref, g):
    return ref[pl.ds(pl.multiple_of(8 * g, 8), 8), :]


def edge_rows(a, j):
    return slice(24 * a + 8 * j, 24 * a + 8 * j + 8)


def add_block(acc, row, value):
    acc[row] = value if acc[row] is None else acc[row] + value


def source_columns():
    rows = lax.broadcasted_iota(jnp.int32, (128, LANES), 0)
    frame = lax.broadcasted_iota(jnp.int32, (1, LANES), 1) // 24
    return jnp.where(rows == (frame % 2) * 8 + frame // 2, 1.0, 0.0).astype(BF16)


def source_columns_t():
    edge = lax.broadcasted_iota(jnp.int32, (8 * LANES, 1), 0)
    frame = (edge % LANES) // 24
    lanes = lax.broadcasted_iota(jnp.int32, (8 * LANES, 128), 1)
    at = (edge // LANES) * 16 + (frame % 2) * 8 + frame // 2
    return jnp.where(lanes == at, 1.0, 0.0).astype(BF16)


def build_terms(acc, cols, inputs, d, rel, xy, coup, m, j):
    x, y = xy
    fu, fv, cu, cv = inputs
    w0, w1, w2, m0, m1, m2 = [rel[k : 1 + k, cols] for k in range(6)]
    x0 = x + w1 - w2 * y + m0 * d
    x1 = y + w2 * x - w0 + m1 * d
    x2 = 1.0 + w0 * y - w1 * x + m2 * d
    q = 1.0 / x2
    u = x0 * q
    v = x1 * q
    ru = fu - (u - x)
    rv = fv - (v - y)
    du = q * (m0 - u * m2)
    dv = q * (m1 - v * m2)
    eu = cu * du
    ev = cv * dv
    dq = d * q
    ju = {0: -(u * y) * q, 1: (1.0 + u * x) * q, 2: -y * q, 3: dq, 5: -u * dq}
    jv = {0: (-1.0 - v * y) * q, 1: v * x * q, 2: x * q, 4: dq, 5: -v * dq}
    for a in range(6):
        if a in ju and a in jv:
            e = ju[a] * eu + jv[a] * ev
        else:
            e = ju[a] * eu if a in ju else jv[a] * ev
        coup[m, edge_rows(a, j), cols] = e
    su = {a: cu * ju[a] for a in ju}
    sv = {a: cv * jv[a] for a in jv}
    for (a, b), row in K_PAIRS:
        if a in ju and b in ju:
            add_block(acc, row, su[a] * ju[b])
        if a in jv and b in jv:
            add_block(acc, row, sv[a] * jv[b])
    for a in range(6):
        if a in ju:
            add_block(acc, H_ROW + a, su[a] * ru)
        if a in jv:
            add_block(acc, H_ROW + a, sv[a] * rv)
    return eu * ru + ev * rv, eu * du + ev * dv


def take_terms(acc, cols, near, coup, m, j):
    ci, gi = -near[0], -near[1]
    e = [coup[m, edge_rows(a, j), cols] for a in range(6)]
    for a in range(6):
        scaled = e[a] * ci
        for (k, b), row in K_PAIRS:
            if k == a:
                add_block(acc, row, scaled * e[b])
        add_block(acc, H_ROW + a, e[a] * gi)


def filled(acc):
    return [jnp.zeros((8, 128), F32) if x is None else x for x in acc]


def tile_cols(t):
    return slice(128 * t, 128 * t + 128)


def pair_at(m, count=1):
    size = 2 * LANES * count
    return pl.ds(pl.multiple_of(size * m, 128), size)


def phase_pass(
    m, j, gs, me, recv, recv_t, table3, hot, hot_t, from_pose, dep, rel, coup, sums, inverse3, kh
):
    at = pair_at(m)
    if j == 0:
        rows = lax.broadcasted_iota(jnp.int32, (256, 2 * LANES), 0).astype(F32)
        targets = jnp.concatenate([group_targets(g, recv_t) for g in gs], 1)
        hot[:, at] = jnp.where(rows == targets, 1.0, 0.0).astype(BF16)
        lanes = lane_iota((128, 256)).astype(F32)
        for t in range(6):
            column = jnp.broadcast_to(targets[:, tile_cols(t)], (128, 128)).T
            column = jnp.concatenate([column, column], 1)
            to = pl.ds(pl.multiple_of(2 * LANES * m + 128 * t, 128), 128)
            hot_t[to, :] = jnp.where(lanes == column, 1.0, 0.0).astype(BF16)
        near = gathered(table3[...], hot[:, at])
        dep[m] = near[0:24]
        relative = jnp.concatenate([rows_of(from_pose, g) for g in gs], 1) - near[24:32]
        rel[m] = relative
    else:
        relative = rel[m]
        back = gathered(inverse3[j - 1], hot[:, at])
    parts = [unpack_group(g, j, recv) for g in gs]
    grads, curvs, blocks = [], [], []
    xy = pixel_xy(me, j)
    for t in range(6):
        cols = tile_cols(t)
        acc = [None] * 27
        d = dep[m, 8 * j : 8 * j + 8, cols]
        tiles = [part[t % 3] for part in parts[t // 3]]
        gd, cd = build_terms(acc, cols, tiles, d, relative, xy, coup, m, j)
        grads.append(gd)
        curvs.append(cd)
        if j > 0:
            take_terms(acc, cols, (back[0:8, cols], back[8:16, cols]), coup, m, j - 1)
        blocks.append(merged_rows(filled(acc)))
    both = jnp.concatenate([jnp.concatenate(grads, 1), jnp.concatenate(curvs, 1)], 0)
    sums[j] += summed(both, hot_t[at, :])
    block = jnp.concatenate(blocks, 1)
    kh[m] = block if j == 0 else kh[m] + block


def last_pass(h, hot, hot_t, own_t, coup, inverse3, kh, total_s, total_t):
    at = pair_at(h, 4)
    near = gathered(inverse3[2], hot[:, at])
    blocks = []
    for t in range(24):
        m = 4 * h + t // 6
        acc = [None] * 27
        cols = tile_cols(t)
        take_terms(acc, tile_cols(t % 6), (near[0:8, cols], near[8:16, cols]), coup, m, 2)
        blocks.append(kh[m, :, tile_cols(t % 6)] + merged_rows(acc))
    parts = split3(jnp.concatenate(blocks, 1))
    total_t[...] += join3(jnp.dot(parts, hot_t[at, :], preferred_element_type=F32))
    total_s[h] = join3(jnp.dot(parts, own_t[...], preferred_element_type=F32))


def third_pass(h, gs, hot_t, coup, from_steps, fix):
    parts = []
    for t in range(24):
        m, cols = 4 * h + t // 6, tile_cols(t % 6)
        motion = rows_of(from_steps, gs[t // 3])
        column = []
        for j in range(3):
            terms = [
                coup[m, edge_rows(a, j), cols] * motion[a : a + 1, tile_cols(t % 3)]
                for a in range(6)
            ]
            column.append(((terms[0] + terms[1]) + (terms[2] + terms[3])) + (terms[4] + terms[5]))
        parts.append(jnp.concatenate(column, 0))
    fix[...] += summed(jnp.concatenate(parts, 1), hot_t[pair_at(h, 4), :])


def solve(matrix, right):
    factor, scale = {}, {}
    for i in range(6):
        for j in range(i + 1):
            e = matrix(i, j)
            if i == j:
                e = e * 1.1 + 0.001
            for k in range(j):
                e = e - factor[i, k] * factor[j, k]
            if i == j:
                scale[i] = 1.0 / jnp.sqrt(e)
            else:
                factor[i, j] = e * scale[j]
    forward = []
    for i in range(6):
        e = right(i)
        for k in range(i):
            e = e - factor[i, k] * forward[k]
        forward.append(e * scale[i])
    z = [None] * 6
    for i in reversed(range(6)):
        e = forward[i]
        for k in range(i + 1, 6):
            e = e - factor[k, i] * z[k]
        z[i] = e * scale[i]
    return z


def ring_steps(d):
    return min(d, 4 - d)


def hops(offset):
    return ring_steps(offset[0]) + ring_steps(offset[1]) + ring_steps(offset[2])


def far_first():
    offsets = [
        (dz, dy, dx, dc)
        for dz in range(4)
        for dy in range(4)
        for dx in range(4)
        for dc in range(2)
        if (dz, dy, dx, dc) != (0, 0, 0, 0)
    ]
    return sorted(offsets, key=lambda o: -hops(o))


def group_offset(n):
    return (n // 4 + n) % 4, n % 4


def pair_order(m, far_ahead):
    order = []
    for n in (2 * m, 2 * m + 1):
        oz, oy = group_offset(n)
        members = [
            ((oz + dx) % 4, (oy + dx) % 4, dx, dc) for dx in range(4) for dc in range(2)
        ]
        order += sorted(members, key=lambda o: -hops(o)) if far_ahead else members
    return [o for o in order if o != (0, 0, 0, 0)]


def to_all(order, act):
    row, col = lax.axis_index("row"), lax.axis_index("col")
    y, x = col // 8, (col // 2) % 4
    zs = [((row + d) % 4) * 32 for d in range(4)]
    ys = [((y + d) % 4) * 8 for d in range(4)]
    xs = [((x + d) % 4) * 2 for d in range(4)]
    cs = [(col + d) % 2 for d in range(2)]
    gz = [((row + 4 - x + d) % 4) * 32 for d in range(4)]
    gy = [((y + 4 - x + d) % 4) * 8 for d in range(4)]
    for dz, dy, dx, dc in order:
        last = xs[dx] + cs[dc]
        act(zs[dz] + ys[dy] + last, gz[(dz - dx) % 4] + gy[(dy - dx) % 4] + last)


def slot_of(d):
    return (d % 16) * 8 + d // 16


def rows_exchange(send, recv, source, slot, send_sem, recv_sem):
    def act(d, place):
        pltpu.make_async_remote_copy(
            src_ref=send.at[pl.ds(source(d, place), 1), :],
            dst_ref=recv.at[pl.ds(slot, 1), :],
            send_sem=send_sem,
            recv_sem=recv_sem,
            device_id=d,
            device_id_type=pl.DeviceIdType.LOGICAL,
        ).start()

    to_all(far_first(), act)


def steps_exchange(order, send, source, recv, slot, send_sem, recv_sem):
    def act(d, _):
        pltpu.make_async_remote_copy(
            src_ref=send.at[pl.ds(source, 1), :],
            dst_ref=recv.at[pl.ds(slot, 1), :],
            send_sem=send_sem,
            recv_sem=recv_sem,
            device_id=d,
            device_id_type=pl.DeviceIdType.LOGICAL,
        ).start()

    to_all(order, act)


def rows_wait(buf, sem, count=NDEV - 1):
    ref = buf.at[pl.ds(0, count), :]
    pltpu.make_async_copy(ref, ref, sem).wait()


def scope(name):
    return contextlib.nullcontext()


def loop(body, count):
    def step(n, carry):
        body(n)
        return carry

    lax.fori_loop(0, count, step, 0)


def main_kernel(
    flow_hbm, weight_hbm, depth_hbm, target_hbm, rotation_hbm, translation_hbm,
    recv_f, pose_hbm,
    flow, weight, depth_ref, target_ref, rotation_ref, translation_ref, low, high, chunks, ints, floats, unfold,
    recv, table, table3, hot, hot_t, own, own_t, from_pose, dep, rel, coup, sums, inverse,
    inverse3, kh,
    total_s, total_t, at_target, steps, from_steps, fix,
    send_t, recv_t, sum_d, send_d, recv_d, send_e, recv_e, send_f, pose_ref,
    in_sem, out_sem, big_send, big_recv, small_send, small_recv,
):
    row, col = lax.axis_index("row"), lax.axis_index("col")
    me = row * 32 + col
    y, x = col // 8, (col // 2) % 4
    my_gz, my_gy = (row + 4 - x) % 4, (y + 4 - x) % 4
    my_group = my_gz * 4 + my_gy
    mine_at = my_group * 8 + col % 8
    other_at = my_group * 8 + (col + 4) % 8
    lane = lane_iota()
    barrier = pltpu.get_barrier_semaphore()

    inputs = [
        (depth_hbm, depth_ref),
        (target_hbm, target_ref),
        (rotation_hbm, rotation_ref),
        (translation_hbm, translation_ref),
        (flow_hbm, flow),
        (weight_hbm, weight),
    ]
    loads = [
        pltpu.make_async_copy(source, to, in_sem.at[k]) for k, (source, to) in enumerate(inputs)
    ]

    def greet(d, _):
        pl.semaphore_signal(
            barrier, inc=1, device_id=d, device_id_type=pl.DeviceIdType.LOGICAL
        )

    with scope("sc_greet"):
        for load in loads:
            load.start()
        to_all(far_first(), greet)

    with scope("sc_tables"):
        high[...] = jnp.zeros_like(high)
        for load in loads[:4]:
            load.wait()
        column, pose = own_edges(target_ref, rotation_ref, translation_ref, ints, floats)
        pack_tables(depth_ref, column, pose, unfold, send_t)
        recv_t[pl.ds(mine_at, 1), :] = send_t[pl.ds(slot_of(me), 1), :]
        turn = col % 8
        for load in loads[4:]:
            load.wait()

    def pack(j):
        def step(b, carry):
            pack_half(b, j, turn, flow, weight, low, high, chunks)
            return carry

        lax.fori_loop(0, 2, step, 0)

    with scope("sc_pack"):
        pack(0)
    with scope("sc_barrier"):
        pl.semaphore_wait(barrier, NDEV - 1)

    with scope("sc_sends"):
        rows_exchange(
            send_t, recv_t, lambda d, _: slot_of(d), mine_at, small_send.at[3], small_recv.at[3]
        )

        def send_phase(j):
            for m in range(8):

                def send_chunk(d, _):
                    pltpu.make_async_remote_copy(
                        src_ref=chunks.at[d, j, pl.ds(0, 12), :],
                        dst_ref=recv.at[mine_at, j, pl.ds(0, 12), :],
                        send_sem=big_send,
                        recv_sem=big_recv.at[j, m],
                        device_id=d,
                        device_id_type=pl.DeviceIdType.LOGICAL,
                    ).start()

                to_all(pair_order(m, j == 2), send_chunk)

        send_phase(0)
        pack(1)
        pack(2)
        send_phase(1)
        send_phase(2)
        recv[mine_at, :, 0:12, :] = chunks[me, :, 0:12, :]

    with scope("sc_waitt"):
        for ref in (sums, total_t, fix, at_target):
            ref[...] = jnp.zeros_like(ref)
        own[...] = source_columns()
        own_t[...] = source_columns_t()
        rows_wait(recv_t, small_recv.at[3])
        known = recv_t[...].T
        for f in range(2):
            at = slice(128 * f, 128 * f + 128)
            table[0:24, at] = known[24 * f : 24 * f + 24]
            table[24:32, at] = known[48 + 8 * f : 56 + 8 * f]
        table3[...] = split3(table[...])
        expand(table[24:32, :], own, from_pose)

    def group_at(n):
        oz, oy = group_offset(n)
        return ((my_gz + 4 - oz) % 4) * 4 + (my_gy + 4 - oy) % 4

    def arrive(m, j):
        gs = [group_at(2 * m), group_at(2 * m + 1)]

        def landed(count):
            ref = recv.at[pl.ds(0, count), j, pl.ds(0, 12), :]
            pltpu.make_async_copy(ref, ref, big_recv.at[j, m]).wait()

        pl.when(m == 0)(lambda: landed(15))
        pl.when(m != 0)(lambda: landed(16))
        phase_pass(
            m, j, gs, me, recv, recv_t, table3, hot, hot_t, from_pose, dep, rel, coup, sums,
            inverse3, kh,
        )

    for j in range(3):
        with scope(f"sc_arrive{j}"):
            loop(functools.partial(arrive, j=j), 8)
            ci = 1.0 / (0.1 + sums[j, 8:16])
            both = jnp.concatenate([ci, sums[j, 0:8] * ci], 0)
            inverse[j] = both
            inverse3[j] = split3(both)
    with scope("sc_last"):
        loop(lambda h: last_pass(h, hot, hot_t, own_t, coup, inverse3, kh, total_s, total_t), 2)

    with scope("sc_sendd"):
        kind = lax.broadcasted_iota(jnp.int32, (32, 256), 0)
        total = jnp.where(kind < H_ROW, total_t[...], -total_t[...])
        by_target = jnp.concatenate(
            [total[:, 0:128], total[:, 128:256], jnp.zeros((64, 128), F32)], 0
        ).T
        for h in range(2):
            by_source = jnp.concatenate([total_s[h], jnp.zeros((96, 128), F32)], 0).T
            for k in range(8):
                to = pl.ds(pl.multiple_of(8 * group_at(8 * h + k), 8), 8)
                first, second = by_source[16 * k : 16 * k + 8], by_source[16 * k + 8 : 16 * k + 16]
                sum_d[to, :] = first + pltpu.roll(second, 32, 1)
        rows = by_target + sum_d[...]
        opposite = [pltpu.roll(rows[8 * g : 8 * g + 8], 4, 0) for g in range(GROUPS)]
        send_d[...] = rows + pltpu.roll(jnp.concatenate(opposite, 0), 64, 1)
        recv_d[pl.ds(mine_at, 1), :] = send_d[pl.ds(mine_at, 1), :]
        rows_exchange(
            send_d, recv_d, lambda _, place: place, mine_at, small_send.at[0], small_recv.at[0]
        )
    with scope("sc_target"):

        def couple(m):
            at_target[...] += summed(coup[m], hot_t[pair_at(m), :])

        loop(couple, 8)
    with scope("sc_waitd"):
        rows_wait(recv_d, small_recv.at[0])
    with scope("sc_solve"):
        line = jnp.sum(recv_d[...], axis=0, keepdims=True)
        sub = lax.broadcasted_iota(jnp.int32, (8, 128), 0)
        lines = jnp.broadcast_to(line, (8, 128))
        for f in range(1, 4):
            lines = jnp.where(sub == f, pltpu.roll(lines, 128 - 32 * f, 1), lines)
        full = jnp.concatenate([lines, jnp.zeros((120, 128), F32)], 0).T
        z = solve(
            lambda i, j: full[K_INDEX[i, j] : K_INDEX[i, j] + 1, :],
            lambda i: full[H_ROW + i : H_ROW + i + 1, :],
        )
        zs = jnp.concatenate([*z, jnp.zeros((122, 128), F32)], 0)
        turned = zs.T
        pose_ref[...] = turned[0:2, 0:6]
        pose_out = pltpu.make_async_copy(pose_ref, pose_hbm, out_sem.at[0])
        pose_out.start()
        later = pltpu.roll(turned[0:8], 8, 1)
        mine, other = turned[0:1] + later[1:2], turned[2:3] + later[3:4]
        send_e[...] = jnp.where(sub == 0, mine, other)
        recv_e[pl.ds(mine_at, 1), :] = mine
        recv_e[pl.ds(other_at, 1), :] = other
    with scope("sc_sende"):
        near = [o for o in far_first() if hops(o) <= 3]
        steps_exchange(near, send_e, 0, recv_e, mine_at, small_send.at[1], small_recv.at[1])
        near = [o for o in near if hops(o) <= 2]
        steps_exchange(near, send_e, 1, recv_e, other_at, small_send.at[1], small_recv.at[1])
    with scope("sc_waite"):
        rows_wait(recv_e, small_recv.at[1], NDEV - 2)
    with scope("sc_third"):
        every = recv_e[...].T
        steps[:, 0:128] = every[0:8]
        steps[:, 128:256] = every[8:16]
        expand(steps[...], own, from_steps)
        loop(
            lambda h: third_pass(
                h, [group_at(8 * h + k) for k in range(8)], hot_t, coup, from_steps, fix
            ),
            2,
        )
    with scope("sc_sendf"):
        back = at_target[0:24] * steps[0:1]
        for a in range(1, 6):
            back += at_target[24 * a : 24 * a + 24] * steps[a : a + 1]
        grad = jnp.concatenate([sums[j, 0:8] for j in range(3)], 0)
        ci = jnp.concatenate([inverse[j, 0:8] for j in range(3)], 0)
        new = table[0:24] + (grad - (fix[...] - back)) * ci
        zero8 = jnp.zeros((8, 128), F32)
        send_f[...] = jnp.concatenate(
            [new[:, 0:128], zero8, new[:, 128:256], zero8, jnp.zeros((64, 128), F32)], 0
        ).T
        slot = slot_of(me)
        own_row = pltpu.make_async_copy(
            send_f.at[pl.ds(mine_at, 1), :], recv_f.at[pl.ds(slot, 1), :], out_sem.at[1]
        )
        own_row.start()
        rows_exchange(
            send_f, recv_f, lambda _, place: place, slot, small_send.at[2], small_recv.at[2]
        )
    with scope("sc_waitf"):
        rows_wait(recv_f, small_recv.at[2])
    own_row.wait()
    pose_out.wait()
    ref = chunks.at[pl.ds(0, NDEV - 1), :, pl.ds(0, 12), :]
    pltpu.make_async_copy(ref, ref, big_send).wait()
    rows_wait(recv_t, small_send.at[3])
    rows_wait(recv_d, small_send.at[0])
    rows_wait(recv_e, small_send.at[1], NDEV - 2)
    rows_wait(recv_f, small_send.at[2])


def run_main(flow, weight, inv_depth, edge_target, rotation, translation):
    v = pltpu.VMEM
    hbm = pl.BlockSpec(memory_space=pltpu.HBM)
    return pl.pallas_call(
        main_kernel,
        in_specs=[hbm] * 6,
        out_specs=[hbm] * 2,
        out_shape=[
            jax.ShapeDtypeStruct((NDEV, 128), F32),
            jax.ShapeDtypeStruct((2, 6), F32),
        ],
        scratch_shapes=[
            v((2, 48, PX * NDEV), F32),
            v((2, 48, PX * NDEV), F32),
            v((2, PX * NDEV), F32),
            v((2, 24), jnp.int32),
            v((2, 3), F32),
            v((2, 3), F32),
            v((128, 512), F32),
            v((128, 512), F32),
            v((NDEV, 3, 16, 128), F32),
            v((8, 128), jnp.int32),
            v((2, 8, 128), F32),
            v((2, 3, 8, 128), F32),
            v((NDEV, 3, 16, 128), F32),
            v((32, 256), F32),
            v((96, 256), BF16),
            v((256, GROUPS * LANES), BF16),
            v((GROUPS * LANES, 256), BF16),
            v((128, LANES), BF16),
            v((8 * LANES, 128), BF16),
            v((128, LANES), F32),
            v((8, 24, 2 * LANES), F32),
            v((8, 8, 2 * LANES), F32),
            v((8, 144, 2 * LANES), F32),
            v((3, 16, 256), F32),
            v((3, 16, 256), F32),
            v((3, 48, 256), BF16),
            v((8, 32, 2 * LANES), F32),
            v((2, 32, 128), F32),
            v((32, 256), F32),
            v((144, 256), F32),
            v((8, 256), F32),
            v((128, LANES), F32),
            v((24, 256), F32),
            v((128, 128), F32),
            v((128, 128), F32),
            v((128, 128), F32),
            v((128, 128), F32),
            v((128, 128), F32),
            v((8, 128), F32),
            v((128, 128), F32),
            v((128, 128), F32),
            v((2, 6), F32),
            pltpu.SemaphoreType.DMA((6,)),
            pltpu.SemaphoreType.DMA((2,)),
            pltpu.SemaphoreType.DMA,
            pltpu.SemaphoreType.DMA((3, GROUPS // 2)),
            pltpu.SemaphoreType.DMA((4,)),
            pltpu.SemaphoreType.DMA((4,)),
        ],
        compiler_params=pltpu.CompilerParams(
            collective_id=0, has_side_effects=True, vmem_limit_bytes=56 * 1024 * 1024
        ),
        name="step",
    )(flow, weight, inv_depth, edge_target, rotation, translation)


def hand_over(parts, pose):
    def kernel(recv_f, pose_ref, out_ref, pose_out):
        lane = lane_iota()
        pose_out[...] = pose_ref[...]
        for f in range(2):
            for j in range(3):
                tile = None
                for i in range(16):
                    shift = 8 * i - 32 * f - 8 * j
                    moved = pltpu.roll(recv_f[8 * i : 8 * i + 8, :], shift % 128, 1)
                    tile = moved if i == 0 else jnp.where(lane >= 8 * i, moved, tile)
                for g in range(8):
                    at = 128 * (8 * j + g)
                    out_ref[f : f + 1, at : at + 128] = tile[g : g + 1]

    vmem = pl.BlockSpec(memory_space=pltpu.VMEM)
    return pl.pallas_call(
        kernel,
        in_specs=[vmem] * 2,
        out_specs=[vmem] * 2,
        out_shape=[
            jax.ShapeDtypeStruct((2, PX * NDEV), F32),
            jax.ShapeDtypeStruct((2, 6), F32),
        ],
        compiler_params=pltpu.CompilerParams(vmem_limit_bytes=56 * 1024 * 1024),
        name="hand_over",
    )(parts, pose)


def shards(inv_depth, rotation, translation, edge_target, flow_obs, weight):
    pixels = inv_depth.shape[1]
    flow = flow_obs.reshape(2, 48, pixels)
    wts = weight.reshape(2, 48, pixels)
    depth, pose = hand_over(
        *run_main(flow, wts, inv_depth, edge_target, rotation.T, translation.T)
    )
    return depth, pose.T


def solution(mesh):
    in_specs = (
        P(("row", "col"), None),
        P(None, ("row", "col")),
        P(None, ("row", "col")),
        P(("row", "col"), None),
        P(None, ("row", "col"), None, None),
        P(None, ("row", "col"), None, None),
    )
    out_specs = (P(("row", "col"), None), P(None, ("row", "col")))
    return jax.shard_map(
        shards, mesh=mesh, in_specs=in_specs, out_specs=out_specs, check_vma=False
    )
```
